32 devices in a mesh: chan: 4 (over y, x), rows: 8 (over z, core).
Axes of the slice: x: 2, y: 2, z: 4, core: 2. Of those that a mesh axis runs over, the one named last changes fastest.
Arguments:
- residual: float32 [4, 256, 16384], P('chan', 'rows'), may hold values from -6 to 6
- psf: float32 [4, 2048, 2048], P('chan', 'rows'), may hold values from -2 to 2
- positions: int32 [32, 2], replicated, may hold values from 0 to 15360, as said below
Outputs:
- residual_out: float32 [4, 256, 16384], P('chan', 'rows')
- normalized: float32 [256, 16384], P('rows', 'chan')
The draws below stay inside these ranges and needn't reach their ends.
Inputs may be any that keep to these rules, and one draw needn't show every extreme that they name: positions[k, 0] is a row of the image, 0 to 255; positions[k, 1] is a column from 1024 to 15360.
All inputs are finite; a program needn't handle non-finite values.
Results may differ from the reference program's by a relative error of at most 0.0001.
Values sent between devices are 32-bit elements; how exact they have to be, the bound alone decides.
A program may use at most 128 MiB of HBM per device.

```python
import jax
import jax.numpy as jnp
from jax import lax

CHANNELS = 4
NCOL = 16384
PATCH = 2048
STEPS = 32
NX = 256


def draw_positions(key, part):
    half = PATCH // 2
    row_key = jax.random.fold_in(key, 11)
    col_key = jax.random.fold_in(key, 12)
    pick_key = jax.random.fold_in(key, 13)
    rows = jax.random.randint(row_key, (STEPS,), 0, NX)
    cols = jax.random.randint(col_key, (STEPS,), half, NCOL - half + 1)
    picks = jax.random.randint(pick_key, (2,), 0, STEPS)
    low_step = picks[0]
    high_step = (low_step + 1) % STEPS
    rows = rows.at[low_step].set(0)
    rows = rows.at[high_step].set(NX - 1)
    cols = cols.at[picks[1]].set(NCOL - half)
    return jnp.stack([rows, cols], axis=1).astype(jnp.int32)


def block_scale(key, shape, shards, least, largest):
    factor_of, own = 1.0, jax.random.fold_in(key, 6)
    for axis_at, parts in shards:
        draws = jnp.exp(jax.random.uniform(jax.random.fold_in(own, axis_at), (parts,), jnp.float32, least / len(shards), largest / len(shards)))
        factor_of = factor_of * jnp.repeat(draws, shape[axis_at] // parts).reshape([-1 if axis == axis_at else 1 for axis in range(len(shape))])
    return factor_of


def normal_values(key, extent, deviation, reach, pieces=(), dtype=jnp.bfloat16):
    array = deviation * jax.random.normal(key, extent, jnp.float32)
    if pieces:
        array = array * block_scale(key, extent, pieces, -0.22, 0.18)
    return jnp.clip(array, -reach, reach).astype(dtype)


def setup_inputs(seed: int = 0) -> dict:
    key_list = jax.random.split(jax.random.key(seed), 4)
    residual = normal_values(key_list[0], (CHANNELS, NX, NCOL), 1.0, 6.0, ((0, 4), (1, 8)), jnp.float32)
    psf = normal_values(key_list[1], (CHANNELS, PATCH, PATCH), 0.3, 2.0, ((0, 4), (1, 8)), jnp.float32)
    positions = draw_positions(jax.random.fold_in(key_list[3], 71), 0)
    return {"residual": residual, "psf": psf, "positions": positions}


def reference(residual, psf, positions):
    half = PATCH // 2
    padded = jnp.pad(residual, ((0, 0), (half, half), (0, 0)))
    zero = jnp.int32(0)

    def step(k, image):
        row = positions[k, 0].astype(jnp.int32)
        col = positions[k, 1].astype(jnp.int32)
        value = lax.dynamic_slice(image, (zero, row + half, col), (CHANNELS, 1, 1)).reshape(CHANNELS)
        total = jnp.sum(value)
        amp = 0.25 * (value + total / CHANNELS)
        window = lax.dynamic_slice(image, (zero, row, col - half), (CHANNELS, PATCH, PATCH))
        window = window - amp[:, None, None] * psf
        return lax.dynamic_update_slice(image, window, (zero, row, col - half))
    padded = lax.fori_loop(0, STEPS, step, padded)
    image = padded[:, half:half + NX, :]
    summed = lax.optimization_barrier(jnp.sum(image, axis=0))
    mean_square = jnp.mean(summed * summed)
    return (image, summed * lax.rsqrt(mean_square + 1e-06))
```

```python
import functools

import jax
import jax.numpy as jnp
from jax import lax
from jax.experimental import pallas as pl
from jax.experimental.pallas import tpu as pltpu
from jax.sharding import PartitionSpec as P

STEPS = 32
LANES = 128
MESH = pl.DeviceIdType.MESH
OUT = pltpu.VMEM


def pick(tile, row, col, lane_to, owned, number, acc):
    moved = pltpu.roll(tile, (lane_to - col) & (LANES - 1), 1)
    target = jnp.where(owned, (row & 7) * LANES + lane_to, -1)
    return jnp.where(number == target, moved, acc)


def cycle_kernel(nchan, nrows, pos, res, psf, image, parts, total_out,
                 work, land, patch_v, psf_v, grid, couple_v, couple_in, start_v, start_in, tables, amps_v, prev_v, last_v,
                 first_far, first_own, passed, second, squares, prev_s, last_s, amps_s,
                 ready, band_sem, psf_sem, index_sem, send_sem, unit_recv, recv_sem, relay_sem, fine_send, fine_recv, fine_relay,
                 start_send, start_recv, couple_send, couple_recv, table_send, table_recv, amp_send, amp_recv,
                 far_send, far_recv, own_send, own_recv, pass_send, pass_recv, square_send, square_recv):
    chan, row = lax.axis_index("chan"), lax.axis_index("rows")
    chip, core = row // 2, row % 2
    partner = row + 1 - 2 * core
    nchips = nrows // 2
    side = chip // (nchips // 2)
    slab, ncols = res.shape[1], res.shape[2]
    shard, patch = psf.shape[1:]
    half, steps, chunks = patch // 2, pos.shape[1], patch // LANES
    unit, tiles, blocks = 2 * slab, slab // 8, ncols // LANES
    base, width = blocks + 1, chunks + 1
    first = row * slab
    roots = (nchips - 1, nchips)
    solvers = (roots[0] ^ 1, roots[1] ^ 1)
    is_root = jnp.logical_or(row == roots[0], row == roots[1])
    is_solver = jnp.logical_or(row == solvers[0], row == solvers[1])
    is_mid = jnp.logical_or(is_root, is_solver)
    is_end = jnp.logical_not(is_mid)
    lane = lax.broadcasted_iota(jnp.int32, (1, LANES), 1)
    lane8 = lax.broadcasted_iota(jnp.int32, (8, LANES), 1)
    number = lax.broadcasted_iota(jnp.int32, (8, LANES), 0) * LANES + lane8
    zero = jnp.zeros((8, LANES), jnp.float32)

    def block_at(index):
        return pl.ds(pl.multiple_of(index * LANES, LANES), LANES)

    bands = [pltpu.make_async_copy(res.at[0, pl.ds(8 * t, 8)], image.at[pl.ds(8 * t, 8)], band_sem.at[t]) for t in range(tiles)]
    for copy in bands:
        copy.start()
    loads = [pltpu.make_async_copy(psf.at[0, :, pl.ds(c * LANES, LANES)], psf_v.at[c], psf_sem.at[c]) for c in range(chunks)]

    barrier = pltpu.get_barrier_semaphore()
    for step in range(1, nrows):
        pl.semaphore_signal(barrier, inc=1, device_id=(chan, (row + step) % nrows), device_id_type=MESH)
    for step in range(1, nchan):
        pl.semaphore_signal(barrier, inc=1, device_id=((chan + step) % nchan, row), device_id_type=MESH)

    @pl.when(is_root)
    def _():
        for copy in loads:
            copy.start()

    begins = [jnp.clip(pos[1, k] - half, 0, ncols - patch) >> 7 for k in range(steps)]
    krow = lax.broadcasted_iota(jnp.int32, (steps, LANES), 0)
    target = jnp.zeros((steps, LANES), jnp.int32)
    for k in range(steps):
        target = jnp.where(krow == k, begins[k], target)
    target = target + lax.broadcasted_iota(jnp.int32, (steps, LANES), 1)
    prev, last = target, lane8
    for k in range(steps):
        inside = target - begins[k]
        prev = jnp.where((inside >= 0) & (inside < width) & (krow > k), inside + (base + width * k), prev)
        inside = lane8 - begins[k]
        last = jnp.where((inside >= 0) & (inside < width), inside + (base + width * k), last)
    prev_v[...] = prev
    last_v[...] = last
    index_copies = [pltpu.make_async_copy(prev_v, prev_s, index_sem.at[0]), pltpu.make_async_copy(last_v, last_s, index_sem.at[1])]
    for copy in index_copies:
        copy.start()
    for t in range(tiles):
        work[t, blocks] = zero
    pl.semaphore_wait(barrier, nrows + nchan - 2)

    def bulk(s):
        mid, end, other = (nchips - 1 + s) // 2, (nchips - 1) * s, nchips // 2 - s
        order = (0, 1) if s == 0 else (1, 0)
        near = list(range(nchips)) if s == 0 else list(range(2 * nchips - 1, nchips - 1, -1))
        across = [nchips - 1 - n if s == 0 else nchips + n for n in range(nchips // 2)]
        local = [u for u in range(mid, mid + nchips + 1) if (u < nchips) == (s == 0)]
        out = []

        def add(u, z, h, rows, to_row, sem):
            out.append(pltpu.make_async_remote_copy(
                src_ref=psf.at[0, pl.ds((u % nchips) * unit + h * slab, rows)], dst_ref=land.at[pl.ds((u - z) * unit + h * slab, rows)],
                send_sem=send_sem.at[len(out)], recv_sem=sem, device_id=(chan, to_row), device_id_type=MESH))

        for u in near:
            for h in order:
                add(u, end, h, slab, 2 * end + h, recv_sem.at[u - end, h])
        for u in across:
            for h in range(2):
                add(u, other, h, slab, 2 * other + h, recv_sem.at[u - other, h])
        for u in local:
            add(u, mid, 0, unit, solvers[s], unit_recv.at[u - mid])
        return out

    for s in range(2):
        @pl.when(row == roots[s])
        def _(s=s):
            for copy in bulk(s):
                copy.start()

    for step in range(1, nchan):
        pl.semaphore_signal(ready, inc=1, device_id=((chan + step) % nchan, row), device_id_type=MESH)

    for copy in bands:
        copy.wait()

    def spread_out(b, carry):
        for t in range(tiles):
            work[t, b] = image[pl.ds(8 * t, 8), block_at(b)]
        return carry

    lax.fori_loop(0, blocks, spread_out, 0, unroll=4)
    acc = zero
    for k in range(steps):
        r, c = pos[0, k] - first, pos[1, k]
        tile = work[(r >> 3) & (tiles - 1), c >> 7]
        acc = pick(tile, r, c, k, (r >= 0) & (r < slab), number, acc)
    start_v[...] = acc

    def start_copy(s, source):
        return pltpu.make_async_remote_copy(
            src_ref=start_v, dst_ref=start_in.at[source], send_sem=start_send, recv_sem=start_recv.at[source],
            device_id=(chan, solvers[s]), device_id_type=MESH)

    def couple_copy(s):
        return pltpu.make_async_remote_copy(
            src_ref=couple_v, dst_ref=couple_in, send_sem=couple_send, recv_sem=couple_recv,
            device_id=(chan, solvers[s]), device_id_type=MESH)

    for s in range(2):
        @pl.when((side == s) & (row != solvers[s]))
        def _(s=s):
            start_copy(s, row).start()

    @pl.when(is_root)
    def _():
        for copy in loads:
            copy.wait()
        low = row * shard - half

        def fill(k, carry):
            rk, qk = pos[0, k] - low, pos[1, k] + half

            def test(g, acc):
                for i in range(8):
                    j = g * 8 + i
                    r, c = rk - pos[0, j], qk - pos[1, j]
                    owned = (r >= 0) & (r < shard) & (c >= 0) & (c < patch) & (j < k)
                    tile = psf_v[(c >> 7) & (chunks - 1), pl.ds(((r >> 3) << 3) & (shard - 1), 8), :]
                    acc = pick(tile, r, c, j, owned, number, acc)
                return acc

            grid[k] = lax.fori_loop(0, (k + 7) >> 3, test, zero)
            return carry

        lax.fori_loop(0, steps, fill, 0)
        couple_v[...] = jnp.sum(grid[...], axis=1)

    for s in range(2):
        @pl.when(row == roots[s])
        def _(s=s):
            couple_copy(s).start()

    def held(m, h, rows=slab):
        return land.at[pl.ds(pl.multiple_of(m * unit + h * slab, 8), rows)]

    def relay(m):
        return pltpu.make_async_remote_copy(
            src_ref=held(m, core), dst_ref=held(m, core), send_sem=relay_sem.at[m], recv_sem=recv_sem.at[m, core],
            device_id=(chan, partner), device_id_type=MESH)

    def arrival(m, h):
        return pltpu.make_async_remote_copy(
            src_ref=held(m, h), dst_ref=held(m, h), send_sem=relay_sem.at[m], recv_sem=recv_sem.at[m, h],
            device_id=(chan, partner), device_id_type=MESH)

    def pass_on(m):
        arrival(m, core).wait_recv()
        relay(m).start()

    def crossed(n):
        return jnp.where(side == 0, nchips - 1 + n, 1 - n)

    def streamed(n):
        return jnp.where(side == 0, n, nchips - n)

    def relayout(source, source_row, dest_row, rows):
        def body(g, carry):
            take, put = pl.multiple_of(source_row + 8 * g, 8), pl.multiple_of(dest_row + 8 * g, 8)
            for c in range(chunks):
                tile = source[c, pl.ds(take, 8), :] if len(source.shape) == 3 else source[pl.ds(take, 8), pl.ds(c * LANES, LANES)]
                patch_v[c, pl.ds(put, 8), :] = tile
            return carry

        lax.fori_loop(0, rows // 8, body, 0)

    @pl.when(is_mid)
    def _():
        pass_on(crossed(0))

    pl.semaphore_wait(ready, nchan - 1)
    me_table = 2 * chan + side

    def table_copy(step):
        other = (me_table + step) % (2 * nchan)
        return pltpu.make_async_remote_copy(
            src_ref=tables.at[me_table], dst_ref=tables.at[me_table], send_sem=table_send.at[step], recv_sem=table_recv.at[step],
            device_id=(other // 2, solvers[0] + (other % 2) * (solvers[1] - solvers[0])), device_id_type=MESH)

    def table_arrival(step):
        other = (me_table + 2 * nchan - step) % (2 * nchan)
        return pltpu.make_async_remote_copy(
            src_ref=tables.at[other], dst_ref=tables.at[other], send_sem=table_send.at[step], recv_sem=table_recv.at[step],
            device_id=(other // 2, solvers[0] + (other % 2) * (solvers[1] - solvers[0])), device_id_type=MESH)

    for s in range(2):
        @pl.when(row == solvers[s])
        def _(s=s):
            total = start_v[...]
            for source in range(s * nchips, (s + 1) * nchips):
                if source != solvers[s]:
                    start_copy(s, source).wait_recv()
                    total = total + start_in[source]
            couple_copy(s).wait_recv()
            tables[me_table, pl.ds(0, steps), :] = couple_in[...]
            tables[me_table, pl.ds(steps, 8), :] = jnp.broadcast_to(jnp.sum(total, axis=0, keepdims=True), total.shape)
            for step in range(1, 2 * nchan):
                table_copy(step).start()

    @pl.when(is_mid)
    def _():
        pass_on(crossed(1))

    def amp_copy(n):
        return pltpu.make_async_remote_copy(
            src_ref=amps_v, dst_ref=amps_v, send_sem=amp_send.at[n], recv_sem=amp_recv,
            device_id=(chan, side * nchips + (row + n) % nchips), device_id_type=MESH)

    @pl.when(is_solver)
    def _():
        for step in range(1, 2 * nchan):
            table_arrival(step).wait_recv()

        def rows_of(index):
            return jnp.concatenate([tables[2 * c, pl.ds(index, 1), :] + tables[2 * c + 1, pl.ds(index, 1), :] for c in range(nchan)], axis=0)

        start = rows_of(steps)

        def solve(k, amps):
            value = jnp.sum(jnp.where(lane == k, start, 0.0) - amps * rows_of(k), axis=1, keepdims=True)
            amp = 0.25 * (value + jnp.sum(value, axis=0, keepdims=True) / nchan)
            return jnp.where(lane == k, amp, amps)

        amps = lax.fori_loop(0, steps, solve, jnp.zeros((nchan, LANES), jnp.float32))
        amps_v[pl.ds(0, nchan), :] = amps
        amps_v[pl.ds(nchan, 8 - nchan), :] = jnp.zeros((8 - nchan, LANES), jnp.float32)
        for n in range(1, nchips):
            amp_copy(n).start()

    def fine_piece(n):
        return jnp.where(side == 0, n, 2 * tiles - 1 - n)

    def fine_at(n):
        return pl.multiple_of(jnp.where(side == 0, nchips, 0) * unit + 8 * fine_piece(n), 8)

    def onward_piece(s, n):
        mid, end = (nchips - 1 + s) // 2, (nchips - 1) * s
        u = nchips - s
        j = n if s == 0 else 2 * tiles - 1 - n
        return pltpu.make_async_remote_copy(
            src_ref=land.at[pl.ds((u - mid) * unit + 8 * j, 8)], dst_ref=land.at[pl.ds((u - end) * unit + 8 * j, 8)],
            send_sem=fine_send.at[n], recv_sem=fine_recv.at[n], device_id=(chan, 2 * end + j // tiles), device_id_type=MESH)

    def fine_copy(n):
        return pltpu.make_async_remote_copy(
            src_ref=land.at[pl.ds(fine_at(n), 8)], dst_ref=land.at[pl.ds(fine_at(n), 8)],
            send_sem=fine_relay.at[n], recv_sem=fine_recv.at[n], device_id=(chan, partner), device_id_type=MESH)

    for s in range(2):
        mid = (nchips - 1 + s) // 2
        local = [u for u in range(mid, mid + nchips + 1) if (u < nchips) == (s == 0)]

        @pl.when(row == roots[s])
        def _(s=s, mid=mid, local=local):
            arrival(crossed(0), 1 - core).wait_recv()
            for n in range(2 * tiles):
                onward_piece(s, n).start()
            relayout(psf_v, (local[0] % nchips) * unit, (local[0] - mid) * unit, len(local) * unit)

        @pl.when(row == solvers[s])
        def _(s=s, mid=mid, local=local):
            arrival(crossed(0), 1 - core).wait_recv()
            for u in local:
                pltpu.make_async_remote_copy(
                    src_ref=held(u - mid, 0, unit), dst_ref=held(u - mid, 0, unit), send_sem=send_sem.at[0], recv_sem=unit_recv.at[u - mid],
                    device_id=(chan, partner), device_id_type=MESH).wait_recv()
            relayout(land, (local[0] - mid) * unit, (local[0] - mid) * unit, len(local) * unit)

    @pl.when(is_mid)
    def _():
        arrival(crossed(1), 1 - core).wait_recv()
        begin = jnp.where(side == 0, nchips - 1, 0) * unit
        relayout(land, begin, begin, 2 * unit)

    @pl.when(is_end)
    def _():
        for n in range(nchips):
            pass_on(streamed(n))
        for n in range(nchips):
            arrival(streamed(n), 1 - core).wait_recv()
        begin = jnp.where(side == 0, 0, 1) * unit
        relayout(land, begin, begin, nchips * unit)

    @pl.when(jnp.logical_not(is_solver))
    def _():
        amp_copy(1).wait_recv()

    amps_copy = pltpu.make_async_copy(amps_v, amps_s, index_sem.at[2])
    amps_copy.start()
    for copy in index_copies:
        copy.wait()
    amps_copy.wait()

    leading = core == side
    cols = ncols // nchan
    span = cols // 2
    bits = ((1, 2), (2, 1))
    top = core * slab + slab * nrows

    def flip(bit):
        if bit == 1:
            return chan + 1 - 2 * (chan % 2)
        return (chan + 2) % 4

    diagonal = 3 - chan

    def tile_at(i):
        return jnp.where(side == 0, i, tiles - 1 - i)

    def rows_at(i):
        return pl.ds(pl.multiple_of(8 * tile_at(i), 8), 8)

    def cols_at(c, p):
        return pl.ds(pl.multiple_of(c * cols + p * span, LANES), span)

    def send(i, p, source, dest, send_sem, recv_sem, to):
        return pltpu.make_async_remote_copy(
            src_ref=source, dst_ref=dest.at[i, p], send_sem=send_sem.at[i, p], recv_sem=recv_sem.at[i, p],
            device_id=(to, row), device_id_type=MESH)

    def far(i, p):
        return send(i, p, image.at[rows_at(i), cols_at(diagonal, p)], first_far, far_send, far_recv, flip(bits[p][0]))

    def mine(i, p):
        return send(i, p, image.at[rows_at(i), cols_at(flip(bits[p][0]), p)], first_own, own_send, own_recv, flip(bits[p][0]))

    def onward(i, p):
        return send(i, p, passed.at[i, p], second, pass_send, pass_recv, flip(bits[p][1]))

    def fetch(n):
        fine_copy(n).wait_recv()

    def pieces_for(i):
        @pl.when(is_end & leading)
        def _():
            fetch(i)
            fine_copy(i).start()
            relayout(land, fine_at(i), fine_at(i), 8)

        @pl.when(is_end & jnp.logical_not(leading))
        def _():
            for n in (range(tiles + 1) if i == 0 else (tiles + i,)):
                fetch(n)
                relayout(land, fine_at(n), fine_at(n), 8)

    def apply(i):
        t = tile_at(i)
        lift = top + 8 * t

        def two(kk, carry):
            for k in (2 * kk, 2 * kk + 1):
                amp = amps_s[chan, k]
                begin = lift - pos[0, k]
                shift = (pos[1, k] - half) & (LANES - 1)
                keep = lane8 < shift
                moved = [zero] + [pltpu.roll(patch_v[c, pl.ds(begin, 8), :] * amp, shift, 1) for c in range(chunks)] + [zero]
                for m in range(width):
                    change = jnp.where(keep, moved[m], moved[m + 1])
                    work[t, base + width * k + m] = work[t, prev_s[k, m]] - change
            return carry

        lax.fori_loop(0, steps // 2, two, 0)

    def finalize(i, c):
        rows = rows_at(i)
        per = cols // LANES

        def body(g, carry):
            for n in range(8):
                b = c * per + g * 8 + n
                image[rows, block_at(b)] = work[tile_at(i), last_s[0, b]]
            return carry

        lax.fori_loop(0, per // 8, body, 0)

    def combine(i):
        for p in range(2):
            far(i, p).wait_recv()
            passed[i, p] = image[rows_at(i), cols_at(flip(bits[p][1]), p)] + first_far[i, p]
            onward(i, p).start()

    for i in range(tiles):
        pieces_for(i)
        apply(i)
        finalize(i, diagonal)
        for p in range(2):
            far(i, p).start()
        if i > 0:
            combine(i - 1)
        for p in range(2):
            finalize(i, flip(bits[p][0]))
            mine(i, p).start()
        finalize(i, chan)
    combine(tiles - 1)
    total = zero
    for i in range(tiles):
        for p in range(2):
            mine(i, p).wait_recv()
            onward(i, p).wait_recv()
            value = image[rows_at(i), cols_at(chan, p)] + first_own[i, p] + second[i, p]
            parts[rows_at(i), pl.ds(p * span, span)] = value
            square = value * value
            for c in range(span // LANES):
                total = total + square[:, c * LANES:(c + 1) * LANES]
    me = row * nchan + chan
    squares[pl.ds(me, 1), :] = jnp.sum(total, axis=0, keepdims=True)

    def spread(step):
        other = (me + step) % (nrows * nchan)
        return pltpu.make_async_remote_copy(
            src_ref=squares.at[pl.ds(me, 1)], dst_ref=squares.at[pl.ds(me, 1)], send_sem=square_send.at[step], recv_sem=square_recv.at[step],
            device_id=(other % nchan, other // nchan), device_id_type=MESH)

    def arrived(step):
        other = (me + nrows * nchan - step) % (nrows * nchan)
        return pltpu.make_async_remote_copy(
            src_ref=squares.at[pl.ds(other, 1)], dst_ref=squares.at[pl.ds(other, 1)], send_sem=square_send.at[step], recv_sem=square_recv.at[step],
            device_id=(other % nchan, other // nchan), device_id_type=MESH)

    for step in range(1, nrows * nchan):
        spread(step).start()

    for s in range(2):
        @pl.when(row == roots[s])
        def _(s=s):
            for copy in bulk(s):
                copy.wait_send()
            for n in range(2 * tiles):
                onward_piece(s, n).wait_send()
            couple_copy(s).wait_send()

    @pl.when(is_mid)
    def _():
        for n in range(2):
            relay(crossed(n)).wait_send()

    @pl.when(is_end)
    def _():
        for n in range(nchips):
            relay(streamed(n)).wait_send()

    @pl.when(is_end & leading)
    def _():
        for n in range(tiles):
            fine_copy(n).wait_send()

    @pl.when(is_solver)
    def _():
        for step in range(1, 2 * nchan):
            table_copy(step).wait_send()
        for n in range(1, nchips):
            amp_copy(n).wait_send()

    @pl.when(jnp.logical_not(is_solver))
    def _():
        start_copy(0, row).wait_send()

    for i in range(tiles):
        for p in range(2):
            far(i, p).wait_send()
            mine(i, p).wait_send()
            onward(i, p).wait_send()
    for step in range(1, nrows * nchan):
        arrived(step).wait_recv()
    everything = jnp.sum(jnp.sum(squares[...], axis=0, keepdims=True), axis=1, keepdims=True)
    total_out[...] = jnp.broadcast_to(everything, total_out.shape)
    for step in range(1, nrows * nchan):
        spread(step).wait_send()


def run_cycle(nchan, nrows, positions, residual, psf):
    slab, ncols = residual.shape[1:]
    shard, patch = psf.shape[1:]
    steps, chunks = positions.shape[1], patch // LANES
    nchips, tiles, cols = nrows // 2, slab // 8, ncols // nchan
    rows = slab * (nrows + 2)
    dma, f32, i32 = pltpu.SemaphoreType.DMA, jnp.float32, jnp.int32
    anywhere = pl.BlockSpec(memory_space=pl.ANY)
    vmem = pl.BlockSpec(memory_space=pltpu.VMEM)
    slots = ncols // LANES + 1 + (chunks + 1) * steps
    stage = pltpu.VMEM((tiles, 2, 8, cols // 2), f32)
    small = pltpu.VMEM((8, LANES), f32)
    return pl.pallas_call(
        functools.partial(cycle_kernel, nchan, nrows),
        out_shape=(OUT((slab, ncols), f32), OUT((slab, cols), f32), OUT((8, LANES), f32)),
        in_specs=[pl.BlockSpec(memory_space=pltpu.SMEM), anywhere, anywhere],
        out_specs=(vmem, vmem, vmem),
        scratch_shapes=[
            pltpu.VMEM((tiles, slots, 8, LANES), f32), pltpu.VMEM((rows, patch), f32), pltpu.VMEM((chunks, rows, LANES), f32),
            pltpu.VMEM((chunks, shard, LANES), f32), pltpu.VMEM((steps, 8, LANES), f32), pltpu.VMEM((steps, LANES), f32),
            pltpu.VMEM((steps, LANES), f32), small, pltpu.VMEM((nrows, 8, LANES), f32),
            pltpu.VMEM((2 * nchan, steps + 8, LANES), f32), small, pltpu.VMEM((steps, LANES), i32), pltpu.VMEM((8, LANES), i32),
            stage, stage, stage, stage, pltpu.VMEM((nrows * nchan, LANES), f32),
            pltpu.SMEM((steps, LANES), i32), pltpu.SMEM((8, LANES), i32), pltpu.SMEM((8, LANES), f32),
            pltpu.SemaphoreType.REGULAR, dma((tiles,)), dma((chunks,)), dma((3,)), dma((4 * nchips,)), dma((nchips + 1,)),
            dma((nchips + 1, 2)), dma((nchips + 1,)), dma((2 * tiles,)), dma((2 * tiles,)), dma((2 * tiles,)),
            dma, dma((nrows,)), dma, dma, dma((2 * nchan,)), dma((2 * nchan,)), dma((nchips,)), dma,
        ] + [dma((tiles, 2))] * 6 + [dma((nrows * nchan,))] * 2,
        compiler_params=pltpu.CompilerParams(collective_id=0, has_side_effects=True),
        name="minor_cycle",
    )(positions, residual, psf)


def write_kernel(count, image, parts, total, image_out, normalized, scaled, sems):
    slab, tiles = image.shape[0], image.shape[0] // 8
    copies = [pltpu.make_async_copy(image.at[pl.ds(8 * t, 8)], image_out.at[0, pl.ds(8 * t, 8)], sems.at[t]) for t in range(tiles)]
    for copy in copies:
        copy.start()
    scale = lax.rsqrt(total[0:1, 0:1] / count + 1e-06)
    for t in range(tiles):
        rows = pl.ds(8 * t, 8)
        scaled[rows, :] = parts[rows, :] * scale
        copies.append(pltpu.make_async_copy(scaled.at[rows], normalized.at[rows], sems.at[tiles + t]))
        copies[-1].start()
    for copy in copies:
        copy.wait()


def write_outputs(count, image, parts, total):
    f32 = jnp.float32
    anywhere, vmem = pl.BlockSpec(memory_space=pl.ANY), pl.BlockSpec(memory_space=pltpu.VMEM)
    return pl.pallas_call(
        functools.partial(write_kernel, count),
        out_shape=(jax.ShapeDtypeStruct((1,) + image.shape, f32), jax.ShapeDtypeStruct(parts.shape, f32)),
        in_specs=[vmem, vmem, vmem],
        out_specs=(anywhere, anywhere),
        scratch_shapes=[pltpu.VMEM(parts.shape, f32), pltpu.SemaphoreType.DMA((image.shape[0] // 4,))],
        name="write_outputs",
        compiler_params=pltpu.CompilerParams(vmem_limit_bytes=4 * 2**20),
    )(*(pltpu.with_memory_space_constraint(x, pltpu.VMEM) for x in (image, parts, total)))


def on_device(residual, psf, positions):
    nchan, nrows = lax.axis_size("chan"), lax.axis_size("rows")
    slab, ncols = residual.shape[1:]
    shard, patch = psf.shape[1:]
    steps = positions.shape[0]
    central = slab * nrows == shard and shard * nrows == patch
    powers = all(n & (n - 1) == 0 for n in (slab, shard, patch)) and patch >= LANES
    lines = nchan == 4 and nrows == 8 and slab % 16 == 0 and ncols % (16 * LANES) == 0 and ncols <= LANES * LANES
    if not (central and powers and lines and steps % 8 == 0 and steps <= LANES and patch < LANES * LANES):
        return on_any_device(residual, psf, positions)
    image, parts, total = run_cycle(nchan, nrows, positions.T, residual, psf)
    return write_outputs(slab * nrows * ncols, image, parts, total)


def on_any_device(residual, psf, positions):
    chan_id = lax.axis_index("chan")
    nchan = lax.axis_size("chan")
    row_id = lax.axis_index("rows")
    nrows = lax.axis_size("rows")
    slab = residual.shape[1]
    ncols = residual.shape[2]
    own_psf = psf[0]
    shard_rows = own_psf.shape[0]
    patch = own_psf.shape[1]
    half = patch // 2
    first = row_id * slab
    chan_hot = (jnp.arange(nchan) == chan_id).astype(jnp.float32)
    full_psf = lax.all_gather(own_psf, "rows", axis=0, tiled=True)
    padded_psf = jnp.pad(full_psf, ((slab, slab), (0, 0)))
    zero = jnp.int32(0)

    def subtract(image, row, col, amount):
        offset = first - row + half
        touches = jnp.logical_and(offset > -slab, offset < patch)
        start = jnp.clip(offset + slab, 0, patch + slab)
        psf_rows = lax.dynamic_slice(padded_psf, (start, zero), (slab, patch))
        window = lax.dynamic_slice(image, (zero, col - half), (slab, patch))
        scale = jnp.where(touches, amount, 0.0)
        return lax.dynamic_update_slice(image, window - scale * psf_rows, (zero, col - half))

    image = residual[0]
    peak_rows = positions[:, 0]
    peak_cols = positions[:, 1]
    inside = jnp.logical_and(peak_rows >= first, peak_rows < first + slab)
    local_rows = jnp.clip(peak_rows - first, 0, slab - 1)
    start_values = jnp.where(inside, image[local_rows, peak_cols], 0.0)
    row_offset = peak_rows[:, None] - peak_rows[None, :] + half - row_id * shard_rows
    col_offset = peak_cols[:, None] - peak_cols[None, :] + half
    owned = (row_offset >= 0) & (row_offset < shard_rows) & (col_offset >= 0) & (col_offset < patch)
    couple = own_psf[jnp.clip(row_offset, 0, shard_rows - 1), jnp.clip(col_offset, 0, patch - 1)]
    couple = jnp.where(owned, couple, 0.0)
    start_table, couple_table = lax.psum(
        (chan_hot[:, None] * start_values[None, :], chan_hot[:, None, None] * couple[None, :, :]),
        ("chan", "rows"),
    )

    def solve(k, amps):
        taken = jnp.sum(amps * lax.dynamic_index_in_dim(couple_table, k, 1, False), axis=1)
        value = lax.dynamic_index_in_dim(start_table, k, 1, False) - taken
        amp = 0.25 * (value + jnp.sum(value) / nchan)
        return lax.dynamic_update_index_in_dim(amps, amp, k, 1)

    amps = lax.fori_loop(0, STEPS, solve, jnp.zeros((nchan, STEPS), jnp.float32))
    own_amps = jnp.sum(chan_hot[:, None] * amps, axis=0)

    def apply(k, image):
        return subtract(image, positions[k, 0], positions[k, 1], own_amps[k])

    image = lax.fori_loop(0, STEPS, apply, image)
    count = slab * nrows * ncols
    parts = lax.psum_scatter(image, "chan", scatter_dimension=1, tiled=True)
    total = lax.psum(jnp.sum(parts * parts), ("chan", "rows"))
    normalized = parts * lax.rsqrt(total / count + 1e-06)
    return (image[None], normalized)


def solution(mesh):
    return jax.shard_map(
        on_device,
        mesh=mesh,
        in_specs=(P("chan", "rows", None), P("chan", "rows", None), P()),
        out_specs=(P("chan", "rows", None), P("rows", "chan")),
        check_vma=False,
    )
```

```python
import functools

import jax
import jax.numpy as jnp
from jax import lax
from jax.experimental import pallas as pl
from jax.experimental.pallas import tpu as pltpu
from jax.sharding import PartitionSpec as P

STEPS = 32
LANES = 128
MESH = pl.DeviceIdType.MESH
OUT = pltpu.VMEM


def pick(tile, row, col, lane_to, owned, number, acc):
    moved = pltpu.roll(tile, (lane_to - col) & (LANES - 1), 1)
    target = jnp.where(owned, (row & 7) * LANES + lane_to, -1)
    return jnp.where(number == target, moved, acc)


def cycle_kernel(nchan, nrows, pos, res, psf, image, parts, total_out,
                 work, land, patch_v, psf_v, grid, couple_v, couple_in, start_v, start_in, tables, amps_v, prev_v, last_v,
                 first_far, first_own, passed, second, squares, changes, prev_s, last_s, amps_s,
                 ready, band_sem, psf_sem, index_sem, send_sem, unit_recv, recv_sem, relay_sem, fine_send, fine_recv, fine_relay,
                 start_send, start_recv, couple_send, couple_recv, table_send, table_recv, amp_send, amp_recv,
                 far_send, far_recv, own_send, own_recv, pass_send, pass_recv, square_send, square_recv):
    chan, row = lax.axis_index("chan"), lax.axis_index("rows")
    chip, core = row // 2, row % 2
    partner = row + 1 - 2 * core
    nchips = nrows // 2
    side = chip // (nchips // 2)
    slab, ncols = res.shape[1], res.shape[2]
    shard, patch = psf.shape[1:]
    half, steps, chunks = patch // 2, pos.shape[1], patch // LANES
    unit, tiles, blocks = 2 * slab, slab // 8, ncols // LANES
    base, width = blocks + 1, chunks + 1
    first = row * slab
    roots = (nchips - 1, nchips)
    solvers = (roots[0] ^ 1, roots[1] ^ 1)
    is_root = jnp.logical_or(row == roots[0], row == roots[1])
    is_solver = jnp.logical_or(row == solvers[0], row == solvers[1])
    is_mid = jnp.logical_or(is_root, is_solver)
    is_end = jnp.logical_not(is_mid)
    lane = lax.broadcasted_iota(jnp.int32, (1, LANES), 1)
    lane8 = lax.broadcasted_iota(jnp.int32, (8, LANES), 1)
    number = lax.broadcasted_iota(jnp.int32, (8, LANES), 0) * LANES + lane8
    zero = jnp.zeros((8, LANES), jnp.float32)

    def block_at(index):
        return pl.ds(pl.multiple_of(index * LANES, LANES), LANES)

    bands = [pltpu.make_async_copy(res.at[0, pl.ds(8 * t, 8)], image.at[pl.ds(8 * t, 8)], band_sem.at[t]) for t in range(tiles)]
    for copy in bands:
        copy.start()
    loads = [pltpu.make_async_copy(psf.at[0, :, pl.ds(c * LANES, LANES)], psf_v.at[c], psf_sem.at[c]) for c in range(chunks)]

    barrier = pltpu.get_barrier_semaphore()
    for step in range(1, nrows):
        pl.semaphore_signal(barrier, inc=1, device_id=(chan, (row + step) % nrows), device_id_type=MESH)
    for step in range(1, nchan):
        pl.semaphore_signal(barrier, inc=1, device_id=((chan + step) % nchan, row), device_id_type=MESH)

    @pl.when(is_root)
    def _():
        for copy in loads:
            copy.start()

    begins = [jnp.clip(pos[1, k] - half, 0, ncols - patch) >> 7 for k in range(steps)]
    krow = lax.broadcasted_iota(jnp.int32, (steps, LANES), 0)
    target = jnp.zeros((steps, LANES), jnp.int32)
    for k in range(steps):
        target = jnp.where(krow == k, begins[k], target)
    target = target + lax.broadcasted_iota(jnp.int32, (steps, LANES), 1)
    prev, last = target, lane8
    for k in range(steps):
        inside = target - begins[k]
        prev = jnp.where((inside >= 0) & (inside < width) & (krow > k), inside + (base + width * k), prev)
        inside = lane8 - begins[k]
        last = jnp.where((inside >= 0) & (inside < width), inside + (base + width * k), last)
    prev_v[...] = prev
    last_v[...] = last
    index_copies = [pltpu.make_async_copy(prev_v, prev_s, index_sem.at[0]), pltpu.make_async_copy(last_v, last_s, index_sem.at[1])]
    for copy in index_copies:
        copy.start()
    for t in range(tiles):
        work[t, blocks] = zero
    pl.semaphore_wait(barrier, nrows + nchan - 2)

    def bulk(s):
        mid, end, other = (nchips - 1 + s) // 2, (nchips - 1) * s, nchips // 2 - s
        order = (0, 1) if s == 0 else (1, 0)
        near = list(range(nchips)) if s == 0 else list(range(2 * nchips - 1, nchips - 1, -1))
        across = [nchips - 1 - n if s == 0 else nchips + n for n in range(nchips // 2)]
        local = [u for u in range(mid, mid + nchips + 1) if (u < nchips) == (s == 0)]
        out = []

        def add(u, z, h, rows, to_row, sem):
            out.append(pltpu.make_async_remote_copy(
                src_ref=psf.at[0, pl.ds((u % nchips) * unit + h * slab, rows)], dst_ref=land.at[pl.ds((u - z) * unit + h * slab, rows)],
                send_sem=send_sem.at[len(out)], recv_sem=sem, device_id=(chan, to_row), device_id_type=MESH))

        for u in near:
            for h in order:
                add(u, end, h, slab, 2 * end + (s if u == near[-1] else h), recv_sem.at[u - end, h])
        for u in across:
            for h in range(2):
                add(u, other, h, slab, 2 * other + h, recv_sem.at[u - other, h])
        for u in local:
            add(u, mid, 0, unit, solvers[s], unit_recv.at[u - mid])
        return out

    for s in range(2):
        @pl.when(row == roots[s])
        def _(s=s):
            for copy in bulk(s):
                copy.start()

    for step in range(1, nchan):
        pl.semaphore_signal(ready, inc=1, device_id=((chan + step) % nchan, row), device_id_type=MESH)

    for copy in bands:
        copy.wait()

    def spread_out(b, carry):
        for t in range(tiles):
            work[t, b] = image[pl.ds(8 * t, 8), block_at(b)]
        return carry

    lax.fori_loop(0, blocks, spread_out, 0, unroll=4)
    acc = zero
    for k in range(steps):
        r, c = pos[0, k] - first, pos[1, k]
        tile = work[(r >> 3) & (tiles - 1), c >> 7]
        acc = pick(tile, r, c, k, (r >= 0) & (r < slab), number, acc)
    start_v[...] = acc

    def start_copy(s, source):
        return pltpu.make_async_remote_copy(
            src_ref=start_v, dst_ref=start_in.at[source], send_sem=start_send, recv_sem=start_recv.at[source],
            device_id=(chan, solvers[s]), device_id_type=MESH)

    def couple_copy(s):
        return pltpu.make_async_remote_copy(
            src_ref=couple_v, dst_ref=couple_in, send_sem=couple_send, recv_sem=couple_recv,
            device_id=(chan, solvers[s]), device_id_type=MESH)

    for s in range(2):
        @pl.when((side == s) & (row != solvers[s]))
        def _(s=s):
            start_copy(s, row).start()

    @pl.when(is_root)
    def _():
        for copy in loads:
            copy.wait()
        low = row * shard - half

        def fill(k, carry):
            rk, qk = pos[0, k] - low, pos[1, k] + half

            def test(g, acc):
                for i in range(8):
                    j = g * 8 + i
                    r, c = rk - pos[0, j], qk - pos[1, j]
                    owned = (r >= 0) & (r < shard) & (c >= 0) & (c < patch) & (j < k)
                    tile = psf_v[(c >> 7) & (chunks - 1), pl.ds(((r >> 3) << 3) & (shard - 1), 8), :]
                    acc = pick(tile, r, c, j, owned, number, acc)
                return acc

            grid[k] = lax.fori_loop(0, (k + 7) >> 3, test, zero)
            return carry

        lax.fori_loop(0, steps, fill, 0)
        couple_v[...] = jnp.sum(grid[...], axis=1)

    for s in range(2):
        @pl.when(row == roots[s])
        def _(s=s):
            couple_copy(s).start()

    def held(m, h, rows=slab):
        return land.at[pl.ds(pl.multiple_of(m * unit + h * slab, 8), rows)]

    def relay(m):
        return pltpu.make_async_remote_copy(
            src_ref=held(m, core), dst_ref=held(m, core), send_sem=relay_sem.at[m], recv_sem=recv_sem.at[m, core],
            device_id=(chan, partner), device_id_type=MESH)

    def arrival(m, h):
        return pltpu.make_async_remote_copy(
            src_ref=held(m, h), dst_ref=held(m, h), send_sem=relay_sem.at[m], recv_sem=recv_sem.at[m, h],
            device_id=(chan, partner), device_id_type=MESH)

    def pass_on(m):
        arrival(m, core).wait_recv()
        relay(m).start()

    def crossed(n):
        return jnp.where(side == 0, nchips - 1 + n, 1 - n)

    def streamed(n):
        return jnp.where(side == 0, n, nchips - n)

    def relayout(source, source_row, dest_row, rows):
        def body(g, carry):
            take, put = pl.multiple_of(source_row + 8 * g, 8), pl.multiple_of(dest_row + 8 * g, 8)
            for c in range(chunks):
                tile = source[c, pl.ds(take, 8), :] if len(source.shape) == 3 else source[pl.ds(take, 8), pl.ds(c * LANES, LANES)]
                patch_v[c, pl.ds(put, 8), :] = tile
            return carry

        lax.fori_loop(0, rows // 8, body, 0)

    @pl.when(is_mid)
    def _():
        pass_on(crossed(0))

    pl.semaphore_wait(ready, nchan - 1)
    me_table = 2 * chan + side

    def table_copy(step):
        other = (me_table + step) % (2 * nchan)
        return pltpu.make_async_remote_copy(
            src_ref=tables.at[me_table], dst_ref=tables.at[me_table], send_sem=table_send.at[step], recv_sem=table_recv.at[step],
            device_id=(other // 2, solvers[0] + (other % 2) * (solvers[1] - solvers[0])), device_id_type=MESH)

    def table_arrival(step):
        other = (me_table + 2 * nchan - step) % (2 * nchan)
        return pltpu.make_async_remote_copy(
            src_ref=tables.at[other], dst_ref=tables.at[other], send_sem=table_send.at[step], recv_sem=table_recv.at[step],
            device_id=(other // 2, solvers[0] + (other % 2) * (solvers[1] - solvers[0])), device_id_type=MESH)

    for s in range(2):
        @pl.when(row == solvers[s])
        def _(s=s):
            total = start_v[...]
            for source in range(s * nchips, (s + 1) * nchips):
                if source != solvers[s]:
                    start_copy(s, source).wait_recv()
                    total = total + start_in[source]
            couple_copy(s).wait_recv()
            tables[me_table, pl.ds(0, steps), :] = couple_in[...]
            tables[me_table, pl.ds(steps, 8), :] = jnp.broadcast_to(jnp.sum(total, axis=0, keepdims=True), total.shape)
            for step in range(1, 2 * nchan):
                table_copy(step).start()

    @pl.when(is_mid)
    def _():
        pass_on(crossed(1))

    def amp_copy(n):
        return pltpu.make_async_remote_copy(
            src_ref=amps_v, dst_ref=amps_v, send_sem=amp_send.at[n], recv_sem=amp_recv,
            device_id=(chan, side * nchips + (row + n) % nchips), device_id_type=MESH)

    @pl.when(is_solver)
    def _():
        for step in range(1, 2 * nchan):
            table_arrival(step).wait_recv()

        def rows_of(index):
            return jnp.concatenate([tables[2 * c, pl.ds(index, 1), :] + tables[2 * c + 1, pl.ds(index, 1), :] for c in range(nchan)], axis=0)

        start = rows_of(steps)

        def solve(k, amps):
            value = jnp.sum(jnp.where(lane == k, start, 0.0) - amps * rows_of(k), axis=1, keepdims=True)
            amp = 0.25 * (value + jnp.sum(value, axis=0, keepdims=True) / nchan)
            return jnp.where(lane == k, amp, amps)

        amps = lax.fori_loop(0, steps, solve, jnp.zeros((nchan, LANES), jnp.float32))
        amps_v[pl.ds(0, nchan), :] = amps
        amps_v[pl.ds(nchan, 8 - nchan), :] = jnp.zeros((8 - nchan, LANES), jnp.float32)
        for n in range(1, nchips):
            amp_copy(n).start()

    def fine_piece(n):
        return jnp.where(side == 0, n, 2 * tiles - 1 - n)

    def fine_at(n):
        return pl.multiple_of(jnp.where(side == 0, nchips, 0) * unit + 8 * fine_piece(n), 8)

    def onward_piece(s, n):
        mid, end = (nchips - 1 + s) // 2, (nchips - 1) * s
        u = nchips - s
        j = n if s == 0 else 2 * tiles - 1 - n
        return pltpu.make_async_remote_copy(
            src_ref=land.at[pl.ds((u - mid) * unit + 8 * j, 8)], dst_ref=land.at[pl.ds((u - end) * unit + 8 * j, 8)],
            send_sem=fine_send.at[n], recv_sem=fine_recv.at[n], device_id=(chan, 2 * end + j // tiles), device_id_type=MESH)

    def fine_copy(n):
        return pltpu.make_async_remote_copy(
            src_ref=land.at[pl.ds(fine_at(n), 8)], dst_ref=land.at[pl.ds(fine_at(n), 8)],
            send_sem=fine_relay.at[n], recv_sem=fine_recv.at[n], device_id=(chan, partner), device_id_type=MESH)

    for s in range(2):
        mid = (nchips - 1 + s) // 2
        local = [u for u in range(mid, mid + nchips + 1) if (u < nchips) == (s == 0)]

        @pl.when(row == roots[s])
        def _(s=s, mid=mid, local=local):
            arrival(crossed(0), 1 - core).wait_recv()
            for n in range(2 * tiles):
                onward_piece(s, n).start()
            relayout(psf_v, (local[0] % nchips) * unit, (local[0] - mid) * unit, len(local) * unit)

        @pl.when(row == solvers[s])
        def _(s=s, mid=mid, local=local):
            arrival(crossed(0), 1 - core).wait_recv()
            for u in local:
                pltpu.make_async_remote_copy(
                    src_ref=held(u - mid, 0, unit), dst_ref=held(u - mid, 0, unit), send_sem=send_sem.at[0], recv_sem=unit_recv.at[u - mid],
                    device_id=(chan, partner), device_id_type=MESH).wait_recv()
            relayout(land, (local[0] - mid) * unit, (local[0] - mid) * unit, len(local) * unit)

    @pl.when(is_mid)
    def _():
        arrival(crossed(1), 1 - core).wait_recv()
        begin = jnp.where(side == 0, nchips - 1, 0) * unit
        relayout(land, begin, begin, 2 * unit)

    amps_copy = pltpu.make_async_copy(amps_v, amps_s, index_sem.at[2])
    leading = core == side

    def half_unit(m, h):
        begin = pl.multiple_of(m * unit + h * slab, 8)
        relayout(land, begin, begin, slab)

    def relay_half(m, h):
        return pltpu.make_async_remote_copy(
            src_ref=held(m, h), dst_ref=held(m, h), send_sem=relay_sem.at[nchips + 1 + h], recv_sem=recv_sem.at[m, h],
            device_id=(chan, partner), device_id_type=MESH)

    @pl.when(is_end)
    def _():
        for n in range(nchips - 1):
            pass_on(streamed(n))
            if n > 0:
                arrival(streamed(n - 1), 1 - core).wait_recv()
                for h in range(2):
                    half_unit(streamed(n - 1), h)
        amp_copy(1).wait_recv()
        amps_copy.start()
        arrival(streamed(nchips - 2), 1 - core).wait_recv()
        for h in range(2):
            half_unit(streamed(nchips - 2), h)

    @pl.when(is_end & leading)
    def _():
        for n in range(2):
            h = jnp.where(side == 0, n, 1 - n)
            arrival(streamed(nchips - 1), h).wait_recv()
            relay_half(streamed(nchips - 1), h).start()
            half_unit(streamed(nchips - 1), h)

    @pl.when(is_end & jnp.logical_not(leading))
    def _():
        for n in range(2):
            h = jnp.where(side == 0, n, 1 - n)
            arrival(streamed(nchips - 1), h).wait_recv()
            half_unit(streamed(nchips - 1), h)

    @pl.when(is_root)
    def _():
        amp_copy(1).wait_recv()

    @pl.when(is_mid)
    def _():
        amps_copy.start()

    for copy in index_copies:
        copy.wait()
    amps_copy.wait()

    cols = ncols // nchan
    span = cols // 2
    bits = ((1, 2), (2, 1))
    top = core * slab + slab * nrows

    def flip(bit):
        if bit == 1:
            return chan + 1 - 2 * (chan % 2)
        return (chan + 2) % 4

    diagonal = 3 - chan

    def tile_at(i):
        return jnp.where(side == 0, i, tiles - 1 - i)

    def rows_at(i):
        return pl.ds(pl.multiple_of(8 * tile_at(i), 8), 8)

    def cols_at(c, p):
        return pl.ds(pl.multiple_of(c * cols + p * span, LANES), span)

    def send(i, p, source, dest, send_sem, recv_sem, to):
        return pltpu.make_async_remote_copy(
            src_ref=source, dst_ref=dest.at[i, p], send_sem=send_sem.at[i, p], recv_sem=recv_sem.at[i, p],
            device_id=(to, row), device_id_type=MESH)

    def far(i, p):
        return send(i, p, image.at[rows_at(i), cols_at(diagonal, p)], first_far, far_send, far_recv, flip(bits[p][0]))

    def mine(i, p):
        return send(i, p, image.at[rows_at(i), cols_at(flip(bits[p][0]), p)], first_own, own_send, own_recv, flip(bits[p][0]))

    def onward(i, p):
        return send(i, p, passed.at[i, p], second, pass_send, pass_recv, flip(bits[p][1]))

    def fetch(n):
        fine_copy(n).wait_recv()

    def tick(n):
        @pl.when(is_end & leading)
        def _():
            fetch(n)
            fine_copy(n).start()
            relayout(land, fine_at(n), fine_at(n), 8)

    def late(n):
        @pl.when(is_end & jnp.logical_not(leading))
        def _():
            fetch(n)
            relayout(land, fine_at(n), fine_at(n), 8)

    def scale_and_shift(i):
        lift = top + 8 * tile_at(i)

        def four(g, carry):
            for n in range(4):
                k = 4 * g + n
                amp = amps_s[chan, k]
                begin = lift - pos[0, k]
                shift = (pos[1, k] - half) & (LANES - 1)
                keep = lane8 < shift
                moved = [zero] + [pltpu.roll(patch_v[c, pl.ds(begin, 8), :] * amp, shift, 1) for c in range(chunks)] + [zero]
                for m in range(width):
                    changes[width * k + m] = jnp.where(keep, moved[m], moved[m + 1])
            return carry

        lax.fori_loop(0, steps // 4, four, 0)

    def subtract(i):
        t = tile_at(i)

        def four(g, carry):
            for n in range(4):
                k = 4 * g + n
                after = [work[t, prev_s[k, m]] - changes[width * k + m] for m in range(width)]
                for m in range(width):
                    work[t, base + width * k + m] = after[m]
            return carry

        lax.fori_loop(0, steps // 4, four, 0)

    def finalize(i, c):
        rows = rows_at(i)
        per = cols // LANES

        def body(g, carry):
            for n in range(8):
                b = c * per + g * 8 + n
                image[rows, block_at(b)] = work[tile_at(i), last_s[0, b]]
            return carry

        lax.fori_loop(0, per // 8, body, 0)

    def combine(i):
        for p in range(2):
            far(i, p).wait_recv()
            passed[i, p] = image[rows_at(i), cols_at(flip(bits[p][1]), p)] + first_far[i, p]
            onward(i, p).start()

    for i in range(tiles):
        if i == 0:
            tick(0)
            for n in range(tiles):
                late(n)
        late(tiles + i)
        scale_and_shift(i)
        if i == 0:
            tick(1)
        subtract(i)
        finalize(i, diagonal)
        for p in range(2):
            far(i, p).start()
        if i == 0:
            for n in range(2, tiles):
                tick(n)
        for p in range(2):
            finalize(i, flip(bits[p][0]))
        finalize(i, chan)
        if i == tiles - 1:
            for p in range(2):
                mine(i - 1, p).start()
        if i > 0:
            combine(i - 1)
        if i < tiles - 2:
            for p in range(2):
                mine(i, p).start()
    combine(tiles - 1)
    for p in range(2):
        mine(tiles - 1, p).start()
    total = zero
    for i in range(tiles):
        for p in range(2):
            mine(i, p).wait_recv()
            onward(i, p).wait_recv()
            value = image[rows_at(i), cols_at(chan, p)] + first_own[i, p] + second[i, p]
            parts[rows_at(i), pl.ds(p * span, span)] = value
            square = value * value
            for c in range(span // LANES):
                total = total + square[:, c * LANES:(c + 1) * LANES]
    me = row * nchan + chan
    squares[pl.ds(me, 1), :] = jnp.sum(total, axis=0, keepdims=True)

    def spread(step):
        other = (me + step) % (nrows * nchan)
        return pltpu.make_async_remote_copy(
            src_ref=squares.at[pl.ds(me, 1)], dst_ref=squares.at[pl.ds(me, 1)], send_sem=square_send.at[step], recv_sem=square_recv.at[step],
            device_id=(other % nchan, other // nchan), device_id_type=MESH)

    def arrived(step):
        other = (me + nrows * nchan - step) % (nrows * nchan)
        return pltpu.make_async_remote_copy(
            src_ref=squares.at[pl.ds(other, 1)], dst_ref=squares.at[pl.ds(other, 1)], send_sem=square_send.at[step], recv_sem=square_recv.at[step],
            device_id=(other % nchan, other // nchan), device_id_type=MESH)

    for step in range(1, nrows * nchan):
        spread(step).start()

    for s in range(2):
        @pl.when(row == roots[s])
        def _(s=s):
            for copy in bulk(s):
                copy.wait_send()
            for n in range(2 * tiles):
                onward_piece(s, n).wait_send()
            couple_copy(s).wait_send()

    @pl.when(is_mid)
    def _():
        for n in range(2):
            relay(crossed(n)).wait_send()

    @pl.when(is_end)
    def _():
        for n in range(nchips - 1):
            relay(streamed(n)).wait_send()

    @pl.when(is_end & leading)
    def _():
        for h in range(2):
            relay_half(streamed(nchips - 1), h).wait_send()
        for n in range(tiles):
            fine_copy(n).wait_send()

    @pl.when(is_solver)
    def _():
        for step in range(1, 2 * nchan):
            table_copy(step).wait_send()
        for n in range(1, nchips):
            amp_copy(n).wait_send()

    @pl.when(jnp.logical_not(is_solver))
    def _():
        start_copy(0, row).wait_send()

    for i in range(tiles):
        for p in range(2):
            far(i, p).wait_send()
            mine(i, p).wait_send()
            onward(i, p).wait_send()
    for step in range(1, nrows * nchan):
        arrived(step).wait_recv()
    everything = jnp.sum(jnp.sum(squares[...], axis=0, keepdims=True), axis=1, keepdims=True)
    total_out[...] = jnp.broadcast_to(everything, total_out.shape)
    for step in range(1, nrows * nchan):
        spread(step).wait_send()


def run_cycle(nchan, nrows, positions, residual, psf):
    slab, ncols = residual.shape[1:]
    shard, patch = psf.shape[1:]
    steps, chunks = positions.shape[1], patch // LANES
    nchips, tiles, cols = nrows // 2, slab // 8, ncols // nchan
    rows = slab * (nrows + 2)
    dma, f32, i32 = pltpu.SemaphoreType.DMA, jnp.float32, jnp.int32
    anywhere = pl.BlockSpec(memory_space=pl.ANY)
    vmem = pl.BlockSpec(memory_space=pltpu.VMEM)
    slots = ncols // LANES + 1 + (chunks + 1) * steps
    stage = pltpu.VMEM((tiles, 2, 8, cols // 2), f32)
    small = pltpu.VMEM((8, LANES), f32)
    return pl.pallas_call(
        functools.partial(cycle_kernel, nchan, nrows),
        out_shape=(OUT((slab, ncols), f32), OUT((slab, cols), f32), OUT((8, LANES), f32)),
        in_specs=[pl.BlockSpec(memory_space=pltpu.SMEM), anywhere, anywhere],
        out_specs=(vmem, vmem, vmem),
        scratch_shapes=[
            pltpu.VMEM((tiles, slots, 8, LANES), f32), pltpu.VMEM((rows, patch), f32), pltpu.VMEM((chunks, rows, LANES), f32),
            pltpu.VMEM((chunks, shard, LANES), f32), pltpu.VMEM((steps, 8, LANES), f32), pltpu.VMEM((steps, LANES), f32),
            pltpu.VMEM((steps, LANES), f32), small, pltpu.VMEM((nrows, 8, LANES), f32),
            pltpu.VMEM((2 * nchan, steps + 8, LANES), f32), small, pltpu.VMEM((steps, LANES), i32), pltpu.VMEM((8, LANES), i32),
            stage, stage, stage, stage, pltpu.VMEM((nrows * nchan, LANES), f32), pltpu.VMEM(((chunks + 1) * steps, 8, LANES), f32),
            pltpu.SMEM((steps, LANES), i32), pltpu.SMEM((8, LANES), i32), pltpu.SMEM((8, LANES), f32),
            pltpu.SemaphoreType.REGULAR, dma((tiles,)), dma((chunks,)), dma((3,)), dma((4 * nchips,)), dma((nchips + 1,)),
            dma((nchips + 1, 2)), dma((nchips + 3,)), dma((2 * tiles,)), dma((2 * tiles,)), dma((2 * tiles,)),
            dma, dma((nrows,)), dma, dma, dma((2 * nchan,)), dma((2 * nchan,)), dma((nchips,)), dma,
        ] + [dma((tiles, 2))] * 6 + [dma((nrows * nchan,))] * 2,
        compiler_params=pltpu.CompilerParams(collective_id=0, has_side_effects=True),
        name="minor_cycle",
    )(positions, residual, psf)


def write_kernel(count, image, parts, total, image_out, normalized, scaled, sems):
    slab, tiles = image.shape[0], image.shape[0] // 8
    copies = [pltpu.make_async_copy(image.at[pl.ds(8 * t, 8)], image_out.at[0, pl.ds(8 * t, 8)], sems.at[t]) for t in range(tiles)]
    for copy in copies:
        copy.start()
    scale = lax.rsqrt(total[0:1, 0:1] / count + 1e-06)
    for t in range(tiles):
        rows = pl.ds(8 * t, 8)
        scaled[rows, :] = parts[rows, :] * scale
        copies.append(pltpu.make_async_copy(scaled.at[rows], normalized.at[rows], sems.at[tiles + t]))
        copies[-1].start()
    for copy in copies:
        copy.wait()


def write_outputs(count, image, parts, total):
    f32 = jnp.float32
    anywhere, vmem = pl.BlockSpec(memory_space=pl.ANY), pl.BlockSpec(memory_space=pltpu.VMEM)
    return pl.pallas_call(
        functools.partial(write_kernel, count),
        out_shape=(jax.ShapeDtypeStruct((1,) + image.shape, f32), jax.ShapeDtypeStruct(parts.shape, f32)),
        in_specs=[vmem, vmem, vmem],
        out_specs=(anywhere, anywhere),
        scratch_shapes=[pltpu.VMEM(parts.shape, f32), pltpu.SemaphoreType.DMA((image.shape[0] // 4,))],
        name="write_outputs",
        compiler_params=pltpu.CompilerParams(vmem_limit_bytes=4 * 2**20),
    )(*(pltpu.with_memory_space_constraint(x, pltpu.VMEM) for x in (image, parts, total)))


def on_device(residual, psf, positions):
    nchan, nrows = lax.axis_size("chan"), lax.axis_size("rows")
    slab, ncols = residual.shape[1:]
    shard, patch = psf.shape[1:]
    steps = positions.shape[0]
    central = slab * nrows == shard and shard * nrows == patch
    powers = all(n & (n - 1) == 0 for n in (slab, shard, patch)) and patch >= LANES
    lines = nchan == 4 and nrows == 8 and slab % 16 == 0 and ncols % (16 * LANES) == 0 and ncols <= LANES * LANES
    if not (central and powers and lines and steps % 8 == 0 and steps <= LANES and patch < LANES * LANES):
        return on_any_device(residual, psf, positions)
    image, parts, total = run_cycle(nchan, nrows, positions.T, residual, psf)
    return write_outputs(slab * nrows * ncols, image, parts, total)


def on_any_device(residual, psf, positions):
    chan_id = lax.axis_index("chan")
    nchan = lax.axis_size("chan")
    row_id = lax.axis_index("rows")
    nrows = lax.axis_size("rows")
    slab = residual.shape[1]
    ncols = residual.shape[2]
    own_psf = psf[0]
    shard_rows = own_psf.shape[0]
    patch = own_psf.shape[1]
    half = patch // 2
    first = row_id * slab
    chan_hot = (jnp.arange(nchan) == chan_id).astype(jnp.float32)
    full_psf = lax.all_gather(own_psf, "rows", axis=0, tiled=True)
    padded_psf = jnp.pad(full_psf, ((slab, slab), (0, 0)))
    zero = jnp.int32(0)

    def subtract(image, row, col, amount):
        offset = first - row + half
        touches = jnp.logical_and(offset > -slab, offset < patch)
        start = jnp.clip(offset + slab, 0, patch + slab)
        psf_rows = lax.dynamic_slice(padded_psf, (start, zero), (slab, patch))
        window = lax.dynamic_slice(image, (zero, col - half), (slab, patch))
        scale = jnp.where(touches, amount, 0.0)
        return lax.dynamic_update_slice(image, window - scale * psf_rows, (zero, col - half))

    image = residual[0]
    peak_rows = positions[:, 0]
    peak_cols = positions[:, 1]
    inside = jnp.logical_and(peak_rows >= first, peak_rows < first + slab)
    local_rows = jnp.clip(peak_rows - first, 0, slab - 1)
    start_values = jnp.where(inside, image[local_rows, peak_cols], 0.0)
    row_offset = peak_rows[:, None] - peak_rows[None, :] + half - row_id * shard_rows
    col_offset = peak_cols[:, None] - peak_cols[None, :] + half
    owned = (row_offset >= 0) & (row_offset < shard_rows) & (col_offset >= 0) & (col_offset < patch)
    couple = own_psf[jnp.clip(row_offset, 0, shard_rows - 1), jnp.clip(col_offset, 0, patch - 1)]
    couple = jnp.where(owned, couple, 0.0)
    start_table, couple_table = lax.psum(
        (chan_hot[:, None] * start_values[None, :], chan_hot[:, None, None] * couple[None, :, :]),
        ("chan", "rows"),
    )

    def solve(k, amps):
        taken = jnp.sum(amps * lax.dynamic_index_in_dim(couple_table, k, 1, False), axis=1)
        value = lax.dynamic_index_in_dim(start_table, k, 1, False) - taken
        amp = 0.25 * (value + jnp.sum(value) / nchan)
        return lax.dynamic_update_index_in_dim(amps, amp, k, 1)

    amps = lax.fori_loop(0, STEPS, solve, jnp.zeros((nchan, STEPS), jnp.float32))
    own_amps = jnp.sum(chan_hot[:, None] * amps, axis=0)

    def apply(k, image):
        return subtract(image, positions[k, 0], positions[k, 1], own_amps[k])

    image = lax.fori_loop(0, STEPS, apply, image)
    count = slab * nrows * ncols
    parts = lax.psum_scatter(image, "chan", scatter_dimension=1, tiled=True)
    total = lax.psum(jnp.sum(parts * parts), ("chan", "rows"))
    normalized = parts * lax.rsqrt(total / count + 1e-06)
    return (image[None], normalized)


def solution(mesh):
    return jax.shard_map(
        on_device,
        mesh=mesh,
        in_specs=(P("chan", "rows", None), P("chan", "rows", None), P()),
        out_specs=(P("chan", "rows", None), P("rows", "chan")),
        check_vma=False,
    )
```

```python
import functools

import jax
import jax.numpy as jnp
from jax import lax
from jax.experimental import pallas as pl
from jax.experimental.pallas import tpu as pltpu
from jax.sharding import PartitionSpec as P

STEPS = 32
LANES = 128
MESH = pl.DeviceIdType.MESH
OUT = pltpu.VMEM


def pick(tile, row, col, lane_to, owned, number, acc):
    moved = pltpu.roll(tile, (lane_to - col) & (LANES - 1), 1)
    target = jnp.where(owned, (row & 7) * LANES + lane_to, -1)
    return jnp.where(number == target, moved, acc)


def cycle_kernel(nchan, nrows, pos, res, psf, image, parts, total_out,
                 work, land, patch_v, psf_v, grid, couple_v, couple_in, start_v, start_in, tables, amps_v, prev_v, last_v,
                 first_far, first_own, passed, second, squares, changes, pair_v, sum_v, prev_s, last_s, amps_s, pair_s,
                 ready, band_sem, psf_sem, index_sem, send_sem, unit_recv, recv_sem, relay_sem, fine_send, fine_recv, fine_relay,
                 start_send, start_recv, couple_send, couple_recv, table_send, table_recv, amp_send, amp_recv,
                 far_send, far_recv, own_send, own_recv, pass_send, pass_recv, square_send, square_recv, guest_sem):
    chan, row = lax.axis_index("chan"), lax.axis_index("rows")
    chip, core = row // 2, row % 2
    partner = row + 1 - 2 * core
    nchips = nrows // 2
    side = chip // (nchips // 2)
    slab, ncols = res.shape[1], res.shape[2]
    shard, patch = psf.shape[1:]
    half, steps, chunks = patch // 2, pos.shape[1], patch // LANES
    unit, tiles, blocks = 2 * slab, slab // 8, ncols // LANES
    base, width = blocks + 1, chunks + 1
    first = row * slab
    begins_at = [z - (1 if z == (nchips - 1) // 2 else 0) for z in range(nchips)]
    lead = jnp.where(chip == (nchips - 1) // 2, 1, 0)
    roots = (nchips - 1, nchips)
    solvers = (roots[0] ^ 1, roots[1] ^ 1)
    is_root = jnp.logical_or(row == roots[0], row == roots[1])
    is_solver = jnp.logical_or(row == solvers[0], row == solvers[1])
    is_mid = jnp.logical_or(is_root, is_solver)
    is_end = jnp.logical_not(is_mid)
    lane = lax.broadcasted_iota(jnp.int32, (1, LANES), 1)
    lane8 = lax.broadcasted_iota(jnp.int32, (8, LANES), 1)
    number = lax.broadcasted_iota(jnp.int32, (8, LANES), 0) * LANES + lane8
    zero = jnp.zeros((8, LANES), jnp.float32)

    def block_at(index):
        return pl.ds(pl.multiple_of(index * LANES, LANES), LANES)

    bands = [pltpu.make_async_copy(res.at[0, pl.ds(8 * t, 8)], image.at[pl.ds(8 * t, 8)], band_sem.at[t]) for t in range(tiles)]
    for copy in bands:
        copy.start()
    loads = [pltpu.make_async_copy(psf.at[0, :, pl.ds(c * LANES, LANES)], psf_v.at[c], psf_sem.at[c]) for c in range(chunks)]

    barrier = pltpu.get_barrier_semaphore()
    for step in range(1, nrows):
        pl.semaphore_signal(barrier, inc=1, device_id=(chan, (row + step) % nrows), device_id_type=MESH)
    for step in range(1, nchan):
        pl.semaphore_signal(barrier, inc=1, device_id=((chan + step) % nchan, row), device_id_type=MESH)

    @pl.when(is_root)
    def _():
        for copy in loads:
            copy.start()

    begins = [jnp.clip(pos[1, k] - half, 0, ncols - patch) >> 7 for k in range(steps)]
    krow = lax.broadcasted_iota(jnp.int32, (steps, LANES), 0)
    target = jnp.zeros((steps, LANES), jnp.int32)
    for k in range(steps):
        target = jnp.where(krow == k, begins[k], target)
    target = target + lax.broadcasted_iota(jnp.int32, (steps, LANES), 1)
    prev, last = target, lane8
    for k in range(steps):
        inside = target - begins[k]
        prev = jnp.where((inside >= 0) & (inside < width) & (krow > k), inside + (base + width * k), prev)
        inside = lane8 - begins[k]
        last = jnp.where((inside >= 0) & (inside < width), inside + (base + width * k), last)
    prev_v[...] = prev
    last_v[...] = last
    lane32 = lax.broadcasted_iota(jnp.int32, (steps, LANES), 1)
    rows_from = jnp.zeros((steps, LANES), jnp.int32)
    cols_from = jnp.zeros((steps, LANES), jnp.int32)
    for k in range(steps):
        rows_from = rows_from + jnp.where(krow == k, pos[0, k], 0) - jnp.where(lane32 == k, pos[0, k], 0)
        cols_from = cols_from + jnp.where(krow == k, pos[1, k], 0) - jnp.where(lane32 == k, pos[1, k], 0)
    rows_from = rows_from + half - row * shard
    cols_from = cols_from + half
    owned = (rows_from >= 0) & (rows_from < shard) & (cols_from >= 0) & (cols_from < patch) & (lane32 < krow)
    pair_v[0] = (cols_from >> 7) & (chunks - 1)
    pair_v[1] = ((rows_from >> 3) << 3) & (shard - 1)
    pair_v[2] = (lane32 - cols_from) & (LANES - 1)
    pair_v[3] = jnp.where(owned, (rows_from & 7) * LANES + lane32, -1)
    pair_copy = pltpu.make_async_copy(pair_v, pair_s, index_sem.at[3])

    @pl.when(is_root)
    def _():
        pair_copy.start()

    index_copies = [pltpu.make_async_copy(prev_v, prev_s, index_sem.at[0]), pltpu.make_async_copy(last_v, last_s, index_sem.at[1])]
    for copy in index_copies:
        copy.start()
    for t in range(tiles):
        work[t, blocks] = zero
    pl.semaphore_wait(barrier, nrows + nchan - 2)

    def bulk(s):
        mid, end, other = (nchips - 1 + s) // 2, (nchips - 1) * s, nchips // 2 - s
        order = (0, 1) if s == 0 else (1, 0)
        near = list(range(nchips)) if s == 0 else list(range(2 * nchips - 1, nchips - 1, -1))
        across = [nchips - 1 - n if s == 0 else nchips + n for n in range(nchips // 2)]
        local = range(s * nchips, (s + 1) * nchips)
        out = []

        def add(u, z, h, rows, to_row, sem):
            out.append(pltpu.make_async_remote_copy(
                src_ref=psf.at[0, pl.ds((u % nchips) * unit + h * slab, rows)], dst_ref=land.at[pl.ds((u - begins_at[z]) * unit + h * slab, rows)],
                send_sem=send_sem.at[len(out)], recv_sem=sem, device_id=(chan, to_row), device_id_type=MESH))

        for u in near:
            for h in order:
                add(u, end, h, slab, 2 * end + (s if u == near[-1] else h), recv_sem.at[u - begins_at[end], h])
        for u in across:
            for h in range(2):
                add(u, other, h, slab, 2 * other + h, recv_sem.at[u - begins_at[other], h])
        for u in local:
            add(u, mid, 0, unit, solvers[s], unit_recv.at[u - begins_at[mid]])
        return out

    for s in range(2):
        @pl.when(row == roots[s])
        def _(s=s):
            for copy in bulk(s):
                copy.start()

    helper = row + 2 - 4 * side
    helped = row - 2 + 4 * side

    def tile_at(i):
        return jnp.where(side == 0, i, tiles - 1 - i)

    def tile_rows(t):
        return pl.ds(pl.multiple_of(8 * t, 8), 8)

    lent = pltpu.make_async_remote_copy(
        src_ref=res.at[0, tile_rows(tile_at(tiles - 1))], dst_ref=image.at[pl.ds(slab, 8)], send_sem=guest_sem.at[0], recv_sem=guest_sem.at[1],
        device_id=(chan, helper), device_id_type=MESH)
    given = pltpu.make_async_remote_copy(
        src_ref=parts.at[pl.ds(slab, 8)], dst_ref=parts.at[tile_rows(tile_at(tiles - 1))], send_sem=guest_sem.at[2], recv_sem=guest_sem.at[3],
        device_id=(chan, helped), device_id_type=MESH)

    @pl.when(is_end)
    def _():
        lent.start()

    for step in range(1, nchan):
        pl.semaphore_signal(ready, inc=1, device_id=((chan + step) % nchan, row), device_id_type=MESH)

    for copy in bands:
        copy.wait()

    def spread_out(b, carry):
        for t in range(tiles):
            work[t, b] = image[pl.ds(8 * t, 8), block_at(b)]
        return carry

    lax.fori_loop(0, blocks, spread_out, 0, unroll=4)
    acc = zero
    for k in range(steps):
        r, c = pos[0, k] - first, pos[1, k]
        tile = work[(r >> 3) & (tiles - 1), c >> 7]
        acc = pick(tile, r, c, k, (r >= 0) & (r < slab), number, acc)
    start_v[...] = acc

    def start_copy(s, source):
        return pltpu.make_async_remote_copy(
            src_ref=start_v, dst_ref=start_in.at[source], send_sem=start_send, recv_sem=start_recv.at[source],
            device_id=(chan, solvers[s]), device_id_type=MESH)

    def couple_copy(s):
        return pltpu.make_async_remote_copy(
            src_ref=couple_v, dst_ref=couple_in, send_sem=couple_send, recv_sem=couple_recv,
            device_id=(chan, solvers[s]), device_id_type=MESH)

    for s in range(2):
        @pl.when((side == s) & (row != solvers[s]))
        def _(s=s):
            start_copy(s, row).start()

    @pl.when(is_root)
    def _():
        for copy in loads:
            copy.wait()
        pair_copy.wait()

        def fill(k, carry):
            acc = zero
            for j in range(steps):
                tile = psf_v[pair_s[0, k, j], pl.ds(pair_s[1, k, j], 8), :]
                acc = jnp.where(number == pair_s[3, k, j], pltpu.roll(tile, pair_s[2, k, j], 1), acc)
            grid[k] = acc
            return carry

        lax.fori_loop(0, steps, fill, 0)
        couple_v[...] = jnp.sum(grid[...], axis=1)

    for s in range(2):
        @pl.when(row == roots[s])
        def _(s=s):
            couple_copy(s).start()

    def held(m, h, rows=slab):
        return land.at[pl.ds(pl.multiple_of(m * unit + h * slab, 8), rows)]

    def relay(m):
        return pltpu.make_async_remote_copy(
            src_ref=held(m, core), dst_ref=held(m, core), send_sem=relay_sem.at[m], recv_sem=recv_sem.at[m, core],
            device_id=(chan, partner), device_id_type=MESH)

    def arrival(m, h):
        return pltpu.make_async_remote_copy(
            src_ref=held(m, h), dst_ref=held(m, h), send_sem=relay_sem.at[m], recv_sem=recv_sem.at[m, h],
            device_id=(chan, partner), device_id_type=MESH)

    def pass_on(m):
        arrival(m, core).wait_recv()
        relay(m).start()

    def crossed(n):
        return jnp.where(side == 0, nchips + n, 1 - n)

    def streamed(n):
        return jnp.where(side == 0, n, nchips - n)

    def relayout(source, source_row, dest_row, rows):
        def body(g, carry):
            take, put = pl.multiple_of(source_row + 8 * g, 8), pl.multiple_of(dest_row + 8 * g, 8)
            for c in range(chunks):
                tile = source[c, pl.ds(take, 8), :] if len(source.shape) == 3 else source[pl.ds(take, 8), pl.ds(c * LANES, LANES)]
                patch_v[c, pl.ds(put, 8), :] = tile
            return carry

        lax.fori_loop(0, rows // 8, body, 0)

    @pl.when(is_mid)
    def _():
        pass_on(crossed(0))

    pl.semaphore_wait(ready, nchan - 1)
    me_table = 2 * chan + side

    def table_copy(step):
        other = (me_table + step) % (2 * nchan)
        return pltpu.make_async_remote_copy(
            src_ref=tables.at[me_table], dst_ref=tables.at[me_table], send_sem=table_send.at[step], recv_sem=table_recv.at[step],
            device_id=(other // 2, solvers[0] + (other % 2) * (solvers[1] - solvers[0])), device_id_type=MESH)

    def table_arrival(step):
        other = (me_table + 2 * nchan - step) % (2 * nchan)
        return pltpu.make_async_remote_copy(
            src_ref=tables.at[other], dst_ref=tables.at[other], send_sem=table_send.at[step], recv_sem=table_recv.at[step],
            device_id=(other // 2, solvers[0] + (other % 2) * (solvers[1] - solvers[0])), device_id_type=MESH)

    for s in range(2):
        @pl.when(row == solvers[s])
        def _(s=s):
            total = start_v[...]
            for source in range(s * nchips, (s + 1) * nchips):
                if source != solvers[s]:
                    start_copy(s, source).wait_recv()
                    total = total + start_in[source]
            couple_copy(s).wait_recv()
            tables[me_table, pl.ds(0, steps), :] = couple_in[...]
            tables[me_table, pl.ds(steps, 8), :] = jnp.broadcast_to(jnp.sum(total, axis=0, keepdims=True), total.shape)
            for step in range(1, 2 * nchan):
                table_copy(step).start()

    @pl.when(is_mid)
    def _():
        pass_on(crossed(1))

    def amp_copy(n):
        return pltpu.make_async_remote_copy(
            src_ref=amps_v, dst_ref=amps_v, send_sem=amp_send.at[n], recv_sem=amp_recv,
            device_id=(chan, side * nchips + (row + n) % nchips), device_id_type=MESH)

    @pl.when(is_solver)
    def _():
        for step in range(1, 2 * nchan):
            table_arrival(step).wait_recv()

        def rows_of(index):
            return jnp.concatenate([tables[2 * c, pl.ds(index, 1), :] + tables[2 * c + 1, pl.ds(index, 1), :] for c in range(nchan)], axis=0)

        start = rows_of(steps)

        def solve(k, amps):
            value = jnp.sum(jnp.where(lane == k, start, 0.0) - amps * rows_of(k), axis=1, keepdims=True)
            amp = 0.25 * (value + jnp.sum(value, axis=0, keepdims=True) / nchan)
            return jnp.where(lane == k, amp, amps)

        amps = lax.fori_loop(0, steps, solve, jnp.zeros((nchan, LANES), jnp.float32))
        amps_v[pl.ds(0, nchan), :] = amps
        amps_v[pl.ds(nchan, 8 - nchan), :] = jnp.zeros((8 - nchan, LANES), jnp.float32)
        for n in range(1, nchips):
            amp_copy(n).start()

    def fine_piece(n):
        return jnp.where(side == 0, n, 2 * tiles - 1 - n)

    def fine_at(n):
        return pl.multiple_of(jnp.where(side == 0, nchips, 0) * unit + 8 * fine_piece(n), 8)

    def onward_piece(s, n):
        mid, end = (nchips - 1 + s) // 2, (nchips - 1) * s
        u = nchips - s
        j = n if s == 0 else 2 * tiles - 1 - n
        return pltpu.make_async_remote_copy(
            src_ref=land.at[pl.ds((u - begins_at[mid]) * unit + 8 * j, 8)], dst_ref=land.at[pl.ds((u - begins_at[end]) * unit + 8 * j, 8)],
            send_sem=fine_send.at[n], recv_sem=fine_recv.at[n], device_id=(chan, 2 * end + j // tiles), device_id_type=MESH)

    def fine_copy(n):
        return pltpu.make_async_remote_copy(
            src_ref=land.at[pl.ds(fine_at(n), 8)], dst_ref=land.at[pl.ds(fine_at(n), 8)],
            send_sem=fine_relay.at[n], recv_sem=fine_recv.at[n], device_id=(chan, partner), device_id_type=MESH)

    for s in range(2):
        offset = s * nchips - begins_at[(nchips - 1 + s) // 2]

        @pl.when(row == roots[s])
        def _(s=s, offset=offset):
            arrival(crossed(0), 1 - core).wait_recv()
            for n in range(2 * tiles):
                onward_piece(s, n).start()
            relayout(psf_v, 0, offset * unit, nchips * unit)

        @pl.when(row == solvers[s])
        def _(s=s, offset=offset):
            arrival(crossed(0), 1 - core).wait_recv()
            for u in range(nchips):
                pltpu.make_async_remote_copy(
                    src_ref=held(u + offset, 0, unit), dst_ref=held(u + offset, 0, unit), send_sem=send_sem.at[0], recv_sem=unit_recv.at[u + offset],
                    device_id=(chan, partner), device_id_type=MESH).wait_recv()
            relayout(land, offset * unit, offset * unit, nchips * unit)

    @pl.when(is_mid)
    def _():
        arrival(crossed(1), 1 - core).wait_recv()
        begin = jnp.where(side == 0, nchips, 0) * unit
        relayout(land, begin, begin, 2 * unit)

    amps_copy = pltpu.make_async_copy(amps_v, amps_s, index_sem.at[2])
    leading = core == side

    def half_unit(m, h):
        begin = pl.multiple_of(m * unit + h * slab, 8)
        relayout(land, begin, begin, slab)

    def relay_half(m, h):
        return pltpu.make_async_remote_copy(
            src_ref=held(m, h), dst_ref=held(m, h), send_sem=relay_sem.at[nchips + 2 + h], recv_sem=recv_sem.at[m, h],
            device_id=(chan, partner), device_id_type=MESH)

    @pl.when(is_end)
    def _():
        for n in range(nchips - 1):
            pass_on(streamed(n))
            if n > 0:
                arrival(streamed(n - 1), 1 - core).wait_recv()
                for h in range(2):
                    half_unit(streamed(n - 1), h)
        amp_copy(1).wait_recv()
        amps_copy.start()
        arrival(streamed(nchips - 2), 1 - core).wait_recv()
        for h in range(2):
            half_unit(streamed(nchips - 2), h)

    @pl.when(is_end & leading)
    def _():
        for n in range(2):
            h = jnp.where(side == 0, n, 1 - n)
            arrival(streamed(nchips - 1), h).wait_recv()
            relay_half(streamed(nchips - 1), h).start()
            half_unit(streamed(nchips - 1), h)

    @pl.when(is_end & jnp.logical_not(leading))
    def _():
        for n in range(2):
            h = jnp.where(side == 0, n, 1 - n)
            arrival(streamed(nchips - 1), h).wait_recv()
            half_unit(streamed(nchips - 1), h)

    @pl.when(is_root)
    def _():
        amp_copy(1).wait_recv()

    @pl.when(is_mid)
    def _():
        amps_copy.start()

    for copy in index_copies:
        copy.wait()
    amps_copy.wait()

    cols = ncols // nchan
    span = cols // 2
    bits = ((1, 2), (2, 1))

    def flip(bit):
        if bit == 1:
            return chan + 1 - 2 * (chan % 2)
        return (chan + 2) % 4

    diagonal = 3 - chan

    def tile_of(n):
        if n == 0:
            return tile_at(0)
        return jnp.where(is_mid, tiles if n == 1 else tile_at(n - 1), tile_at(n))

    def rows_at(n):
        return tile_rows(tile_of(n))

    def lift_of(n):
        own_lift = slab * nrows + lead * unit + core * slab + 8 * tile_of(n)
        if n != 1:
            return own_lift
        guest_lift = slab * nrows + side * unit + core * slab + 8 * tile_at(tiles - 1)
        return jnp.where(is_mid, guest_lift, own_lift)

    def cols_at(c, p):
        return pl.ds(pl.multiple_of(c * cols + p * span, LANES), span)

    def send(i, p, source, dest, send_sem, recv_sem, to):
        return pltpu.make_async_remote_copy(
            src_ref=source, dst_ref=dest.at[i, p], send_sem=send_sem.at[i, p], recv_sem=recv_sem.at[i, p],
            device_id=(to, row), device_id_type=MESH)

    def far(i, p):
        return send(i, p, image.at[rows_at(i), cols_at(diagonal, p)], first_far, far_send, far_recv, flip(bits[p][0]))

    def mine(i, p):
        return send(i, p, image.at[rows_at(i), cols_at(flip(bits[p][0]), p)], first_own, own_send, own_recv, flip(bits[p][0]))

    def onward(i, p):
        return send(i, p, passed.at[i, p], second, pass_send, pass_recv, flip(bits[p][1]))

    def fetch(n):
        fine_copy(n).wait_recv()

    def tick(n):
        @pl.when(is_end & leading)
        def _():
            fetch(n)
            fine_copy(n).start()
            relayout(land, fine_at(n), fine_at(n), 8)

    def late(n):
        @pl.when(is_end & jnp.logical_not(leading))
        def _():
            fetch(n)
            relayout(land, fine_at(n), fine_at(n), 8)

    def scale_and_shift(i):
        lift = lift_of(i)

        def eight(g, carry):
            for n in range(8):
                k = 8 * g + n
                amp = amps_s[chan, k]
                begin = lift - pos[0, k]
                shift = (pos[1, k] - half) & (LANES - 1)
                keep = lane8 < shift
                moved = [zero] + [pltpu.roll(patch_v[c, pl.ds(begin, 8), :] * amp, shift, 1) for c in range(chunks)] + [zero]
                for m in range(width):
                    changes[width * k + m] = jnp.where(keep, moved[m], moved[m + 1])
            return carry

        lax.fori_loop(0, steps // 8, eight, 0)

    def subtract(i):
        t = tile_of(i)

        def eight(g, carry):
            for n in range(8):
                k = 8 * g + n
                after = [work[t, prev_s[k, m]] - changes[width * k + m] for m in range(width)]
                for m in range(width):
                    work[t, base + width * k + m] = after[m]
            return carry

        lax.fori_loop(0, steps // 8, eight, 0)

    def finalize(i, c):
        rows = rows_at(i)
        per = cols // LANES

        def body(g, carry):
            for n in range(8):
                b = c * per + g * 8 + n
                image[rows, block_at(b)] = work[tile_of(i), last_s[0, b]]
            return carry

        lax.fori_loop(0, per // 8, body, 0)

    def combine(i):
        for p in range(2):
            far(i, p).wait_recv()
            passed[i, p] = image[rows_at(i), cols_at(flip(bits[p][1]), p)] + first_far[i, p]
            onward(i, p).start()

    def own(n):
        for p in range(2):
            mine(n, p).wait_recv()
            onward(n, p).wait_recv()
            value = image[rows_at(n), cols_at(chan, p)] + first_own[n, p] + second[n, p]
            parts[rows_at(n), pl.ds(p * span, span)] = value
            square = value * value
            total = zero
            for c in range(span // LANES):
                total = total + square[:, c * LANES:(c + 1) * LANES]
            sum_v[...] = sum_v[...] + total

    def start_far(n):
        for p in range(2):
            far(n, p).start()

    def start_mine(n):
        for p in range(2):
            mine(n, p).start()

    def finish(n):
        for p in range(2):
            finalize(n, flip(bits[p][0]))
        finalize(n, chan)

    sum_v[...] = zero
    for n in range(tiles - 1):
        if n == 0:
            tick(0)
            for piece in range(tiles):
                late(piece)
        if n == 1:
            @pl.when(is_mid)
            def _():
                lent.wait_recv()

                def guest(b, carry):
                    work[tiles, b] = image[pl.ds(slab, 8), block_at(b)]
                    return carry

                lax.fori_loop(0, blocks, guest, 0, unroll=4)

        late(tiles + n)
        scale_and_shift(n)
        if n == 0:
            tick(1)
        subtract(n)
        finalize(n, diagonal)
        start_far(n)
        if n == 0:
            for piece in range(2, tiles):
                tick(piece)
        finish(n)
        if n > 0:
            combine(n - 1)
        if n < tiles - 2:
            start_mine(n)

    @pl.when(is_mid)
    def _():
        start_mine(tiles - 2)

    late(2 * tiles - 1)
    scale_and_shift(tiles - 1)

    @pl.when(is_end)
    def _():
        combine(tiles - 2)
        start_mine(tiles - 2)

    subtract(tiles - 1)
    finalize(tiles - 1, diagonal)

    @pl.when(is_mid)
    def _():
        start_far(tiles - 1)

    finish(tiles - 1)

    @pl.when(is_mid)
    def _():
        combine(tiles - 2)
        own(1)
        given.start()
        scale_and_shift(tiles)
        subtract(tiles)
        finalize(tiles, diagonal)
        start_far(tiles)
        finish(tiles)
        start_mine(tiles - 1)
        combine(tiles - 1)
        combine(tiles)
        start_mine(tiles)

    own(0)

    @pl.when(is_end)
    def _():
        own(1)

    own(2)

    @pl.when(is_mid)
    def _():
        own(tiles - 1)
        own(tiles)

    total = sum_v[...]
    me = row * nchan + chan
    squares[pl.ds(me, 1), :] = jnp.sum(total, axis=0, keepdims=True)

    def spread(step):
        other = (me + step) % (nrows * nchan)
        return pltpu.make_async_remote_copy(
            src_ref=squares.at[pl.ds(me, 1)], dst_ref=squares.at[pl.ds(me, 1)], send_sem=square_send.at[step], recv_sem=square_recv.at[step],
            device_id=(other % nchan, other // nchan), device_id_type=MESH)

    def arrived(step):
        other = (me + nrows * nchan - step) % (nrows * nchan)
        return pltpu.make_async_remote_copy(
            src_ref=squares.at[pl.ds(other, 1)], dst_ref=squares.at[pl.ds(other, 1)], send_sem=square_send.at[step], recv_sem=square_recv.at[step],
            device_id=(other % nchan, other // nchan), device_id_type=MESH)

    for step in range(1, nrows * nchan):
        spread(step).start()

    for s in range(2):
        @pl.when(row == roots[s])
        def _(s=s):
            for copy in bulk(s):
                copy.wait_send()
            for n in range(2 * tiles):
                onward_piece(s, n).wait_send()
            couple_copy(s).wait_send()

    @pl.when(is_mid)
    def _():
        for n in range(2):
            relay(crossed(n)).wait_send()

    @pl.when(is_end)
    def _():
        for n in range(nchips - 1):
            relay(streamed(n)).wait_send()

    @pl.when(is_end & leading)
    def _():
        for h in range(2):
            relay_half(streamed(nchips - 1), h).wait_send()
        for n in range(tiles):
            fine_copy(n).wait_send()

    @pl.when(is_solver)
    def _():
        for step in range(1, 2 * nchan):
            table_copy(step).wait_send()
        for n in range(1, nchips):
            amp_copy(n).wait_send()

    @pl.when(jnp.logical_not(is_solver))
    def _():
        start_copy(0, row).wait_send()

    def sent(n):
        for p in range(2):
            far(n, p).wait_send()
            mine(n, p).wait_send()
            onward(n, p).wait_send()

    for n in range(tiles - 1):
        sent(n)

    @pl.when(is_mid)
    def _():
        sent(tiles - 1)
        sent(tiles)
        given.wait_send()

    @pl.when(is_end)
    def _():
        lent.wait_send()
        given.wait_recv()

    for step in range(1, nrows * nchan):
        arrived(step).wait_recv()
    everything = jnp.sum(jnp.sum(squares[...], axis=0, keepdims=True), axis=1, keepdims=True)
    total_out[...] = jnp.broadcast_to(everything, total_out.shape)
    for step in range(1, nrows * nchan):
        spread(step).wait_send()


def run_cycle(nchan, nrows, positions, residual, psf):
    slab, ncols = residual.shape[1:]
    shard, patch = psf.shape[1:]
    steps, chunks = positions.shape[1], patch // LANES
    nchips, tiles, cols = nrows // 2, slab // 8, ncols // nchan
    rows = slab * (nrows + 4)
    dma, f32, i32 = pltpu.SemaphoreType.DMA, jnp.float32, jnp.int32
    anywhere = pl.BlockSpec(memory_space=pl.ANY)
    vmem = pl.BlockSpec(memory_space=pltpu.VMEM)
    slots = ncols // LANES + 1 + (chunks + 1) * steps
    stage = pltpu.VMEM((tiles + 1, 2, 8, cols // 2), f32)
    small = pltpu.VMEM((8, LANES), f32)
    return pl.pallas_call(
        functools.partial(cycle_kernel, nchan, nrows),
        out_shape=(OUT((slab + 8, ncols), f32), OUT((slab + 8, cols), f32), OUT((8, LANES), f32)),
        in_specs=[pl.BlockSpec(memory_space=pltpu.SMEM), anywhere, anywhere],
        out_specs=(vmem, vmem, vmem),
        scratch_shapes=[
            pltpu.VMEM((tiles + 1, slots, 8, LANES), f32), pltpu.VMEM((rows, patch), f32), pltpu.VMEM((chunks, rows, LANES), f32),
            pltpu.VMEM((chunks, shard, LANES), f32), pltpu.VMEM((steps, 8, LANES), f32), pltpu.VMEM((steps, LANES), f32),
            pltpu.VMEM((steps, LANES), f32), small, pltpu.VMEM((nrows, 8, LANES), f32),
            pltpu.VMEM((2 * nchan, steps + 8, LANES), f32), small, pltpu.VMEM((steps, LANES), i32), pltpu.VMEM((8, LANES), i32),
            stage, stage, stage, stage, pltpu.VMEM((nrows * nchan, LANES), f32), pltpu.VMEM(((chunks + 1) * steps, 8, LANES), f32), pltpu.VMEM((4, steps, LANES), i32), small,
            pltpu.SMEM((steps, LANES), i32), pltpu.SMEM((8, LANES), i32), pltpu.SMEM((8, LANES), f32), pltpu.SMEM((4, steps, LANES), i32),
            pltpu.SemaphoreType.REGULAR, dma((tiles,)), dma((chunks,)), dma((4,)), dma((4 * nchips,)), dma((nchips + 2,)),
            dma((nchips + 2, 2)), dma((nchips + 4,)), dma((2 * tiles,)), dma((2 * tiles,)), dma((2 * tiles,)),
            dma, dma((nrows,)), dma, dma, dma((2 * nchan,)), dma((2 * nchan,)), dma((nchips,)), dma,
        ] + [dma((tiles + 1, 2))] * 6 + [dma((nrows * nchan,))] * 2 + [dma((4,))],
        compiler_params=pltpu.CompilerParams(collective_id=0, has_side_effects=True),
        name="minor_cycle",
    )(positions, residual, psf)


def write_kernel(count, image, parts, total, image_out, normalized, scaled, sems):
    slab, tiles = scaled.shape[0], scaled.shape[0] // 8
    copies = [pltpu.make_async_copy(image.at[pl.ds(8 * t, 8)], image_out.at[0, pl.ds(8 * t, 8)], sems.at[t]) for t in range(tiles)]
    for copy in copies:
        copy.start()
    scale = lax.rsqrt(total[0:1, 0:1] / count + 1e-06)
    for t in range(tiles):
        rows = pl.ds(8 * t, 8)
        scaled[rows, :] = parts[rows, :] * scale
        copies.append(pltpu.make_async_copy(scaled.at[rows], normalized.at[rows], sems.at[tiles + t]))
        copies[-1].start()
    for copy in copies:
        copy.wait()


def write_outputs(count, slab, image, parts, total):
    f32, ncols, cols = jnp.float32, image.shape[1], parts.shape[1]
    anywhere, vmem = pl.BlockSpec(memory_space=pl.ANY), pl.BlockSpec(memory_space=pltpu.VMEM)
    return pl.pallas_call(
        functools.partial(write_kernel, count),
        out_shape=(jax.ShapeDtypeStruct((1, slab, ncols), f32), jax.ShapeDtypeStruct((slab, cols), f32)),
        in_specs=[vmem, vmem, vmem],
        out_specs=(anywhere, anywhere),
        scratch_shapes=[pltpu.VMEM((slab, cols), f32), pltpu.SemaphoreType.DMA((slab // 4,))],
        name="write_outputs",
        compiler_params=pltpu.CompilerParams(vmem_limit_bytes=4 * 2**20),
    )(*(pltpu.with_memory_space_constraint(x, pltpu.VMEM) for x in (image, parts, total)))


def on_device(residual, psf, positions):
    nchan, nrows = lax.axis_size("chan"), lax.axis_size("rows")
    slab, ncols = residual.shape[1:]
    shard, patch = psf.shape[1:]
    steps = positions.shape[0]
    central = slab * nrows == shard and shard * nrows == patch
    powers = all(n & (n - 1) == 0 for n in (slab, shard, patch)) and patch >= LANES
    lines = nchan == 4 and nrows == 8 and slab % 16 == 0 and ncols % (16 * LANES) == 0 and ncols <= LANES * LANES
    if not (central and powers and lines and steps % 8 == 0 and steps <= LANES and patch < LANES * LANES):
        return on_any_device(residual, psf, positions)
    image, parts, total = run_cycle(nchan, nrows, positions.T, residual, psf)
    return write_outputs(slab * nrows * ncols, slab, image, parts, total)


def on_any_device(residual, psf, positions):
    chan_id = lax.axis_index("chan")
    nchan = lax.axis_size("chan")
    row_id = lax.axis_index("rows")
    nrows = lax.axis_size("rows")
    slab = residual.shape[1]
    ncols = residual.shape[2]
    own_psf = psf[0]
    shard_rows = own_psf.shape[0]
    patch = own_psf.shape[1]
    half = patch // 2
    first = row_id * slab
    chan_hot = (jnp.arange(nchan) == chan_id).astype(jnp.float32)
    full_psf = lax.all_gather(own_psf, "rows", axis=0, tiled=True)
    padded_psf = jnp.pad(full_psf, ((slab, slab), (0, 0)))
    zero = jnp.int32(0)

    def subtract(image, row, col, amount):
        offset = first - row + half
        touches = jnp.logical_and(offset > -slab, offset < patch)
        start = jnp.clip(offset + slab, 0, patch + slab)
        psf_rows = lax.dynamic_slice(padded_psf, (start, zero), (slab, patch))
        window = lax.dynamic_slice(image, (zero, col - half), (slab, patch))
        scale = jnp.where(touches, amount, 0.0)
        return lax.dynamic_update_slice(image, window - scale * psf_rows, (zero, col - half))

    image = residual[0]
    peak_rows = positions[:, 0]
    peak_cols = positions[:, 1]
    inside = jnp.logical_and(peak_rows >= first, peak_rows < first + slab)
    local_rows = jnp.clip(peak_rows - first, 0, slab - 1)
    start_values = jnp.where(inside, image[local_rows, peak_cols], 0.0)
    row_offset = peak_rows[:, None] - peak_rows[None, :] + half - row_id * shard_rows
    col_offset = peak_cols[:, None] - peak_cols[None, :] + half
    owned = (row_offset >= 0) & (row_offset < shard_rows) & (col_offset >= 0) & (col_offset < patch)
    couple = own_psf[jnp.clip(row_offset, 0, shard_rows - 1), jnp.clip(col_offset, 0, patch - 1)]
    couple = jnp.where(owned, couple, 0.0)
    start_table, couple_table = lax.psum(
        (chan_hot[:, None] * start_values[None, :], chan_hot[:, None, None] * couple[None, :, :]),
        ("chan", "rows"),
    )

    def solve(k, amps):
        taken = jnp.sum(amps * lax.dynamic_index_in_dim(couple_table, k, 1, False), axis=1)
        value = lax.dynamic_index_in_dim(start_table, k, 1, False) - taken
        amp = 0.25 * (value + jnp.sum(value) / nchan)
        return lax.dynamic_update_index_in_dim(amps, amp, k, 1)

    amps = lax.fori_loop(0, STEPS, solve, jnp.zeros((nchan, STEPS), jnp.float32))
    own_amps = jnp.sum(chan_hot[:, None] * amps, axis=0)

    def apply(k, image):
        return subtract(image, positions[k, 0], positions[k, 1], own_amps[k])

    image = lax.fori_loop(0, STEPS, apply, image)
    count = slab * nrows * ncols
    parts = lax.psum_scatter(image, "chan", scatter_dimension=1, tiled=True)
    total = lax.psum(jnp.sum(parts * parts), ("chan", "rows"))
    normalized = parts * lax.rsqrt(total / count + 1e-06)
    return (image[None], normalized)


def solution(mesh):
    return jax.shard_map(
        on_device,
        mesh=mesh,
        in_specs=(P("chan", "rows", None), P("chan", "rows", None), P()),
        out_specs=(P("chan", "rows", None), P("rows", "chan")),
        check_vma=False,
    )
```

```python
import functools

import jax
import jax.numpy as jnp
from jax import lax
from jax.experimental import pallas as pl
from jax.experimental.pallas import tpu as pltpu
from jax.sharding import PartitionSpec as P

STEPS = 32
LANES = 128
MESH = pl.DeviceIdType.MESH
OUT = pltpu.VMEM


def pick(tile, row, col, lane_to, owned, number, acc):
    moved = pltpu.roll(tile, (lane_to - col) & (LANES - 1), 1)
    target = jnp.where(owned, (row & 7) * LANES + lane_to, -1)
    return jnp.where(number == target, moved, acc)


def cycle_kernel(nchan, nrows, pos, res, psf, image, parts, total_out,
                 work, land, patch_v, psf_v, grid, couple_v, couple_in, start_v, start_in, tables, amps_v, prev_v, last_v,
                 first_far, first_own, passed, second, squares, changes, pair_v, sum_v, prev_s, last_s, amps_s, pair_s,
                 ready, band_sem, psf_sem, index_sem, send_sem, unit_recv, recv_sem, relay_sem, fine_send, fine_recv, fine_relay,
                 start_send, start_recv, couple_send, couple_recv, table_send, table_recv, amp_send, amp_recv,
                 far_send, far_recv, own_send, own_recv, pass_send, pass_recv, square_send, square_recv, guest_sem):
    chan, row = lax.axis_index("chan"), lax.axis_index("rows")
    chip, core = row // 2, row % 2
    partner = row + 1 - 2 * core
    nchips = nrows // 2
    side = chip // (nchips // 2)
    slab, ncols = res.shape[1], res.shape[2]
    shard, patch = psf.shape[1:]
    half, steps, chunks = patch // 2, pos.shape[1], patch // LANES
    unit, tiles, blocks = 2 * slab, slab // 8, ncols // LANES
    base, width = blocks + 1, chunks + 1
    first = row * slab
    begins_at = [z - (1 if z == (nchips - 1) // 2 else 0) for z in range(nchips)]
    lead = jnp.where(chip == (nchips - 1) // 2, 1, 0)
    roots = (nchips - 1, nchips)
    solvers = (roots[0] ^ 1, roots[1] ^ 1)
    is_root = jnp.logical_or(row == roots[0], row == roots[1])
    is_solver = jnp.logical_or(row == solvers[0], row == solvers[1])
    is_mid = jnp.logical_or(is_root, is_solver)
    is_end = jnp.logical_not(is_mid)
    lane = lax.broadcasted_iota(jnp.int32, (1, LANES), 1)
    lane8 = lax.broadcasted_iota(jnp.int32, (8, LANES), 1)
    number = lax.broadcasted_iota(jnp.int32, (8, LANES), 0) * LANES + lane8
    zero = jnp.zeros((8, LANES), jnp.float32)

    def block_at(index):
        return pl.ds(pl.multiple_of(index * LANES, LANES), LANES)

    bands = [pltpu.make_async_copy(res.at[0, pl.ds(8 * t, 8)], image.at[pl.ds(8 * t, 8)], band_sem.at[t]) for t in range(tiles)]
    for copy in bands:
        copy.start()
    loads = [pltpu.make_async_copy(psf.at[0, :, pl.ds(c * LANES, LANES)], psf_v.at[pl.ds(c * shard, shard)], psf_sem.at[c]) for c in range(chunks)]

    barrier = pltpu.get_barrier_semaphore()
    for step in range(1, nrows):
        pl.semaphore_signal(barrier, inc=1, device_id=(chan, (row + step) % nrows), device_id_type=MESH)
    for step in range(1, nchan):
        pl.semaphore_signal(barrier, inc=1, device_id=((chan + step) % nchan, row), device_id_type=MESH)

    @pl.when(is_root)
    def _():
        for copy in loads:
            copy.start()

    begins = [jnp.clip(pos[1, k] - half, 0, ncols - patch) >> 7 for k in range(steps)]
    krow = lax.broadcasted_iota(jnp.int32, (steps, LANES), 0)
    target = jnp.zeros((steps, LANES), jnp.int32)
    for k in range(steps):
        target = jnp.where(krow == k, begins[k], target)
    target = target + lax.broadcasted_iota(jnp.int32, (steps, LANES), 1)
    prev, last = target, lane8
    for k in range(steps):
        inside = target - begins[k]
        prev = jnp.where((inside >= 0) & (inside < width) & (krow > k), inside + (base + width * k), prev)
        inside = lane8 - begins[k]
        last = jnp.where((inside >= 0) & (inside < width), inside + (base + width * k), last)
    prev_v[...] = prev
    last_v[...] = last
    lane32 = lax.broadcasted_iota(jnp.int32, (steps, LANES), 1)
    rows_from = jnp.zeros((steps, LANES), jnp.int32)
    cols_from = jnp.zeros((steps, LANES), jnp.int32)
    for k in range(steps):
        rows_from = rows_from + jnp.where(krow == k, pos[0, k], 0) - jnp.where(lane32 == k, pos[0, k], 0)
        cols_from = cols_from + jnp.where(krow == k, pos[1, k], 0) - jnp.where(lane32 == k, pos[1, k], 0)
    rows_from = rows_from + half - row * shard
    cols_from = cols_from + half
    owned = (rows_from >= 0) & (rows_from < shard) & (cols_from >= 0) & (cols_from < patch) & (lane32 < krow)
    pair_v[0] = ((cols_from >> 7) & (chunks - 1)) * shard + (((rows_from >> 3) << 3) & (shard - 1))
    pair_v[1] = (lane32 - cols_from) & (LANES - 1)
    pair_v[2] = jnp.where(owned, (rows_from & 7) * LANES + lane32, -1)
    pair_copy = pltpu.make_async_copy(pair_v, pair_s, index_sem.at[3])

    @pl.when(is_root)
    def _():
        pair_copy.start()

    index_copies = [pltpu.make_async_copy(prev_v, prev_s, index_sem.at[0]), pltpu.make_async_copy(last_v, last_s, index_sem.at[1])]
    for copy in index_copies:
        copy.start()
    for t in range(tiles):
        work[t, blocks] = zero
    pl.semaphore_wait(barrier, nrows + nchan - 2)

    def bulk(s):
        mid, end, other = (nchips - 1 + s) // 2, (nchips - 1) * s, nchips // 2 - s
        order = (0, 1) if s == 0 else (1, 0)
        near = list(range(nchips)) if s == 0 else list(range(2 * nchips - 1, nchips - 1, -1))
        across = [nchips - 1 - n if s == 0 else nchips + n for n in range(nchips // 2)]
        local = range(s * nchips, (s + 1) * nchips)
        out = []

        def add(u, z, h, rows, to_row, sem):
            out.append(pltpu.make_async_remote_copy(
                src_ref=psf.at[0, pl.ds((u % nchips) * unit + h * slab, rows)], dst_ref=land.at[pl.ds((u - begins_at[z]) * unit + h * slab, rows)],
                send_sem=send_sem.at[len(out)], recv_sem=sem, device_id=(chan, to_row), device_id_type=MESH))

        for u in near:
            for h in order:
                add(u, end, h, slab, 2 * end + (s if u == near[-1] else h), recv_sem.at[u - begins_at[end], h])
        for u in across:
            for h in range(2):
                add(u, other, h, slab, 2 * other + h, recv_sem.at[u - begins_at[other], h])
        for u in local:
            add(u, mid, 0, unit, solvers[s], unit_recv.at[u - begins_at[mid]])
        return out

    for s in range(2):
        @pl.when(row == roots[s])
        def _(s=s):
            for copy in bulk(s):
                copy.start()

    trail = 1 - side
    is_lead, is_trail = is_end & (core == side), is_end & (core == trail)
    host = jnp.where(core == side, 0, 1)

    def tile_at(i):
        return jnp.where(side == 0, i, tiles - 1 - i)

    def tile_rows(t):
        return pl.ds(pl.multiple_of(8 * t, 8), 8)

    def lent(g):
        return pltpu.make_async_remote_copy(
            src_ref=res.at[0, tile_rows(tile_at(tiles - 2 + g))], dst_ref=image.at[pl.ds(slab, 8)], send_sem=guest_sem.at[g], recv_sem=guest_sem.at[2],
            device_id=(chan, nchips - 2 + 2 * side + (side if g == 0 else trail)), device_id_type=MESH)

    def given(g):
        return pltpu.make_async_remote_copy(
            src_ref=parts.at[pl.ds(slab, 8)], dst_ref=parts.at[tile_rows(tile_at(tiles - 2 + g))], send_sem=guest_sem.at[3], recv_sem=guest_sem.at[4 + g],
            device_id=(chan, side * (nrows - 2) + trail), device_id_type=MESH)

    for step in range(1, nchan):
        pl.semaphore_signal(ready, inc=1, device_id=((chan + step) % nchan, row), device_id_type=MESH)

    for copy in bands:
        copy.wait()

    def spread_out(b, carry):
        for t in range(tiles):
            work[t, b] = image[pl.ds(8 * t, 8), block_at(b)]
        return carry

    lax.fori_loop(0, blocks, spread_out, 0, unroll=4)
    acc = zero
    for k in range(steps):
        r, c = pos[0, k] - first, pos[1, k]
        tile = work[(r >> 3) & (tiles - 1), c >> 7]
        acc = pick(tile, r, c, k, (r >= 0) & (r < slab), number, acc)
    start_v[...] = acc

    def start_copy(s, source):
        return pltpu.make_async_remote_copy(
            src_ref=start_v, dst_ref=start_in.at[source], send_sem=start_send, recv_sem=start_recv.at[source],
            device_id=(chan, solvers[s]), device_id_type=MESH)

    def couple_copy(s):
        return pltpu.make_async_remote_copy(
            src_ref=couple_v, dst_ref=couple_in, send_sem=couple_send, recv_sem=couple_recv,
            device_id=(chan, solvers[s]), device_id_type=MESH)

    for s in range(2):
        @pl.when((side == s) & (row != solvers[s]))
        def _(s=s):
            start_copy(s, row).start()

    @pl.when(is_trail)
    def _():
        for g in range(2):
            lent(g).start()

    @pl.when(is_root)
    def _():
        for copy in loads:
            copy.wait()
        pair_copy.wait()

        def fill(count, k, carry):
            acc = zero
            for j in range(count):
                tile = psf_v[pl.ds(pair_s[0, k, j], 8), :]
                acc = jnp.where(number == pair_s[2, k, j], pltpu.roll(tile, pair_s[1, k, j], 1), acc)
            grid[k] = acc
            return carry

        for g in range(steps // 8):
            lax.fori_loop(8 * g, 8 * g + 8, functools.partial(fill, 8 * g + 8), 0)
        couple_v[...] = jnp.sum(grid[...], axis=1)

    for s in range(2):
        @pl.when(row == roots[s])
        def _(s=s):
            couple_copy(s).start()

    def held(m, h, rows=slab):
        return land.at[pl.ds(pl.multiple_of(m * unit + h * slab, 8), rows)]

    def relay(m):
        return pltpu.make_async_remote_copy(
            src_ref=held(m, core), dst_ref=held(m, core), send_sem=relay_sem.at[m], recv_sem=recv_sem.at[m, core],
            device_id=(chan, partner), device_id_type=MESH)

    def arrival(m, h):
        return pltpu.make_async_remote_copy(
            src_ref=held(m, h), dst_ref=held(m, h), send_sem=relay_sem.at[m], recv_sem=recv_sem.at[m, h],
            device_id=(chan, partner), device_id_type=MESH)

    def pass_on(m):
        arrival(m, core).wait_recv()
        relay(m).start()

    def crossed(n):
        return jnp.where(side == 0, nchips + n, 1 - n)

    def streamed(n):
        return jnp.where(side == 0, n, nchips - n)

    def relayout(source, source_row, dest_row, rows):
        def body(g, carry):
            take, put = pl.multiple_of(source_row + 8 * g, 8), pl.multiple_of(dest_row + 8 * g, 8)
            for c in range(chunks):
                narrow = source.shape[1] == LANES
                tile = source[pl.ds(pl.multiple_of(c * shard + take, 8), 8), :] if narrow else source[pl.ds(take, 8), pl.ds(c * LANES, LANES)]
                patch_v[c, pl.ds(put, 8), :] = tile
            return carry

        lax.fori_loop(0, rows // 8, body, 0)

    @pl.when(is_root)
    def _():
        pass_on(crossed(0))

    pl.semaphore_wait(ready, nchan - 1)
    me_table = 2 * chan + side

    def table_copy(step):
        other = (me_table + step) % (2 * nchan)
        return pltpu.make_async_remote_copy(
            src_ref=tables.at[me_table], dst_ref=tables.at[me_table], send_sem=table_send.at[step], recv_sem=table_recv.at[step],
            device_id=(other // 2, solvers[0] + (other % 2) * (solvers[1] - solvers[0])), device_id_type=MESH)

    def table_arrival(step):
        other = (me_table + 2 * nchan - step) % (2 * nchan)
        return pltpu.make_async_remote_copy(
            src_ref=tables.at[other], dst_ref=tables.at[other], send_sem=table_send.at[step], recv_sem=table_recv.at[step],
            device_id=(other // 2, solvers[0] + (other % 2) * (solvers[1] - solvers[0])), device_id_type=MESH)

    for s in range(2):
        @pl.when(row == solvers[s])
        def _(s=s):
            total = start_v[...]
            for source in range(s * nchips, (s + 1) * nchips):
                if source != solvers[s]:
                    start_copy(s, source).wait_recv()
                    total = total + start_in[source]
            couple_copy(s).wait_recv()
            tables[me_table, pl.ds(0, steps), :] = couple_in[...]
            tables[me_table, pl.ds(steps, 8), :] = jnp.broadcast_to(jnp.sum(total, axis=0, keepdims=True), total.shape)
            for step in range(1, 2 * nchan):
                table_copy(step).start()
            pass_on(crossed(0))

    @pl.when(is_root)
    def _():
        pass_on(crossed(1))

    def amp_copy(n):
        return pltpu.make_async_remote_copy(
            src_ref=amps_v, dst_ref=amps_v, send_sem=amp_send.at[n], recv_sem=amp_recv,
            device_id=(chan, side * nchips + (row + n) % nchips), device_id_type=MESH)

    @pl.when(is_solver)
    def _():
        for step in range(1, 2 * nchan):
            table_arrival(step).wait_recv()

        def rows_of(index):
            return jnp.concatenate([tables[2 * c, pl.ds(index, 1), :] + tables[2 * c + 1, pl.ds(index, 1), :] for c in range(nchan)], axis=0)

        start = rows_of(steps)

        def solve(k, amps):
            value = jnp.sum(jnp.where(lane == k, start, 0.0) - amps * rows_of(k), axis=1, keepdims=True)
            amp = 0.25 * (value + jnp.sum(value, axis=0, keepdims=True) / nchan)
            return jnp.where(lane == k, amp, amps)

        amps = lax.fori_loop(0, steps, solve, jnp.zeros((nchan, LANES), jnp.float32), unroll=4)
        amps_v[pl.ds(0, nchan), :] = amps
        amps_v[pl.ds(nchan, 8 - nchan), :] = jnp.zeros((8 - nchan, LANES), jnp.float32)
        for n in range(1, nchips):
            amp_copy(n).start()
        pass_on(crossed(1))

    def fine_piece(n):
        return jnp.where(side == 0, n, 2 * tiles - 1 - n)

    def fine_at(n):
        return pl.multiple_of(jnp.where(side == 0, nchips, 0) * unit + 8 * fine_piece(n), 8)

    def onward_piece(s, n):
        mid, end = (nchips - 1 + s) // 2, (nchips - 1) * s
        u = nchips - s
        j = n if s == 0 else 2 * tiles - 1 - n
        return pltpu.make_async_remote_copy(
            src_ref=land.at[pl.ds((u - begins_at[mid]) * unit + 8 * j, 8)], dst_ref=land.at[pl.ds((u - begins_at[end]) * unit + 8 * j, 8)],
            send_sem=fine_send.at[n], recv_sem=fine_recv.at[n], device_id=(chan, 2 * end + j // tiles), device_id_type=MESH)

    def fine_copy(n):
        return pltpu.make_async_remote_copy(
            src_ref=land.at[pl.ds(fine_at(n), 8)], dst_ref=land.at[pl.ds(fine_at(n), 8)],
            send_sem=fine_relay.at[n], recv_sem=fine_recv.at[n], device_id=(chan, partner), device_id_type=MESH)

    for s in range(2):
        offset = s * nchips - begins_at[(nchips - 1 + s) // 2]

        @pl.when(row == roots[s])
        def _(s=s, offset=offset):
            arrival(crossed(0), 1 - core).wait_recv()
            for n in range(2 * tiles):
                onward_piece(s, n).start()
            relayout(psf_v, 0, offset * unit, nchips * unit)

        @pl.when(row == solvers[s])
        def _(s=s, offset=offset):
            arrival(crossed(0), 1 - core).wait_recv()
            for u in range(nchips):
                pltpu.make_async_remote_copy(
                    src_ref=held(u + offset, 0, unit), dst_ref=held(u + offset, 0, unit), send_sem=send_sem.at[0], recv_sem=unit_recv.at[u + offset],
                    device_id=(chan, partner), device_id_type=MESH).wait_recv()
            relayout(land, offset * unit, offset * unit, nchips * unit)

    @pl.when(is_mid)
    def _():
        arrival(crossed(1), 1 - core).wait_recv()
        begin = jnp.where(side == 0, nchips, 0) * unit
        relayout(land, begin, begin, 2 * unit)

    amps_copy = pltpu.make_async_copy(amps_v, amps_s, index_sem.at[2])
    leading = core == side

    def half_unit(m, h):
        begin = pl.multiple_of(m * unit + h * slab, 8)
        relayout(land, begin, begin, slab)

    def relay_half(m, h):
        return pltpu.make_async_remote_copy(
            src_ref=held(m, h), dst_ref=held(m, h), send_sem=relay_sem.at[nchips + 2 + h], recv_sem=recv_sem.at[m, h],
            device_id=(chan, partner), device_id_type=MESH)

    @pl.when(is_end)
    def _():
        for n in range(nchips - 1):
            pass_on(streamed(n))
            if n > 0:
                arrival(streamed(n - 1), 1 - core).wait_recv()
                for h in range(2):
                    half_unit(streamed(n - 1), h)
        amp_copy(1).wait_recv()
        amps_copy.start()
        arrival(streamed(nchips - 2), 1 - core).wait_recv()
        for h in range(2):
            half_unit(streamed(nchips - 2), h)

    @pl.when(is_end & leading)
    def _():
        for n in range(2):
            h = jnp.where(side == 0, n, 1 - n)
            arrival(streamed(nchips - 1), h).wait_recv()
            relay_half(streamed(nchips - 1), h).start()
            half_unit(streamed(nchips - 1), h)

    @pl.when(is_end & jnp.logical_not(leading))
    def _():
        for n in range(2):
            h = jnp.where(side == 0, n, 1 - n)
            arrival(streamed(nchips - 1), h).wait_recv()
            half_unit(streamed(nchips - 1), h)

    @pl.when(is_root)
    def _():
        amp_copy(1).wait_recv()

    @pl.when(is_mid)
    def _():
        amps_copy.start()

    for copy in index_copies:
        copy.wait()
    amps_copy.wait()

    cols = ncols // nchan
    span = cols // 2
    bits = ((1, 2), (2, 1))

    def flip(bit):
        if bit == 1:
            return chan + 1 - 2 * (chan % 2)
        return (chan + 2) % 4

    diagonal = 3 - chan

    def tile_of(n):
        if n == 0:
            return tile_at(0)
        return jnp.where(is_mid, tiles if n == 1 else tile_at(n - 1), tile_at(n))

    def rows_at(n):
        return tile_rows(tile_of(n))

    def lift_of(n):
        own_lift = slab * nrows + lead * unit + core * slab + 8 * tile_of(n)
        if n != 1:
            return own_lift
        guest_lift = slab * nrows + side * unit + trail * slab + 8 * tile_at(tiles - 2 + host)
        return jnp.where(is_mid, guest_lift, own_lift)

    def cols_at(c, p):
        return pl.ds(pl.multiple_of(c * cols + p * span, LANES), span)

    def send(i, p, source, dest, send_sem, recv_sem, to):
        return pltpu.make_async_remote_copy(
            src_ref=source, dst_ref=dest.at[i, p], send_sem=send_sem.at[i, p], recv_sem=recv_sem.at[i, p],
            device_id=(to, row), device_id_type=MESH)

    def far(i, p):
        return send(i, p, image.at[rows_at(i), cols_at(diagonal, p)], first_far, far_send, far_recv, flip(bits[p][0]))

    def mine(i, p):
        return send(i, p, image.at[rows_at(i), cols_at(flip(bits[p][0]), p)], first_own, own_send, own_recv, flip(bits[p][0]))

    def onward(i, p):
        return send(i, p, passed.at[i, p], second, pass_send, pass_recv, flip(bits[p][1]))

    def fetch(n):
        fine_copy(n).wait_recv()

    def tick(n):
        @pl.when(is_end & leading)
        def _():
            fetch(n)
            fine_copy(n).start()
            relayout(land, fine_at(n), fine_at(n), 8)

    def late(n):
        @pl.when(is_end & jnp.logical_not(leading))
        def _():
            fetch(n)
            relayout(land, fine_at(n), fine_at(n), 8)

    def scale_and_shift(i):
        lift = lift_of(i)

        def eight(g, carry):
            for n in range(8):
                k = 8 * g + n
                amp = amps_s[chan, k]
                begin = lift - pos[0, k]
                shift = (pos[1, k] - half) & (LANES - 1)
                keep = lane8 < shift
                moved = [zero] + [pltpu.roll(patch_v[c, pl.ds(begin, 8), :] * amp, shift, 1) for c in range(chunks)] + [zero]
                for m in range(width):
                    changes[width * k + m] = jnp.where(keep, moved[m], moved[m + 1])
            return carry

        lax.fori_loop(0, steps // 8, eight, 0)

    def subtract(i):
        t = tile_of(i)

        def eight(g, carry):
            for n in range(8):
                k = 8 * g + n
                after = [work[t, prev_s[k, m]] - changes[width * k + m] for m in range(width)]
                for m in range(width):
                    work[t, base + width * k + m] = after[m]
            return carry

        lax.fori_loop(0, steps // 8, eight, 0)

    def finalize(i, c):
        rows = rows_at(i)
        per = cols // LANES

        def body(g, carry):
            for n in range(8):
                b = c * per + g * 8 + n
                image[rows, block_at(b)] = work[tile_of(i), last_s[0, b]]
            return carry

        lax.fori_loop(0, per // 8, body, 0)

    def combine(i):
        for p in range(2):
            far(i, p).wait_recv()
            passed[i, p] = image[rows_at(i), cols_at(flip(bits[p][1]), p)] + first_far[i, p]
            onward(i, p).start()

    def own(n):
        for p in range(2):
            mine(n, p).wait_recv()
            onward(n, p).wait_recv()
            value = image[rows_at(n), cols_at(chan, p)] + first_own[n, p] + second[n, p]
            parts[rows_at(n), pl.ds(p * span, span)] = value
            square = value * value
            total = zero
            for c in range(span // LANES):
                total = total + square[:, c * LANES:(c + 1) * LANES]
            sum_v[...] = sum_v[...] + total

    def start_far(n):
        for p in range(2):
            far(n, p).start()

    def start_mine(n):
        for p in range(2):
            mine(n, p).start()

    def finish(n):
        for p in range(2):
            finalize(n, flip(bits[p][0]))
        finalize(n, chan)

    sum_v[...] = zero
    for n in range(2):
        if n == 0:
            tick(0)
            for piece in range(tiles):
                late(piece)
        else:
            @pl.when(is_mid)
            def _():
                lent(0).wait_recv()

                def guest(b, carry):
                    work[tiles, b] = image[pl.ds(slab, 8), block_at(b)]
                    return carry

                lax.fori_loop(0, blocks, guest, 0, unroll=4)

        late(tiles + n)
        scale_and_shift(n)
        if n == 0:
            tick(1)
        subtract(n)
        finalize(n, diagonal)
        start_far(n)
        if n == 0:
            for piece in range(2, tiles):
                tick(piece)
        finish(n)
        if n == 0:
            start_mine(0)
    combine(0)

    @pl.when(jnp.logical_not(is_trail))
    def _():
        start_mine(1)

    late(tiles + 2)
    scale_and_shift(2)

    @pl.when(is_trail)
    def _():
        combine(1)
        start_mine(1)

    subtract(2)
    finalize(2, diagonal)

    @pl.when(jnp.logical_not(is_trail))
    def _():
        start_far(2)

    finish(2)

    @pl.when(jnp.logical_not(is_trail))
    def _():
        combine(1)

    @pl.when(is_mid)
    def _():
        start_mine(2)

    late(tiles + 3)
    scale_and_shift(3)
    subtract(3)
    finalize(3, diagonal)

    @pl.when(jnp.logical_not(is_trail))
    def _():
        start_far(3)

    finish(3)

    @pl.when(is_lead)
    def _():
        start_mine(2)
        combine(2)
        combine(3)
        start_mine(3)

    @pl.when(is_mid)
    def _():
        combine(2)
        own(1)
        given(host).start()
        scale_and_shift(4)
        subtract(4)
        finalize(4, diagonal)
        start_far(4)
        finish(4)
        start_mine(3)
        combine(3)
        combine(4)
        start_mine(4)

    own(0)

    @pl.when(is_end)
    def _():
        own(1)

    @pl.when(jnp.logical_not(is_trail))
    def _():
        own(2)
        own(3)

    @pl.when(is_mid)
    def _():
        own(4)

    total = sum_v[...]
    me = row * nchan + chan
    squares[pl.ds(me, 1), :] = jnp.sum(total, axis=0, keepdims=True)

    def spread(step):
        other = (me + step) % (nrows * nchan)
        return pltpu.make_async_remote_copy(
            src_ref=squares.at[pl.ds(me, 1)], dst_ref=squares.at[pl.ds(me, 1)], send_sem=square_send.at[step], recv_sem=square_recv.at[step],
            device_id=(other % nchan, other // nchan), device_id_type=MESH)

    def arrived(step):
        other = (me + nrows * nchan - step) % (nrows * nchan)
        return pltpu.make_async_remote_copy(
            src_ref=squares.at[pl.ds(other, 1)], dst_ref=squares.at[pl.ds(other, 1)], send_sem=square_send.at[step], recv_sem=square_recv.at[step],
            device_id=(other % nchan, other // nchan), device_id_type=MESH)

    for step in range(1, nrows * nchan):
        spread(step).start()

    for s in range(2):
        @pl.when(row == roots[s])
        def _(s=s):
            for copy in bulk(s):
                copy.wait_send()
            for n in range(2 * tiles):
                onward_piece(s, n).wait_send()
            couple_copy(s).wait_send()

    @pl.when(is_mid)
    def _():
        for n in range(2):
            relay(crossed(n)).wait_send()

    @pl.when(is_end)
    def _():
        for n in range(nchips - 1):
            relay(streamed(n)).wait_send()

    @pl.when(is_end & leading)
    def _():
        for h in range(2):
            relay_half(streamed(nchips - 1), h).wait_send()
        for n in range(tiles):
            fine_copy(n).wait_send()

    @pl.when(is_solver)
    def _():
        for step in range(1, 2 * nchan):
            table_copy(step).wait_send()
        for n in range(1, nchips):
            amp_copy(n).wait_send()

    @pl.when(jnp.logical_not(is_solver))
    def _():
        start_copy(0, row).wait_send()

    def sent(n):
        for p in range(2):
            far(n, p).wait_send()
            mine(n, p).wait_send()
            onward(n, p).wait_send()

    for n in range(2):
        sent(n)

    @pl.when(jnp.logical_not(is_trail))
    def _():
        sent(2)
        sent(3)

    @pl.when(is_mid)
    def _():
        sent(4)
        given(host).wait_send()

    @pl.when(is_trail)
    def _():
        for g in range(2):
            lent(g).wait_send()
            given(g).wait_recv()

    for step in range(1, nrows * nchan):
        arrived(step).wait_recv()
    everything = jnp.sum(jnp.sum(squares[...], axis=0, keepdims=True), axis=1, keepdims=True)
    total_out[...] = jnp.broadcast_to(everything, total_out.shape)
    for step in range(1, nrows * nchan):
        spread(step).wait_send()


def run_cycle(nchan, nrows, positions, residual, psf):
    slab, ncols = residual.shape[1:]
    shard, patch = psf.shape[1:]
    steps, chunks = positions.shape[1], patch // LANES
    nchips, tiles, cols = nrows // 2, slab // 8, ncols // nchan
    rows = slab * (nrows + 4)
    dma, f32, i32 = pltpu.SemaphoreType.DMA, jnp.float32, jnp.int32
    anywhere = pl.BlockSpec(memory_space=pl.ANY)
    vmem = pl.BlockSpec(memory_space=pltpu.VMEM)
    slots = ncols // LANES + 1 + (chunks + 1) * steps
    stage = pltpu.VMEM((tiles + 1, 2, 8, cols // 2), f32)
    small = pltpu.VMEM((8, LANES), f32)
    return pl.pallas_call(
        functools.partial(cycle_kernel, nchan, nrows),
        out_shape=(OUT((slab + 8, ncols), f32), OUT((slab + 8, cols), f32), OUT((8, LANES), f32)),
        in_specs=[pl.BlockSpec(memory_space=pltpu.SMEM), anywhere, anywhere],
        out_specs=(vmem, vmem, vmem),
        scratch_shapes=[
            pltpu.VMEM((tiles + 1, slots, 8, LANES), f32), pltpu.VMEM((rows, patch), f32), pltpu.VMEM((chunks, rows, LANES), f32),
            pltpu.VMEM((chunks * shard, LANES), f32), pltpu.VMEM((steps, 8, LANES), f32), pltpu.VMEM((steps, LANES), f32),
            pltpu.VMEM((steps, LANES), f32), small, pltpu.VMEM((nrows, 8, LANES), f32),
            pltpu.VMEM((2 * nchan, steps + 8, LANES), f32), small, pltpu.VMEM((steps, LANES), i32), pltpu.VMEM((8, LANES), i32),
            stage, stage, stage, stage, pltpu.VMEM((nrows * nchan, LANES), f32), pltpu.VMEM(((chunks + 1) * steps, 8, LANES), f32), pltpu.VMEM((3, steps, LANES), i32), small,
            pltpu.SMEM((steps, LANES), i32), pltpu.SMEM((8, LANES), i32), pltpu.SMEM((8, LANES), f32), pltpu.SMEM((3, steps, LANES), i32),
            pltpu.SemaphoreType.REGULAR, dma((tiles,)), dma((chunks,)), dma((4,)), dma((4 * nchips,)), dma((nchips + 2,)),
            dma((nchips + 2, 2)), dma((nchips + 4,)), dma((2 * tiles,)), dma((2 * tiles,)), dma((2 * tiles,)),
            dma, dma((nrows,)), dma, dma, dma((2 * nchan,)), dma((2 * nchan,)), dma((nchips,)), dma,
        ] + [dma((tiles + 1, 2))] * 6 + [dma((nrows * nchan,))] * 2 + [dma((6,))],
        compiler_params=pltpu.CompilerParams(collective_id=0, has_side_effects=True),
        name="minor_cycle",
    )(positions, residual, psf)


def write_kernel(count, image, parts, total, image_out, normalized, scaled, sems):
    slab, tiles = scaled.shape[0], scaled.shape[0] // 8
    copies = [pltpu.make_async_copy(image.at[pl.ds(8 * t, 8)], image_out.at[0, pl.ds(8 * t, 8)], sems.at[t]) for t in range(tiles)]
    for copy in copies:
        copy.start()
    scale = lax.rsqrt(total[0:1, 0:1] / count + 1e-06)
    for t in range(tiles):
        rows = pl.ds(8 * t, 8)
        scaled[rows, :] = parts[rows, :] * scale
        copies.append(pltpu.make_async_copy(scaled.at[rows], normalized.at[rows], sems.at[tiles + t]))
        copies[-1].start()
    for copy in copies:
        copy.wait()


def write_outputs(count, slab, image, parts, total):
    f32, ncols, cols = jnp.float32, image.shape[1], parts.shape[1]
    anywhere, vmem = pl.BlockSpec(memory_space=pl.ANY), pl.BlockSpec(memory_space=pltpu.VMEM)
    return pl.pallas_call(
        functools.partial(write_kernel, count),
        out_shape=(jax.ShapeDtypeStruct((1, slab, ncols), f32), jax.ShapeDtypeStruct((slab, cols), f32)),
        in_specs=[vmem, vmem, vmem],
        out_specs=(anywhere, anywhere),
        scratch_shapes=[pltpu.VMEM((slab, cols), f32), pltpu.SemaphoreType.DMA((slab // 4,))],
        name="write_outputs",
        compiler_params=pltpu.CompilerParams(vmem_limit_bytes=4 * 2**20),
    )(*(pltpu.with_memory_space_constraint(x, pltpu.VMEM) for x in (image, parts, total)))


def on_device(residual, psf, positions):
    nchan, nrows = lax.axis_size("chan"), lax.axis_size("rows")
    slab, ncols = residual.shape[1:]
    shard, patch = psf.shape[1:]
    steps = positions.shape[0]
    central = slab * nrows == shard and shard * nrows == patch
    powers = all(n & (n - 1) == 0 for n in (slab, shard, patch)) and patch >= LANES
    lines = nchan == 4 and nrows == 8 and slab == 32 and ncols % (16 * LANES) == 0 and ncols <= LANES * LANES
    if not (central and powers and lines and steps % 8 == 0 and steps <= LANES and patch < LANES * LANES):
        return on_any_device(residual, psf, positions)
    image, parts, total = run_cycle(nchan, nrows, positions.T, residual, psf)
    return write_outputs(slab * nrows * ncols, slab, image, parts, total)


def on_any_device(residual, psf, positions):
    chan_id = lax.axis_index("chan")
    nchan = lax.axis_size("chan")
    row_id = lax.axis_index("rows")
    nrows = lax.axis_size("rows")
    slab = residual.shape[1]
    ncols = residual.shape[2]
    own_psf = psf[0]
    shard_rows = own_psf.shape[0]
    patch = own_psf.shape[1]
    half = patch // 2
    first = row_id * slab
    chan_hot = (jnp.arange(nchan) == chan_id).astype(jnp.float32)
    full_psf = lax.all_gather(own_psf, "rows", axis=0, tiled=True)
    padded_psf = jnp.pad(full_psf, ((slab, slab), (0, 0)))
    zero = jnp.int32(0)

    def subtract(image, row, col, amount):
        offset = first - row + half
        touches = jnp.logical_and(offset > -slab, offset < patch)
        start = jnp.clip(offset + slab, 0, patch + slab)
        psf_rows = lax.dynamic_slice(padded_psf, (start, zero), (slab, patch))
        window = lax.dynamic_slice(image, (zero, col - half), (slab, patch))
        scale = jnp.where(touches, amount, 0.0)
        return lax.dynamic_update_slice(image, window - scale * psf_rows, (zero, col - half))

    image = residual[0]
    peak_rows = positions[:, 0]
    peak_cols = positions[:, 1]
    inside = jnp.logical_and(peak_rows >= first, peak_rows < first + slab)
    local_rows = jnp.clip(peak_rows - first, 0, slab - 1)
    start_values = jnp.where(inside, image[local_rows, peak_cols], 0.0)
    row_offset = peak_rows[:, None] - peak_rows[None, :] + half - row_id * shard_rows
    col_offset = peak_cols[:, None] - peak_cols[None, :] + half
    owned = (row_offset >= 0) & (row_offset < shard_rows) & (col_offset >= 0) & (col_offset < patch)
    couple = own_psf[jnp.clip(row_offset, 0, shard_rows - 1), jnp.clip(col_offset, 0, patch - 1)]
    couple = jnp.where(owned, couple, 0.0)
    start_table, couple_table = lax.psum(
        (chan_hot[:, None] * start_values[None, :], chan_hot[:, None, None] * couple[None, :, :]),
        ("chan", "rows"),
    )

    def solve(k, amps):
        taken = jnp.sum(amps * lax.dynamic_index_in_dim(couple_table, k, 1, False), axis=1)
        value = lax.dynamic_index_in_dim(start_table, k, 1, False) - taken
        amp = 0.25 * (value + jnp.sum(value) / nchan)
        return lax.dynamic_update_index_in_dim(amps, amp, k, 1)

    amps = lax.fori_loop(0, STEPS, solve, jnp.zeros((nchan, STEPS), jnp.float32))
    own_amps = jnp.sum(chan_hot[:, None] * amps, axis=0)

    def apply(k, image):
        return subtract(image, positions[k, 0], positions[k, 1], own_amps[k])

    image = lax.fori_loop(0, STEPS, apply, image)
    count = slab * nrows * ncols
    parts = lax.psum_scatter(image, "chan", scatter_dimension=1, tiled=True)
    total = lax.psum(jnp.sum(parts * parts), ("chan", "rows"))
    normalized = parts * lax.rsqrt(total / count + 1e-06)
    return (image[None], normalized)


def solution(mesh):
    return jax.shard_map(
        on_device,
        mesh=mesh,
        in_specs=(P("chan", "rows", None), P("chan", "rows", None), P()),
        out_specs=(P("chan", "rows", None), P("rows", "chan")),
        check_vma=False,
    )
```

```python
import functools

import jax
import jax.numpy as jnp
from jax import lax
from jax.experimental import pallas as pl
from jax.experimental.pallas import tpu as pltpu
from jax.sharding import PartitionSpec as P

STEPS = 32
LANES = 128
MESH = pl.DeviceIdType.MESH
OUT = pltpu.VMEM
VMEM = 67043328


def pick(tile, row, col, lane_to, owned, number, acc):
    moved = pltpu.roll(tile, (lane_to - col) & (LANES - 1), 1)
    target = jnp.where(owned, (row & 7) * LANES + lane_to, -1)
    return jnp.where(number == target, moved, acc)


def cycle_kernel(nchan, nrows, pos, res, psf, image, parts, total_out,
                 work, land, patch_v, psf_v, grid, couple_v, couple_in, start_v, start_in, tables, amps_v, prev_v, last_v,
                 first_far, first_own, passed, second, squares, changes, pair_v, sum_v, prev_s, last_s, amps_s, pair_s,
                 ready, band_sem, psf_sem, index_sem, send_sem, unit_recv, recv_sem, relay_sem, fine_send, fine_recv, fine_relay,
                 start_send, start_recv, couple_send, couple_recv, table_send, table_recv, amp_send, amp_recv,
                 far_send, far_recv, own_send, own_recv, pass_send, pass_recv, square_send, square_recv, guest_sem):
    chan, row = lax.axis_index("chan"), lax.axis_index("rows")
    chip, core = row // 2, row % 2
    partner = row + 1 - 2 * core
    nchips = nrows // 2
    side = chip // (nchips // 2)
    slab, ncols = res.shape[1], res.shape[2]
    shard, patch = psf.shape[1:]
    half, steps, chunks = patch // 2, pos.shape[1], patch // LANES
    unit, tiles, blocks = 2 * slab, slab // 8, ncols // LANES
    base, width = blocks + 1, chunks + 1
    first = row * slab
    begins_at = [z - (1 if z == (nchips - 1) // 2 else 0) for z in range(nchips)]
    lead = jnp.where(chip == (nchips - 1) // 2, 1, 0)
    roots = (nchips - 1, nchips)
    solvers = (roots[0] ^ 1, roots[1] ^ 1)
    is_root = jnp.logical_or(row == roots[0], row == roots[1])
    is_solver = jnp.logical_or(row == solvers[0], row == solvers[1])
    is_mid = jnp.logical_or(is_root, is_solver)
    is_end = jnp.logical_not(is_mid)
    lane = lax.broadcasted_iota(jnp.int32, (1, LANES), 1)
    lane8 = lax.broadcasted_iota(jnp.int32, (8, LANES), 1)
    number = lax.broadcasted_iota(jnp.int32, (8, LANES), 0) * LANES + lane8
    zero = jnp.zeros((8, LANES), jnp.float32)

    def block_at(index):
        return pl.ds(pl.multiple_of(index * LANES, LANES), LANES)

    bands = [pltpu.make_async_copy(res.at[0, pl.ds(8 * t, 8)], image.at[pl.ds(8 * t, 8)], band_sem.at[t]) for t in range(tiles)]
    for copy in bands:
        copy.start()
    loads = [pltpu.make_async_copy(psf.at[0, :, pl.ds(c * LANES, LANES)], psf_v.at[pl.ds(c * shard, shard)], psf_sem.at[c]) for c in range(chunks)]

    barrier = pltpu.get_barrier_semaphore()
    for step in range(1, nrows):
        pl.semaphore_signal(barrier, inc=1, device_id=(chan, (row + step) % nrows), device_id_type=MESH)
    for step in range(1, nchan):
        pl.semaphore_signal(barrier, inc=1, device_id=((chan + step) % nchan, row), device_id_type=MESH)

    @pl.when(is_root)
    def _():
        for copy in loads:
            copy.start()

    begins = [jnp.clip(pos[1, k] - half, 0, ncols - patch) >> 7 for k in range(steps)]
    krow = lax.broadcasted_iota(jnp.int32, (steps, LANES), 0)
    target = jnp.zeros((steps, LANES), jnp.int32)
    for k in range(steps):
        target = jnp.where(krow == k, begins[k], target)
    target = target + lax.broadcasted_iota(jnp.int32, (steps, LANES), 1)
    prev, last = target, lane8
    for k in range(steps):
        inside = target - begins[k]
        prev = jnp.where((inside >= 0) & (inside < width) & (krow > k), inside + (base + width * k), prev)
        inside = lane8 - begins[k]
        last = jnp.where((inside >= 0) & (inside < width), inside + (base + width * k), last)
    prev_v[...] = prev
    last_v[...] = last
    lane32 = lax.broadcasted_iota(jnp.int32, (steps, LANES), 1)
    rows_from = jnp.zeros((steps, LANES), jnp.int32)
    cols_from = jnp.zeros((steps, LANES), jnp.int32)
    for k in range(steps):
        rows_from = rows_from + jnp.where(krow == k, pos[0, k], 0) - jnp.where(lane32 == k, pos[0, k], 0)
        cols_from = cols_from + jnp.where(krow == k, pos[1, k], 0) - jnp.where(lane32 == k, pos[1, k], 0)
    rows_from = rows_from + half - row * shard
    cols_from = cols_from + half
    owned = (rows_from >= 0) & (rows_from < shard) & (cols_from >= 0) & (cols_from < patch) & (lane32 < krow)
    pair_v[0] = ((cols_from >> 7) & (chunks - 1)) * shard + (((rows_from >> 3) << 3) & (shard - 1))
    pair_v[1] = (lane32 - cols_from) & (LANES - 1)
    pair_v[2] = jnp.where(owned, (rows_from & 7) * LANES + lane32, -1)
    pair_copy = pltpu.make_async_copy(pair_v, pair_s, index_sem.at[3])

    @pl.when(is_root)
    def _():
        pair_copy.start()

    index_copies = [pltpu.make_async_copy(prev_v, prev_s, index_sem.at[0]), pltpu.make_async_copy(last_v, last_s, index_sem.at[1])]
    for copy in index_copies:
        copy.start()
    for t in range(tiles):
        work[t, blocks] = zero
    pl.semaphore_wait(barrier, nrows + nchan - 2)

    def bulk(s):
        mid, end, other = (nchips - 1 + s) // 2, (nchips - 1) * s, nchips // 2 - s
        order = (0, 1) if s == 0 else (1, 0)
        near = list(range(nchips)) if s == 0 else list(range(2 * nchips - 1, nchips - 1, -1))
        across = [nchips - 1 - n if s == 0 else nchips + n for n in range(nchips // 2)]
        local = range(s * nchips, (s + 1) * nchips)
        out = []

        def add(u, z, h, rows, to_row, sem):
            out.append(pltpu.make_async_remote_copy(
                src_ref=psf.at[0, pl.ds((u % nchips) * unit + h * slab, rows)], dst_ref=land.at[pl.ds((u - begins_at[z]) * unit + h * slab, rows)],
                send_sem=send_sem.at[len(out)], recv_sem=sem, device_id=(chan, to_row), device_id_type=MESH))

        for u in near:
            for h in order:
                add(u, end, h, slab, 2 * end + (s if u == near[-1] else h), recv_sem.at[u - begins_at[end], h])
        for u in across:
            for h in range(2):
                add(u, other, h, slab, 2 * other + h, recv_sem.at[u - begins_at[other], h])
        for u in local:
            add(u, mid, 0, unit, solvers[s], unit_recv.at[u - begins_at[mid]])
        return out

    for s in range(2):
        @pl.when(row == roots[s])
        def _(s=s):
            for copy in bulk(s):
                copy.start()

    early = core == side
    is_lead, is_trail = is_end & early, is_end & jnp.logical_not(early)
    doubled = is_mid & jnp.logical_not(early)
    sends = jnp.where(is_end, jnp.where(early, tiles - 1, tiles - 2), jnp.where(early, tiles + 1, tiles + 2))
    count = jnp.where(is_end, tiles, sends)

    def tile_at(i):
        return jnp.where(side == 0, i, tiles - 1 - i)

    def tile_rows(t):
        return pl.ds(pl.multiple_of(8 * t, 8), 8)

    def guest_tile(g):
        return tile_at(jnp.where(early, tiles - 1, tiles - 2 + g))

    def lent(g):
        return pltpu.make_async_remote_copy(
            src_ref=res.at[0, tile_rows(guest_tile(g))], dst_ref=image.at[tile_rows(tiles + g)], send_sem=guest_sem.at[g], recv_sem=guest_sem.at[2 + g],
            device_id=(chan, row + 2 - 4 * side), device_id_type=MESH)

    def given(g):
        return pltpu.make_async_remote_copy(
            src_ref=parts.at[tile_rows(tiles + g)], dst_ref=parts.at[tile_rows(guest_tile(g))], send_sem=guest_sem.at[4 + g], recv_sem=guest_sem.at[6 + g],
            device_id=(chan, row - 2 + 4 * side), device_id_type=MESH)

    for step in range(1, nchan):
        pl.semaphore_signal(ready, inc=1, device_id=((chan + step) % nchan, row), device_id_type=MESH)

    for copy in bands:
        copy.wait()

    def spread_out(b, carry):
        for t in range(tiles):
            work[t, b] = image[pl.ds(8 * t, 8), block_at(b)]
        return carry

    lax.fori_loop(0, blocks, spread_out, 0, unroll=4)
    acc = zero
    for k in range(steps):
        r, c = pos[0, k] - first, pos[1, k]
        tile = work[(r >> 3) & (tiles - 1), c >> 7]
        acc = pick(tile, r, c, k, (r >= 0) & (r < slab), number, acc)
    start_v[...] = acc

    def start_copy(s, source):
        return pltpu.make_async_remote_copy(
            src_ref=start_v, dst_ref=start_in.at[source], send_sem=start_send, recv_sem=start_recv.at[source],
            device_id=(chan, solvers[s]), device_id_type=MESH)

    def couple_copy(s):
        return pltpu.make_async_remote_copy(
            src_ref=couple_v, dst_ref=couple_in, send_sem=couple_send, recv_sem=couple_recv,
            device_id=(chan, solvers[s]), device_id_type=MESH)

    for s in range(2):
        @pl.when((side == s) & (row != solvers[s]))
        def _(s=s):
            start_copy(s, row).start()

    @pl.when(is_end)
    def _():
        lent(0).start()

    @pl.when(is_trail)
    def _():
        lent(1).start()

    @pl.when(is_root)
    def _():
        for copy in loads:
            copy.wait()
        pair_copy.wait()

        def fill(count, k, carry):
            acc = zero
            for j in range(count):
                tile = psf_v[pl.ds(pair_s[0, k, j], 8), :]
                acc = jnp.where(number == pair_s[2, k, j], pltpu.roll(tile, pair_s[1, k, j], 1), acc)
            grid[k] = acc
            return carry

        for g in range(steps // 8):
            lax.fori_loop(8 * g, 8 * g + 8, functools.partial(fill, 8 * g + 8), 0)
        couple_v[...] = jnp.sum(grid[...], axis=1)

    for s in range(2):
        @pl.when(row == roots[s])
        def _(s=s):
            couple_copy(s).start()

    def held(m, h, rows=slab):
        return land.at[pl.ds(pl.multiple_of(m * unit + h * slab, 8), rows)]

    def relay(m):
        return pltpu.make_async_remote_copy(
            src_ref=held(m, core), dst_ref=held(m, core), send_sem=relay_sem.at[m], recv_sem=recv_sem.at[m, core],
            device_id=(chan, partner), device_id_type=MESH)

    def arrival(m, h):
        return pltpu.make_async_remote_copy(
            src_ref=held(m, h), dst_ref=held(m, h), send_sem=relay_sem.at[m], recv_sem=recv_sem.at[m, h],
            device_id=(chan, partner), device_id_type=MESH)

    def pass_on(m):
        arrival(m, core).wait_recv()
        relay(m).start()

    def crossed(n):
        return jnp.where(side == 0, nchips + n, 1 - n)

    def streamed(n):
        return jnp.where(side == 0, n, nchips - n)

    def relayout(source, source_row, dest_row, rows):
        def body(g, carry):
            take, put = pl.multiple_of(source_row + 8 * g, 8), pl.multiple_of(dest_row + 8 * g, 8)
            for c in range(chunks):
                narrow = source.shape[1] == LANES
                tile = source[pl.ds(pl.multiple_of(c * shard + take, 8), 8), :] if narrow else source[pl.ds(take, 8), pl.ds(c * LANES, LANES)]
                patch_v[c, pl.ds(put, 8), :] = tile
            return carry

        lax.fori_loop(0, rows // 8, body, 0)

    @pl.when(is_root)
    def _():
        pass_on(crossed(0))

    pl.semaphore_wait(ready, nchan - 1)
    me_table = 2 * chan + side

    def table_copy(step):
        other = (me_table + step) % (2 * nchan)
        return pltpu.make_async_remote_copy(
            src_ref=tables.at[me_table], dst_ref=tables.at[me_table], send_sem=table_send.at[step], recv_sem=table_recv.at[step],
            device_id=(other // 2, solvers[0] + (other % 2) * (solvers[1] - solvers[0])), device_id_type=MESH)

    def table_arrival(step):
        other = (me_table + 2 * nchan - step) % (2 * nchan)
        return pltpu.make_async_remote_copy(
            src_ref=tables.at[other], dst_ref=tables.at[other], send_sem=table_send.at[step], recv_sem=table_recv.at[step],
            device_id=(other // 2, solvers[0] + (other % 2) * (solvers[1] - solvers[0])), device_id_type=MESH)

    for s in range(2):
        @pl.when(row == solvers[s])
        def _(s=s):
            total = start_v[...]
            for source in range(s * nchips, (s + 1) * nchips):
                if source != solvers[s]:
                    start_copy(s, source).wait_recv()
                    total = total + start_in[source]
            couple_copy(s).wait_recv()
            tables[me_table, pl.ds(0, steps), :] = couple_in[...]
            tables[me_table, pl.ds(steps, 8), :] = jnp.broadcast_to(jnp.sum(total, axis=0, keepdims=True), total.shape)
            for step in range(1, 2 * nchan):
                table_copy(step).start()
            pass_on(crossed(0))

    def amp_copy(n):
        return pltpu.make_async_remote_copy(
            src_ref=amps_v, dst_ref=amps_v, send_sem=amp_send.at[n], recv_sem=amp_recv,
            device_id=(chan, side * nchips + (row + n) % nchips), device_id_type=MESH)

    @pl.when(is_solver)
    def _():
        for step in range(1, 2 * nchan):
            table_arrival(step).wait_recv()

        def rows_of(index):
            return jnp.concatenate([tables[2 * c, pl.ds(index, 1), :] + tables[2 * c + 1, pl.ds(index, 1), :] for c in range(nchan)], axis=0)

        start = rows_of(steps)

        def solve(k, amps):
            value = jnp.sum(jnp.where(lane == k, start, 0.0) - amps * rows_of(k), axis=1, keepdims=True)
            amp = 0.25 * (value + jnp.sum(value, axis=0, keepdims=True) / nchan)
            return jnp.where(lane == k, amp, amps)

        amps = lax.fori_loop(0, steps, solve, jnp.zeros((nchan, LANES), jnp.float32), unroll=4)
        amps_v[pl.ds(0, nchan), :] = amps
        amps_v[pl.ds(nchan, 8 - nchan), :] = jnp.zeros((8 - nchan, LANES), jnp.float32)
        for n in range(1, nchips):
            amp_copy(n).start()

    def fine_piece(n):
        return jnp.where(side == 0, n, 2 * tiles - 1 - n)

    def fine_at(n):
        return pl.multiple_of(jnp.where(side == 0, nchips, 0) * unit + 8 * fine_piece(n), 8)

    def onward_piece(s, n):
        mid, end = (nchips - 1 + s) // 2, (nchips - 1) * s
        u = nchips - s
        j = n if s == 0 else 2 * tiles - 1 - n
        return pltpu.make_async_remote_copy(
            src_ref=land.at[pl.ds((u - begins_at[mid]) * unit + 8 * j, 8)], dst_ref=land.at[pl.ds((u - begins_at[end]) * unit + 8 * j, 8)],
            send_sem=fine_send.at[n], recv_sem=fine_recv.at[n], device_id=(chan, 2 * end + j // tiles), device_id_type=MESH)

    def fine_copy(n):
        return pltpu.make_async_remote_copy(
            src_ref=land.at[pl.ds(fine_at(n), 8)], dst_ref=land.at[pl.ds(fine_at(n), 8)],
            send_sem=fine_relay.at[n], recv_sem=fine_recv.at[n], device_id=(chan, partner), device_id_type=MESH)

    for s in range(2):
        offset = s * nchips - begins_at[(nchips - 1 + s) // 2]

        @pl.when(row == roots[s])
        def _(s=s, offset=offset):
            arrival(crossed(0), 1 - core).wait_recv()
            for n in range(2 * tiles):
                onward_piece(s, n).start()
            relayout(psf_v, 0, offset * unit, nchips * unit)

        @pl.when(row == solvers[s])
        def _(s=s, offset=offset):
            arrival(crossed(0), 1 - core).wait_recv()
            for u in range(nchips):
                pltpu.make_async_remote_copy(
                    src_ref=held(u + offset, 0, unit), dst_ref=held(u + offset, 0, unit), send_sem=send_sem.at[0], recv_sem=unit_recv.at[u + offset],
                    device_id=(chan, partner), device_id_type=MESH).wait_recv()
            relayout(land, offset * unit, offset * unit, nchips * unit)

    def relayout_crossed(n):
        begin = pl.multiple_of(crossed(n) * unit, 8)
        relayout(land, begin, begin, unit)

    @pl.when(is_mid)
    def _():
        relayout_crossed(0)

    amps_copy = pltpu.make_async_copy(amps_v, amps_s, index_sem.at[2])
    leading = early

    def half_unit(m, h):
        begin = pl.multiple_of(m * unit + h * slab, 8)
        relayout(land, begin, begin, slab)

    def relay_half(m, h):
        return pltpu.make_async_remote_copy(
            src_ref=held(m, h), dst_ref=held(m, h), send_sem=relay_sem.at[nchips + 2 + h], recv_sem=recv_sem.at[m, h],
            device_id=(chan, partner), device_id_type=MESH)

    @pl.when(is_end)
    def _():
        for n in range(nchips - 1):
            pass_on(streamed(n))
            if n > 0:
                arrival(streamed(n - 1), 1 - core).wait_recv()
                for h in range(2):
                    half_unit(streamed(n - 1), h)
        amp_copy(1).wait_recv()
        amps_copy.start()
        arrival(streamed(nchips - 2), 1 - core).wait_recv()
        for h in range(2):
            half_unit(streamed(nchips - 2), h)

    @pl.when(is_end & leading)
    def _():
        for n in range(2):
            h = jnp.where(side == 0, n, 1 - n)
            arrival(streamed(nchips - 1), h).wait_recv()
            relay_half(streamed(nchips - 1), h).start()
            half_unit(streamed(nchips - 1), h)

    @pl.when(is_end & jnp.logical_not(leading))
    def _():
        for n in range(2):
            h = jnp.where(side == 0, n, 1 - n)
            arrival(streamed(nchips - 1), h).wait_recv()
            half_unit(streamed(nchips - 1), h)

    @pl.when(is_root)
    def _():
        amp_copy(1).wait_recv()

    @pl.when(is_mid)
    def _():
        amps_copy.start()

    for copy in index_copies:
        copy.wait()
    amps_copy.wait()

    cols = ncols // nchan
    span = cols // 2
    bits = ((1, 2), (2, 1))

    def flip(bit):
        if bit == 1:
            return chan + 1 - 2 * (chan % 2)
        return (chan + 2) % 4

    diagonal = 3 - chan

    def is_guest(n):
        return (n == 0) | (doubled & (n == 2))

    def own_index(n):
        return jnp.where(is_mid, n - 1 - jnp.where(doubled & (n > 2), 1, 0), n)

    def tile_of(n):
        return jnp.where(is_mid & is_guest(n), tiles + n // 2, tile_at(own_index(n)))

    def rows_at(n):
        return tile_rows(tile_of(n))

    def lift_of(n):
        own_lift = lead * unit + 8 * tile_at(own_index(n))
        guest_lift = side * unit + 8 * guest_tile(n // 2)
        return slab * nrows + core * slab + jnp.where(is_mid & is_guest(n), guest_lift, own_lift)

    def cols_at(c, p):
        return pl.ds(pl.multiple_of(c * cols + p * span, LANES), span)

    def send(i, p, source, dest, send_sem, recv_sem, to):
        return pltpu.make_async_remote_copy(
            src_ref=source, dst_ref=dest.at[i, p], send_sem=send_sem.at[i, p], recv_sem=recv_sem.at[i, p],
            device_id=(to, row), device_id_type=MESH)

    def far(i, p):
        return send(i, p, image.at[rows_at(i), cols_at(diagonal, p)], first_far, far_send, far_recv, flip(bits[p][0]))

    def mine(i, p):
        return send(i, p, image.at[rows_at(i), cols_at(flip(bits[p][0]), p)], first_own, own_send, own_recv, flip(bits[p][0]))

    def onward(i, p):
        return send(i, p, passed.at[i, p], second, pass_send, pass_recv, flip(bits[p][1]))

    def fetch(n):
        fine_copy(n).wait_recv()

    def tick(n):
        @pl.when(is_end & leading)
        def _():
            fetch(n)
            fine_copy(n).start()
            relayout(land, fine_at(n), fine_at(n), 8)

    def late(n):
        @pl.when(is_end & jnp.logical_not(leading))
        def _():
            fetch(n)
            relayout(land, fine_at(n), fine_at(n), 8)

    def scale_and_shift(i):
        lift = lift_of(i)

        def eight(g, carry):
            for n in range(8):
                k = 8 * g + n
                amp = amps_s[chan, k]
                begin = lift - pos[0, k]
                shift = (pos[1, k] - half) & (LANES - 1)
                keep = lane8 < shift
                moved = [zero] + [pltpu.roll(patch_v[c, pl.ds(begin, 8), :] * amp, shift, 1) for c in range(chunks)] + [zero]
                for m in range(width):
                    changes[width * k + m] = jnp.where(keep, moved[m], moved[m + 1])
            return carry

        lax.fori_loop(0, steps // 8, eight, 0)

    def subtract(i):
        t = tile_of(i)

        def eight(g, carry):
            for n in range(8):
                k = 8 * g + n
                after = [work[t, prev_s[k, m]] - changes[width * k + m] for m in range(width)]
                for m in range(width):
                    work[t, base + width * k + m] = after[m]
            return carry

        lax.fori_loop(0, steps // 8, eight, 0)

    def finalize(i, c):
        rows = rows_at(i)
        per = cols // LANES

        def body(g, carry):
            for n in range(8):
                b = c * per + g * 8 + n
                image[rows, block_at(b)] = work[tile_of(i), last_s[0, b]]
            return carry

        lax.fori_loop(0, per // 8, body, 0)

    def combine(i):
        for p in range(2):
            far(i, p).wait_recv()
            passed[i, p] = image[rows_at(i), cols_at(flip(bits[p][1]), p)] + first_far[i, p]
            onward(i, p).start()

    def own(n):
        for p in range(2):
            mine(n, p).wait_recv()
            onward(n, p).wait_recv()
            value = image[rows_at(n), cols_at(chan, p)] + first_own[n, p] + second[n, p]
            parts[rows_at(n), pl.ds(p * span, span)] = value
            square = value * value
            total = zero
            for c in range(span // LANES):
                total = total + square[:, c * LANES:(c + 1) * LANES]
            sum_v[...] = sum_v[...] + total

    def start_far(n):
        for p in range(2):
            far(n, p).start()

    def start_mine(n):
        for p in range(2):
            mine(n, p).start()

    def finish(n):
        for p in range(2):
            finalize(n, flip(bits[p][0]))
        finalize(n, chan)

    sum_v[...] = zero

    def advance(n, carry):
        active = n < count

        @pl.when(n == 0)
        def _():
            tick(0)
            for piece in range(tiles):
                late(piece)

        @pl.when(is_trail & active)
        def _():
            late(tiles + n)

        @pl.when(is_mid & is_guest(n))
        def _():
            lent(n // 2).wait_recv()

            def guest(b, carry):
                work[tiles + n // 2, b] = image[tile_rows(tiles + n // 2), block_at(b)]
                return carry

            lax.fori_loop(0, blocks, guest, 0, unroll=4)

        @pl.when(is_mid & (n == 1))
        def _():
            arrival(crossed(1), 1 - core).wait_recv()
            relayout_crossed(1)

        @pl.when(active)
        def _():
            scale_and_shift(n)

        @pl.when(n == 0)
        def _():
            tick(1)

        @pl.when(is_mid & (n == 0))
        def _():
            pass_on(crossed(1))

        @pl.when(n == sends)
        def _():
            combine(n - 1)
            start_mine(n - 1)

        @pl.when(active)
        def _():
            subtract(n)
            finalize(n, diagonal)

        @pl.when(n < sends)
        def _():
            start_far(n)

        @pl.when(n == 0)
        def _():
            for piece in range(2, tiles):
                tick(piece)

        @pl.when(active)
        def _():
            finish(n)

        @pl.when((n == sends - 1) & (n > 1))
        def _():
            start_mine(n - 1)

        @pl.when((n > 0) & (n < sends))
        def _():
            combine(n - 1)

        @pl.when((n == 0) | (n < sends - 2))
        def _():
            start_mine(n)

        @pl.when(is_mid & (n == 3))
        def _():
            own(0)
            given(0).start()

        @pl.when(doubled & (n == 5))
        def _():
            own(2)
            given(1).start()

        return carry

    lax.fori_loop(0, tiles + 3, advance, 0)

    def settle(n, carry):
        @pl.when((n < sends) & jnp.logical_not(is_mid & is_guest(n)))
        def _():
            own(n)

        return carry

    lax.fori_loop(0, tiles + 2, settle, 0)
    total = sum_v[...]
    me = row * nchan + chan
    squares[pl.ds(me, 1), :] = jnp.sum(total, axis=0, keepdims=True)

    def spread(step):
        other = (me + step) % (nrows * nchan)
        return pltpu.make_async_remote_copy(
            src_ref=squares.at[pl.ds(me, 1)], dst_ref=squares.at[pl.ds(me, 1)], send_sem=square_send.at[step], recv_sem=square_recv.at[step],
            device_id=(other % nchan, other // nchan), device_id_type=MESH)

    def arrived(step):
        other = (me + nrows * nchan - step) % (nrows * nchan)
        return pltpu.make_async_remote_copy(
            src_ref=squares.at[pl.ds(other, 1)], dst_ref=squares.at[pl.ds(other, 1)], send_sem=square_send.at[step], recv_sem=square_recv.at[step],
            device_id=(other % nchan, other // nchan), device_id_type=MESH)

    for step in range(1, nrows * nchan):
        spread(step).start()

    for s in range(2):
        @pl.when(row == roots[s])
        def _(s=s):
            for copy in bulk(s):
                copy.wait_send()
            for n in range(2 * tiles):
                onward_piece(s, n).wait_send()
            couple_copy(s).wait_send()

    @pl.when(is_mid)
    def _():
        for n in range(2):
            relay(crossed(n)).wait_send()

    @pl.when(is_end)
    def _():
        for n in range(nchips - 1):
            relay(streamed(n)).wait_send()

    @pl.when(is_end & leading)
    def _():
        for h in range(2):
            relay_half(streamed(nchips - 1), h).wait_send()
        for n in range(tiles):
            fine_copy(n).wait_send()

    @pl.when(is_solver)
    def _():
        for step in range(1, 2 * nchan):
            table_copy(step).wait_send()
        for n in range(1, nchips):
            amp_copy(n).wait_send()

    @pl.when(jnp.logical_not(is_solver))
    def _():
        start_copy(0, row).wait_send()

    def sent(n, carry):
        @pl.when(n < sends)
        def _():
            for p in range(2):
                far(n, p).wait_send()
                mine(n, p).wait_send()
                onward(n, p).wait_send()

        return carry

    lax.fori_loop(0, tiles + 2, sent, 0)

    @pl.when(is_mid)
    def _():
        given(0).wait_send()

    @pl.when(doubled)
    def _():
        given(1).wait_send()

    @pl.when(is_end)
    def _():
        lent(0).wait_send()
        given(0).wait_recv()

    @pl.when(is_trail)
    def _():
        lent(1).wait_send()
        given(1).wait_recv()

    for step in range(1, nrows * nchan):
        arrived(step).wait_recv()
    everything = jnp.sum(jnp.sum(squares[...], axis=0, keepdims=True), axis=1, keepdims=True)
    total_out[...] = jnp.broadcast_to(everything, total_out.shape)
    for step in range(1, nrows * nchan):
        spread(step).wait_send()


def run_cycle(nchan, nrows, positions, residual, psf):
    slab, ncols = residual.shape[1:]
    shard, patch = psf.shape[1:]
    steps, chunks = positions.shape[1], patch // LANES
    nchips, tiles, cols = nrows // 2, slab // 8, ncols // nchan
    rows = slab * (nrows + 4)
    dma, f32, i32 = pltpu.SemaphoreType.DMA, jnp.float32, jnp.int32
    anywhere = pl.BlockSpec(memory_space=pl.ANY)
    vmem = pl.BlockSpec(memory_space=pltpu.VMEM)
    slots = ncols // LANES + 1 + (chunks + 1) * steps
    stage = pltpu.VMEM((tiles + 2, 2, 8, cols // 2), f32)
    small = pltpu.VMEM((8, LANES), f32)
    return pl.pallas_call(
        functools.partial(cycle_kernel, nchan, nrows),
        out_shape=(OUT((slab + 16, ncols), f32), OUT((slab + 16, cols), f32), OUT((8, LANES), f32)),
        in_specs=[pl.BlockSpec(memory_space=pltpu.SMEM), anywhere, anywhere],
        out_specs=(vmem, vmem, vmem),
        scratch_shapes=[
            pltpu.VMEM((tiles + 2, slots, 8, LANES), f32), pltpu.VMEM((rows, patch), f32), pltpu.VMEM((chunks, rows, LANES), f32),
            pltpu.VMEM((chunks * shard, LANES), f32), pltpu.VMEM((steps, 8, LANES), f32), pltpu.VMEM((steps, LANES), f32),
            pltpu.VMEM((steps, LANES), f32), small, pltpu.VMEM((nrows, 8, LANES), f32),
            pltpu.VMEM((2 * nchan, steps + 8, LANES), f32), small, pltpu.VMEM((steps, LANES), i32), pltpu.VMEM((8, LANES), i32),
            stage, stage, stage, stage, pltpu.VMEM((nrows * nchan, LANES), f32), pltpu.VMEM(((chunks + 1) * steps, 8, LANES), f32), pltpu.VMEM((3, steps, LANES), i32), small,
            pltpu.SMEM((steps, LANES), i32), pltpu.SMEM((8, LANES), i32), pltpu.SMEM((8, LANES), f32), pltpu.SMEM((3, steps, LANES), i32),
            pltpu.SemaphoreType.REGULAR, dma((tiles,)), dma((chunks,)), dma((4,)), dma((4 * nchips,)), dma((nchips + 2,)),
            dma((nchips + 2, 2)), dma((nchips + 4,)), dma((2 * tiles,)), dma((2 * tiles,)), dma((2 * tiles,)),
            dma, dma((nrows,)), dma, dma, dma((2 * nchan,)), dma((2 * nchan,)), dma((nchips,)), dma,
        ] + [dma((tiles + 2, 2))] * 6 + [dma((nrows * nchan,))] * 2 + [dma((8,))],
        compiler_params=pltpu.CompilerParams(collective_id=0, has_side_effects=True, vmem_limit_bytes=VMEM - 4 * ((slab + 16) * (ncols + cols) + 8 * LANES)),
        name="minor_cycle",
    )(positions, residual, psf)


def write_kernel(count, image, parts, total, image_out, normalized, scaled, sems):
    slab, tiles = scaled.shape[0], scaled.shape[0] // 8
    copies = [pltpu.make_async_copy(image.at[pl.ds(8 * t, 8)], image_out.at[0, pl.ds(8 * t, 8)], sems.at[t]) for t in range(tiles)]
    for copy in copies:
        copy.start()
    scale = lax.rsqrt(total[0:1, 0:1] / count + 1e-06)
    for t in range(tiles):
        rows = pl.ds(8 * t, 8)
        scaled[rows, :] = parts[rows, :] * scale
        copies.append(pltpu.make_async_copy(scaled.at[rows], normalized.at[rows], sems.at[tiles + t]))
        copies[-1].start()
    for copy in copies:
        copy.wait()


def write_outputs(count, slab, image, parts, total):
    f32, ncols, cols = jnp.float32, image.shape[1], parts.shape[1]
    anywhere, vmem = pl.BlockSpec(memory_space=pl.ANY), pl.BlockSpec(memory_space=pltpu.VMEM)
    return pl.pallas_call(
        functools.partial(write_kernel, count),
        out_shape=(jax.ShapeDtypeStruct((1, slab, ncols), f32), jax.ShapeDtypeStruct((slab, cols), f32)),
        in_specs=[vmem, vmem, vmem],
        out_specs=(anywhere, anywhere),
        scratch_shapes=[pltpu.VMEM((slab, cols), f32), pltpu.SemaphoreType.DMA((slab // 4,))],
        name="write_outputs",
        compiler_params=pltpu.CompilerParams(vmem_limit_bytes=4 * 2**20),
    )(*(pltpu.with_memory_space_constraint(x, pltpu.VMEM) for x in (image, parts, total)))


def on_device(residual, psf, positions):
    nchan, nrows = lax.axis_size("chan"), lax.axis_size("rows")
    slab, ncols = residual.shape[1:]
    shard, patch = psf.shape[1:]
    steps = positions.shape[0]
    central = slab * nrows == shard and shard * nrows == patch
    powers = all(n & (n - 1) == 0 for n in (slab, shard, patch)) and patch >= LANES
    lines = nchan == 4 and nrows == 8 and slab == 32 and ncols % (16 * LANES) == 0 and ncols <= LANES * LANES
    if not (central and powers and lines and steps % 8 == 0 and steps <= LANES and patch < LANES * LANES):
        return on_any_device(residual, psf, positions)
    image, parts, total = run_cycle(nchan, nrows, positions.T, residual, psf)
    return write_outputs(slab * nrows * ncols, slab, image, parts, total)


def on_any_device(residual, psf, positions):
    chan_id = lax.axis_index("chan")
    nchan = lax.axis_size("chan")
    row_id = lax.axis_index("rows")
    nrows = lax.axis_size("rows")
    slab = residual.shape[1]
    ncols = residual.shape[2]
    own_psf = psf[0]
    shard_rows = own_psf.shape[0]
    patch = own_psf.shape[1]
    half = patch // 2
    first = row_id * slab
    chan_hot = (jnp.arange(nchan) == chan_id).astype(jnp.float32)
    full_psf = lax.all_gather(own_psf, "rows", axis=0, tiled=True)
    padded_psf = jnp.pad(full_psf, ((slab, slab), (0, 0)))
    zero = jnp.int32(0)

    def subtract(image, row, col, amount):
        offset = first - row + half
        touches = jnp.logical_and(offset > -slab, offset < patch)
        start = jnp.clip(offset + slab, 0, patch + slab)
        psf_rows = lax.dynamic_slice(padded_psf, (start, zero), (slab, patch))
        window = lax.dynamic_slice(image, (zero, col - half), (slab, patch))
        scale = jnp.where(touches, amount, 0.0)
        return lax.dynamic_update_slice(image, window - scale * psf_rows, (zero, col - half))

    image = residual[0]
    peak_rows = positions[:, 0]
    peak_cols = positions[:, 1]
    inside = jnp.logical_and(peak_rows >= first, peak_rows < first + slab)
    local_rows = jnp.clip(peak_rows - first, 0, slab - 1)
    start_values = jnp.where(inside, image[local_rows, peak_cols], 0.0)
    row_offset = peak_rows[:, None] - peak_rows[None, :] + half - row_id * shard_rows
    col_offset = peak_cols[:, None] - peak_cols[None, :] + half
    owned = (row_offset >= 0) & (row_offset < shard_rows) & (col_offset >= 0) & (col_offset < patch)
    couple = own_psf[jnp.clip(row_offset, 0, shard_rows - 1), jnp.clip(col_offset, 0, patch - 1)]
    couple = jnp.where(owned, couple, 0.0)
    start_table, couple_table = lax.psum(
        (chan_hot[:, None] * start_values[None, :], chan_hot[:, None, None] * couple[None, :, :]),
        ("chan", "rows"),
    )

    def solve(k, amps):
        taken = jnp.sum(amps * lax.dynamic_index_in_dim(couple_table, k, 1, False), axis=1)
        value = lax.dynamic_index_in_dim(start_table, k, 1, False) - taken
        amp = 0.25 * (value + jnp.sum(value) / nchan)
        return lax.dynamic_update_index_in_dim(amps, amp, k, 1)

    amps = lax.fori_loop(0, STEPS, solve, jnp.zeros((nchan, STEPS), jnp.float32))
    own_amps = jnp.sum(chan_hot[:, None] * amps, axis=0)

    def apply(k, image):
        return subtract(image, positions[k, 0], positions[k, 1], own_amps[k])

    image = lax.fori_loop(0, STEPS, apply, image)
    count = slab * nrows * ncols
    parts = lax.psum_scatter(image, "chan", scatter_dimension=1, tiled=True)
    total = lax.psum(jnp.sum(parts * parts), ("chan", "rows"))
    normalized = parts * lax.rsqrt(total / count + 1e-06)
    return (image[None], normalized)


def solution(mesh):
    return jax.shard_map(
        on_device,
        mesh=mesh,
        in_specs=(P("chan", "rows", None), P("chan", "rows", None), P()),
        out_specs=(P("chan", "rows", None), P("rows", "chan")),
        check_vma=False,
    )
```

```python
import functools

import jax
import jax.numpy as jnp
from jax import lax
from jax.experimental import pallas as pl
from jax.experimental.pallas import tpu as pltpu
from jax.sharding import PartitionSpec as P

STEPS = 32
LANES = 128
MESH = pl.DeviceIdType.MESH
OUT = pltpu.VMEM
VMEM = 67043328


def pick(tile, row, col, lane_to, owned, number, acc):
    moved = pltpu.roll(tile, (lane_to - col) & (LANES - 1), 1)
    target = jnp.where(owned, (row & 7) * LANES + lane_to, -1)
    return jnp.where(number == target, moved, acc)


def cycle_kernel(nchan, nrows, pos, res, psf, image, parts, total_out,
                 work, land, patch_v, psf_v, grid, couple_v, couple_in, start_v, start_in, tables, amps_v, prev_v, last_v,
                 first_far, first_own, passed, second, squares, changes, pair_v, sum_v, prev_s, last_s, amps_s, pair_s,
                 ready, band_sem, psf_sem, index_sem, send_sem, unit_recv, recv_sem, relay_sem, fine_send, fine_recv, fine_relay,
                 start_send, start_recv, couple_send, couple_recv, table_send, table_recv, amp_send, amp_recv,
                 far_send, far_recv, own_send, own_recv, pass_send, pass_recv, square_send, square_recv, guest_sem):
    chan, row = lax.axis_index("chan"), lax.axis_index("rows")
    chip, core = row // 2, row % 2
    partner = row + 1 - 2 * core
    nchips = nrows // 2
    side = chip // (nchips // 2)
    slab, ncols = res.shape[1], res.shape[2]
    shard, patch = psf.shape[1:]
    half, steps, chunks = patch // 2, pos.shape[1], patch // LANES
    unit, tiles, blocks = 2 * slab, slab // 8, ncols // LANES
    base, width = blocks + 1, chunks + 1
    first = row * slab
    begins_at = [z - (1 if z == (nchips - 1) // 2 else 0) for z in range(nchips)]
    lead = jnp.where(chip == (nchips - 1) // 2, 1, 0)
    roots = (nchips - 1, nchips)
    solvers = (roots[0] ^ 1, roots[1] ^ 1)
    is_root = jnp.logical_or(row == roots[0], row == roots[1])
    is_solver = jnp.logical_or(row == solvers[0], row == solvers[1])
    is_mid = jnp.logical_or(is_root, is_solver)
    is_end = jnp.logical_not(is_mid)
    lane = lax.broadcasted_iota(jnp.int32, (1, LANES), 1)
    lane8 = lax.broadcasted_iota(jnp.int32, (8, LANES), 1)
    number = lax.broadcasted_iota(jnp.int32, (8, LANES), 0) * LANES + lane8
    zero = jnp.zeros((8, LANES), jnp.float32)

    def block_at(index):
        return pl.ds(pl.multiple_of(index * LANES, LANES), LANES)

    def flip(bit):
        if bit == 1:
            return chan + 1 - 2 * (chan % 2)
        return (chan + 2) % 4

    barrier = pltpu.get_barrier_semaphore()
    for bit in (1, 2):
        pl.semaphore_signal(barrier, inc=1, device_id=(flip(bit), row), device_id_type=MESH)
    pl.semaphore_signal(barrier, inc=1, device_id=(chan, partner), device_id_type=MESH)

    @pl.when(chip > 0)
    def _():
        for c in range(2):
            pl.semaphore_signal(barrier, inc=1, device_id=(chan, 2 * chip - 2 + c), device_id_type=MESH)

    @pl.when(chip < nchips - 1)
    def _():
        for c in range(2):
            pl.semaphore_signal(barrier, inc=1, device_id=(chan, 2 * chip + 2 + c), device_id_type=MESH)

    bands = [pltpu.make_async_copy(res.at[0, pl.ds(8 * t, 8)], image.at[pl.ds(8 * t, 8)], band_sem.at[t]) for t in range(tiles)]
    for copy in bands:
        copy.start()
    loads = [pltpu.make_async_copy(psf.at[0, :, pl.ds(c * LANES, LANES)], psf_v.at[pl.ds(c * shard, shard)], psf_sem.at[c]) for c in range(chunks)]

    @pl.when(is_root)
    def _():
        for copy in loads:
            copy.start()

    begins = [jnp.clip(pos[1, k] - half, 0, ncols - patch) >> 7 for k in range(steps)]
    krow = lax.broadcasted_iota(jnp.int32, (steps, LANES), 0)
    target = jnp.zeros((steps, LANES), jnp.int32)
    for k in range(steps):
        target = jnp.where(krow == k, begins[k], target)
    target = target + lax.broadcasted_iota(jnp.int32, (steps, LANES), 1)
    prev, last = target, lane8
    for k in range(steps):
        inside = target - begins[k]
        prev = jnp.where((inside >= 0) & (inside < width) & (krow > k), inside + (base + width * k), prev)
        inside = lane8 - begins[k]
        last = jnp.where((inside >= 0) & (inside < width), inside + (base + width * k), last)
    prev_v[...] = prev
    last_v[...] = last
    lane32 = lax.broadcasted_iota(jnp.int32, (steps, LANES), 1)
    rows_from = jnp.zeros((steps, LANES), jnp.int32)
    cols_from = jnp.zeros((steps, LANES), jnp.int32)
    for k in range(steps):
        rows_from = rows_from + jnp.where(krow == k, pos[0, k], 0) - jnp.where(lane32 == k, pos[0, k], 0)
        cols_from = cols_from + jnp.where(krow == k, pos[1, k], 0) - jnp.where(lane32 == k, pos[1, k], 0)
    rows_from = rows_from + half - row * shard
    cols_from = cols_from + half
    owned = (rows_from >= 0) & (rows_from < shard) & (cols_from >= 0) & (cols_from < patch) & (lane32 < krow)
    pair_v[0] = ((cols_from >> 7) & (chunks - 1)) * shard + (((rows_from >> 3) << 3) & (shard - 1))
    pair_v[1] = (lane32 - cols_from) & (LANES - 1)
    pair_v[2] = jnp.where(owned, (rows_from & 7) * LANES + lane32, -1)
    pair_copy = pltpu.make_async_copy(pair_v, pair_s, index_sem.at[3])

    @pl.when(is_root)
    def _():
        pair_copy.start()

    index_copies = [pltpu.make_async_copy(prev_v, prev_s, index_sem.at[0]), pltpu.make_async_copy(last_v, last_s, index_sem.at[1])]
    for copy in index_copies:
        copy.start()
    for t in range(tiles):
        work[t, blocks] = zero

    @pl.when(is_end)
    def _():
        pl.semaphore_wait(barrier, 5)

    @pl.when(is_mid)
    def _():
        pl.semaphore_wait(barrier, 7)


    def bulk(s):
        mid, end, other = (nchips - 1 + s) // 2, (nchips - 1) * s, nchips // 2 - s
        order = (0, 1) if s == 0 else (1, 0)
        near = list(range(nchips)) if s == 0 else list(range(2 * nchips - 1, nchips - 1, -1))
        across = [nchips - 1 - n if s == 0 else nchips + n for n in range(nchips // 2)]
        local = range(s * nchips, (s + 1) * nchips)
        out = []

        def add(u, z, h, rows, to_row, sem):
            out.append(pltpu.make_async_remote_copy(
                src_ref=psf.at[0, pl.ds((u % nchips) * unit + h * slab, rows)], dst_ref=land.at[pl.ds((u - begins_at[z]) * unit + h * slab, rows)],
                send_sem=send_sem.at[len(out)], recv_sem=sem, device_id=(chan, to_row), device_id_type=MESH))

        for u in near:
            for h in order:
                add(u, end, h, slab, 2 * end + (s if u == near[-1] else h), recv_sem.at[u - begins_at[end], h])
        for u in across:
            for h in range(2):
                add(u, other, h, slab, 2 * other + h, recv_sem.at[u - begins_at[other], h])
        for u in local:
            add(u, mid, 0, unit, solvers[s], unit_recv.at[u - begins_at[mid]])
        return out

    for s in range(2):
        @pl.when(row == roots[s])
        def _(s=s):
            for copy in bulk(s):
                copy.start()

    early = core == side
    is_lead, is_trail = is_end & early, is_end & jnp.logical_not(early)
    doubled = is_mid & jnp.logical_not(early)
    sends = jnp.where(is_end, jnp.where(early, tiles - 1, tiles - 2), jnp.where(early, tiles + 1, tiles + 2))
    count = jnp.where(is_end, tiles, sends)

    def tile_at(i):
        return jnp.where(side == 0, i, tiles - 1 - i)

    def tile_rows(t):
        return pl.ds(pl.multiple_of(8 * t, 8), 8)

    def guest_tile(g):
        return tile_at(jnp.where(early, tiles - 1, tiles - 2 + g))

    def lent(g):
        return pltpu.make_async_remote_copy(
            src_ref=res.at[0, tile_rows(guest_tile(g))], dst_ref=image.at[tile_rows(tiles + g)], send_sem=guest_sem.at[g], recv_sem=guest_sem.at[2 + g],
            device_id=(chan, row + 2 - 4 * side), device_id_type=MESH)

    def given(g):
        return pltpu.make_async_remote_copy(
            src_ref=parts.at[tile_rows(tiles + g)], dst_ref=parts.at[tile_rows(guest_tile(g))], send_sem=guest_sem.at[4 + g], recv_sem=guest_sem.at[6 + g],
            device_id=(chan, row - 2 + 4 * side), device_id_type=MESH)

    for bit in (1, 2):
        pl.semaphore_signal(ready.at[0], inc=1, device_id=(flip(bit), row), device_id_type=MESH)

    for copy in bands:
        copy.wait()

    def spread_out(b, carry):
        for t in range(tiles):
            work[t, b] = image[pl.ds(8 * t, 8), block_at(b)]
        return carry

    lax.fori_loop(0, blocks, spread_out, 0, unroll=4)
    acc = zero
    for k in range(steps):
        r, c = pos[0, k] - first, pos[1, k]
        tile = work[(r >> 3) & (tiles - 1), c >> 7]
        acc = pick(tile, r, c, k, (r >= 0) & (r < slab), number, acc)
    start_v[...] = acc

    def start_copy(s, source):
        return pltpu.make_async_remote_copy(
            src_ref=start_v, dst_ref=start_in.at[source], send_sem=start_send, recv_sem=start_recv.at[source],
            device_id=(chan, solvers[s]), device_id_type=MESH)

    def couple_copy(s):
        return pltpu.make_async_remote_copy(
            src_ref=couple_v, dst_ref=couple_in, send_sem=couple_send, recv_sem=couple_recv,
            device_id=(chan, solvers[s]), device_id_type=MESH)

    for s in range(2):
        @pl.when((side == s) & (row != solvers[s]))
        def _(s=s):
            start_copy(s, row).start()

    @pl.when(is_end)
    def _():
        lent(0).start()

    @pl.when(is_trail)
    def _():
        lent(1).start()

    @pl.when(is_root)
    def _():
        for copy in loads:
            copy.wait()
        pair_copy.wait()

        def fill(count, k, carry):
            acc = zero
            for j in range(count):
                tile = psf_v[pl.ds(pair_s[0, k, j], 8), :]
                acc = jnp.where(number == pair_s[2, k, j], pltpu.roll(tile, pair_s[1, k, j], 1), acc)
            grid[k] = acc
            return carry

        for g in range(steps // 8):
            lax.fori_loop(8 * g, 8 * g + 8, functools.partial(fill, 8 * g + 8), 0)
        couple_v[...] = jnp.sum(grid[...], axis=1)

    for s in range(2):
        @pl.when(row == roots[s])
        def _(s=s):
            couple_copy(s).start()

    def held(m, h, rows=slab):
        return land.at[pl.ds(pl.multiple_of(m * unit + h * slab, 8), rows)]

    def relay(m):
        return pltpu.make_async_remote_copy(
            src_ref=held(m, core), dst_ref=held(m, core), send_sem=relay_sem.at[m], recv_sem=recv_sem.at[m, core],
            device_id=(chan, partner), device_id_type=MESH)

    def arrival(m, h):
        return pltpu.make_async_remote_copy(
            src_ref=held(m, h), dst_ref=held(m, h), send_sem=relay_sem.at[m], recv_sem=recv_sem.at[m, h],
            device_id=(chan, partner), device_id_type=MESH)

    def pass_on(m):
        arrival(m, core).wait_recv()
        relay(m).start()

    def crossed(n):
        return jnp.where(side == 0, nchips + n, 1 - n)

    def streamed(n):
        return jnp.where(side == 0, n, nchips - n)

    def relayout(source, source_row, dest_row, rows):
        def body(g, carry):
            take, put = pl.multiple_of(source_row + 8 * g, 8), pl.multiple_of(dest_row + 8 * g, 8)
            for c in range(chunks):
                narrow = source.shape[1] == LANES
                tile = source[pl.ds(pl.multiple_of(c * shard + take, 8), 8), :] if narrow else source[pl.ds(take, 8), pl.ds(c * LANES, LANES)]
                patch_v[c, pl.ds(put, 8), :] = tile
            return carry

        lax.fori_loop(0, rows // 8, body, 0)

    @pl.when(is_root)
    def _():
        pass_on(crossed(0))

    pl.semaphore_wait(ready.at[0], 2)
    for bit in (1, 2):
        pl.semaphore_signal(ready.at[1], inc=1, device_id=(flip(bit), row), device_id_type=MESH)
    pl.semaphore_wait(ready.at[1], 2)
    me_table = 2 * chan + side

    def table_copy(step):
        other = (me_table + step) % (2 * nchan)
        return pltpu.make_async_remote_copy(
            src_ref=tables.at[me_table], dst_ref=tables.at[me_table], send_sem=table_send.at[step], recv_sem=table_recv.at[step],
            device_id=(other // 2, solvers[0] + (other % 2) * (solvers[1] - solvers[0])), device_id_type=MESH)

    def table_arrival(step):
        other = (me_table + 2 * nchan - step) % (2 * nchan)
        return pltpu.make_async_remote_copy(
            src_ref=tables.at[other], dst_ref=tables.at[other], send_sem=table_send.at[step], recv_sem=table_recv.at[step],
            device_id=(other // 2, solvers[0] + (other % 2) * (solvers[1] - solvers[0])), device_id_type=MESH)

    for s in range(2):
        @pl.when(row == solvers[s])
        def _(s=s):
            total = start_v[...]
            for source in range(s * nchips, (s + 1) * nchips):
                if source != solvers[s]:
                    start_copy(s, source).wait_recv()
                    total = total + start_in[source]
            couple_copy(s).wait_recv()
            tables[me_table, pl.ds(0, steps), :] = couple_in[...]
            tables[me_table, pl.ds(steps, 8), :] = jnp.broadcast_to(jnp.sum(total, axis=0, keepdims=True), total.shape)
            for step in range(1, 2 * nchan):
                table_copy(step).start()
            pass_on(crossed(0))

    def amp_copy(n):
        return pltpu.make_async_remote_copy(
            src_ref=amps_v, dst_ref=amps_v, send_sem=amp_send.at[n], recv_sem=amp_recv,
            device_id=(chan, side * nchips + (row + n) % nchips), device_id_type=MESH)

    @pl.when(is_solver)
    def _():
        for step in range(1, 2 * nchan):
            table_arrival(step).wait_recv()

        def rows_of(index):
            return jnp.concatenate([tables[2 * c, pl.ds(index, 1), :] + tables[2 * c + 1, pl.ds(index, 1), :] for c in range(nchan)], axis=0)

        start = rows_of(steps)

        def solve(k, amps):
            value = jnp.sum(jnp.where(lane == k, start, 0.0) - amps * rows_of(k), axis=1, keepdims=True)
            amp = 0.25 * (value + jnp.sum(value, axis=0, keepdims=True) / nchan)
            return jnp.where(lane == k, amp, amps)

        amps = lax.fori_loop(0, steps, solve, jnp.zeros((nchan, LANES), jnp.float32), unroll=4)
        amps_v[pl.ds(0, nchan), :] = amps
        amps_v[pl.ds(nchan, 8 - nchan), :] = jnp.zeros((8 - nchan, LANES), jnp.float32)
        for n in range(1, nchips):
            amp_copy(n).start()

    def fine_piece(n):
        return jnp.where(side == 0, n, 2 * tiles - 1 - n)

    def fine_at(n):
        return pl.multiple_of(jnp.where(side == 0, nchips, 0) * unit + 8 * fine_piece(n), 8)

    def onward_piece(s, n):
        mid, end = (nchips - 1 + s) // 2, (nchips - 1) * s
        u = nchips - s
        j = n if s == 0 else 2 * tiles - 1 - n
        return pltpu.make_async_remote_copy(
            src_ref=land.at[pl.ds((u - begins_at[mid]) * unit + 8 * j, 8)], dst_ref=land.at[pl.ds((u - begins_at[end]) * unit + 8 * j, 8)],
            send_sem=fine_send.at[n], recv_sem=fine_recv.at[n], device_id=(chan, 2 * end + (s if n == 0 else 1 - s)), device_id_type=MESH)

    def fine_copy(n):
        return pltpu.make_async_remote_copy(
            src_ref=land.at[pl.ds(fine_at(n), 8)], dst_ref=land.at[pl.ds(fine_at(n), 8)],
            send_sem=fine_relay.at[n], recv_sem=fine_recv.at[n], device_id=(chan, partner), device_id_type=MESH)

    for s in range(2):
        offset = s * nchips - begins_at[(nchips - 1 + s) // 2]

        @pl.when(row == roots[s])
        def _(s=s, offset=offset):
            arrival(crossed(0), 1 - core).wait_recv()
            for n in range(2 * tiles):
                onward_piece(s, n).start()
            relayout(psf_v, 0, offset * unit, nchips * unit)

        @pl.when(row == solvers[s])
        def _(s=s, offset=offset):
            arrival(crossed(0), 1 - core).wait_recv()
            for u in range(nchips):
                pltpu.make_async_remote_copy(
                    src_ref=held(u + offset, 0, unit), dst_ref=held(u + offset, 0, unit), send_sem=send_sem.at[0], recv_sem=unit_recv.at[u + offset],
                    device_id=(chan, partner), device_id_type=MESH).wait_recv()
            relayout(land, offset * unit, offset * unit, nchips * unit)

    def relayout_crossed(n):
        begin = pl.multiple_of(crossed(n) * unit, 8)
        relayout(land, begin, begin, unit)

    @pl.when(is_mid)
    def _():
        relayout_crossed(0)

    amps_copy = pltpu.make_async_copy(amps_v, amps_s, index_sem.at[2])
    leading = early

    def half_unit(m, h):
        begin = pl.multiple_of(m * unit + h * slab, 8)
        relayout(land, begin, begin, slab)

    def relay_half(m, h):
        return pltpu.make_async_remote_copy(
            src_ref=held(m, h), dst_ref=held(m, h), send_sem=relay_sem.at[nchips + 2 + h], recv_sem=recv_sem.at[m, h],
            device_id=(chan, partner), device_id_type=MESH)

    @pl.when(is_end)
    def _():
        for n in range(nchips - 1):
            pass_on(streamed(n))
            if n > 0:
                arrival(streamed(n - 1), 1 - core).wait_recv()
                for h in range(2):
                    half_unit(streamed(n - 1), h)
        amp_copy(1).wait_recv()
        amps_copy.start()
        arrival(streamed(nchips - 2), 1 - core).wait_recv()
        for h in range(2):
            half_unit(streamed(nchips - 2), h)

    @pl.when(is_end & leading)
    def _():
        for n in range(2):
            h = jnp.where(side == 0, n, 1 - n)
            arrival(streamed(nchips - 1), h).wait_recv()
            relay_half(streamed(nchips - 1), h).start()
            half_unit(streamed(nchips - 1), h)

    @pl.when(is_end & jnp.logical_not(leading))
    def _():
        for n in range(2):
            h = jnp.where(side == 0, n, 1 - n)
            arrival(streamed(nchips - 1), h).wait_recv()
            half_unit(streamed(nchips - 1), h)

    @pl.when(is_root)
    def _():
        amp_copy(1).wait_recv()

    @pl.when(is_mid)
    def _():
        amps_copy.start()

    for copy in index_copies:
        copy.wait()
    amps_copy.wait()

    cols = ncols // nchan
    span = cols // 2
    bits = ((1, 2), (2, 1))

    diagonal = 3 - chan

    def is_guest(n):
        return (n == 0) | (doubled & (n == 2))

    def own_index(n):
        return jnp.where(is_mid, n - 1 - jnp.where(doubled & (n > 2), 1, 0), n)

    def tile_of(n):
        return jnp.where(is_mid & is_guest(n), tiles + n // 2, tile_at(own_index(n)))

    def rows_at(n):
        return tile_rows(tile_of(n))

    def lift_of(n):
        own_lift = lead * unit + 8 * tile_at(own_index(n))
        guest_lift = side * unit + 8 * guest_tile(n // 2)
        return slab * nrows + core * slab + jnp.where(is_mid & is_guest(n), guest_lift, own_lift)

    def cols_at(c, p):
        return pl.ds(pl.multiple_of(c * cols + p * span, LANES), span)

    def send(i, p, source, dest, send_sem, recv_sem, to):
        return pltpu.make_async_remote_copy(
            src_ref=source, dst_ref=dest.at[i, p], send_sem=send_sem.at[i, p], recv_sem=recv_sem.at[i, p],
            device_id=(to, row), device_id_type=MESH)

    def far(i, p):
        return send(i, p, image.at[rows_at(i), cols_at(diagonal, p)], first_far, far_send, far_recv, flip(bits[p][0]))

    def mine(i, p):
        return send(i, p, image.at[rows_at(i), cols_at(flip(bits[p][0]), p)], first_own, own_send, own_recv, flip(bits[p][0]))

    def onward(i, p):
        return send(i, p, passed.at[i, p], second, pass_send, pass_recv, flip(bits[p][1]))

    def fetch(n):
        fine_copy(n).wait_recv()

    def arrive(n):
        fetch(n)
        relayout(land, fine_at(n), fine_at(n), 8)

    def share(n):
        fetch(n)
        fine_copy(n).start()
        relayout(land, fine_at(n), fine_at(n), 8)

    def scale_and_shift(i):
        lift = lift_of(i)

        def eight(g, carry):
            for n in range(8):
                k = 8 * g + n
                amp = amps_s[chan, k]
                begin = lift - pos[0, k]
                shift = (pos[1, k] - half) & (LANES - 1)
                keep = lane8 < shift
                moved = [zero] + [pltpu.roll(patch_v[c, pl.ds(begin, 8), :] * amp, shift, 1) for c in range(chunks)] + [zero]
                for m in range(width):
                    changes[width * k + m] = jnp.where(keep, moved[m], moved[m + 1])
            return carry

        lax.fori_loop(0, steps // 8, eight, 0)

    def subtract(i):
        t = tile_of(i)

        def eight(g, carry):
            for n in range(8):
                k = 8 * g + n
                after = [work[t, prev_s[k, m]] - changes[width * k + m] for m in range(width)]
                for m in range(width):
                    work[t, base + width * k + m] = after[m]
            return carry

        lax.fori_loop(0, steps // 8, eight, 0)

    def finalize(i, c):
        rows = rows_at(i)
        per = cols // LANES

        def body(g, carry):
            for n in range(8):
                b = c * per + g * 8 + n
                image[rows, block_at(b)] = work[tile_of(i), last_s[0, b]]
            return carry

        lax.fori_loop(0, per // 8, body, 0)

    def combine(i):
        for p in range(2):
            far(i, p).wait_recv()
            passed[i, p] = image[rows_at(i), cols_at(flip(bits[p][1]), p)] + first_far[i, p]
            onward(i, p).start()

    def own(n):
        for p in range(2):
            mine(n, p).wait_recv()
            onward(n, p).wait_recv()
            value = image[rows_at(n), cols_at(chan, p)] + first_own[n, p] + second[n, p]
            parts[rows_at(n), pl.ds(p * span, span)] = value
            square = value * value
            total = zero
            for c in range(span // LANES):
                total = total + square[:, c * LANES:(c + 1) * LANES]
            sum_v[...] = sum_v[...] + total

    def start_far(n):
        for p in range(2):
            far(n, p).start()

    def start_mine(n):
        for p in range(2):
            mine(n, p).start()

    def finish(n):
        for p in range(2):
            finalize(n, flip(bits[p][0]))
        finalize(n, chan)

    sum_v[...] = zero

    def advance(n, carry):
        active = n < count

        @pl.when(is_lead & (n == 0))
        def _():
            share(0)

        @pl.when(is_lead & (n > 0) & active)
        def _():
            arrive(n)

        @pl.when(is_trail & (n == 0))
        def _():
            arrive(0)
            for piece in range(1, tiles):
                share(piece)

        @pl.when(is_trail & active)
        def _():
            arrive(tiles + n)

        @pl.when(is_mid & is_guest(n))
        def _():
            lent(n // 2).wait_recv()

            def guest(b, carry):
                work[tiles + n // 2, b] = image[tile_rows(tiles + n // 2), block_at(b)]
                return carry

            lax.fori_loop(0, blocks, guest, 0, unroll=4)

        @pl.when(is_mid & (n == 1))
        def _():
            arrival(crossed(1), 1 - core).wait_recv()
            relayout_crossed(1)

        @pl.when(active)
        def _():
            scale_and_shift(n)

        @pl.when(is_mid & (n == 0))
        def _():
            pass_on(crossed(1))

        @pl.when(n == sends)
        def _():
            combine(n - 1)
            start_mine(n - 1)

        @pl.when(active)
        def _():
            subtract(n)
            finalize(n, diagonal)

        @pl.when(n < sends)
        def _():
            start_far(n)

        @pl.when(active)
        def _():
            finish(n)

        @pl.when((n == sends - 1) & (n > 1))
        def _():
            start_mine(n - 1)

        @pl.when((n > 0) & (n < sends))
        def _():
            combine(n - 1)

        @pl.when((n == 0) | (n < sends - 2))
        def _():
            start_mine(n)

        @pl.when(is_mid & (n == 3))
        def _():
            own(0)
            given(0).start()

        @pl.when(doubled & (n == 5))
        def _():
            own(2)
            given(1).start()

        return carry

    lax.fori_loop(0, tiles + 3, advance, 0)

    def settle(n, carry):
        @pl.when((n < sends) & jnp.logical_not(is_mid & is_guest(n)))
        def _():
            own(n)

        return carry

    lax.fori_loop(0, tiles + 2, settle, 0)
    total = sum_v[...]
    me = row * nchan + chan
    squares[pl.ds(me, 1), :] = jnp.sum(total, axis=0, keepdims=True)

    everyone = nrows * nchan

    def spread(step):
        other = (me + jnp.where(side == 0, everyone - step, step)) % everyone
        return pltpu.make_async_remote_copy(
            src_ref=squares.at[pl.ds(me, 1)], dst_ref=squares.at[pl.ds(me, 1)], send_sem=square_send.at[step], recv_sem=square_recv.at[me],
            device_id=(other % nchan, other // nchan), device_id_type=MESH)

    def arrived(step):
        other = (me + step) % everyone
        return pltpu.make_async_remote_copy(
            src_ref=squares.at[pl.ds(other, 1)], dst_ref=squares.at[pl.ds(other, 1)], send_sem=square_send.at[step], recv_sem=square_recv.at[other],
            device_id=(other % nchan, other // nchan), device_id_type=MESH)

    for step in range(1, nrows * nchan):
        spread(step).start()

    for s in range(2):
        @pl.when(row == roots[s])
        def _(s=s):
            for copy in bulk(s):
                copy.wait_send()
            for n in range(2 * tiles):
                onward_piece(s, n).wait_send()
            couple_copy(s).wait_send()

    @pl.when(is_mid)
    def _():
        for n in range(2):
            relay(crossed(n)).wait_send()

    @pl.when(is_end)
    def _():
        for n in range(nchips - 1):
            relay(streamed(n)).wait_send()

    @pl.when(is_end & leading)
    def _():
        for h in range(2):
            relay_half(streamed(nchips - 1), h).wait_send()
        fine_copy(0).wait_send()

    @pl.when(is_trail)
    def _():
        for n in range(1, tiles):
            fine_copy(n).wait_send()

    @pl.when(is_solver)
    def _():
        for step in range(1, 2 * nchan):
            table_copy(step).wait_send()
        for n in range(1, nchips):
            amp_copy(n).wait_send()

    @pl.when(jnp.logical_not(is_solver))
    def _():
        start_copy(0, row).wait_send()

    def sent(n, carry):
        @pl.when(n < sends)
        def _():
            for p in range(2):
                far(n, p).wait_send()
                mine(n, p).wait_send()
                onward(n, p).wait_send()

        return carry

    lax.fori_loop(0, tiles + 2, sent, 0)

    @pl.when(is_mid)
    def _():
        given(0).wait_send()

    @pl.when(doubled)
    def _():
        given(1).wait_send()

    @pl.when(is_end)
    def _():
        lent(0).wait_send()
        given(0).wait_recv()

    @pl.when(is_trail)
    def _():
        lent(1).wait_send()
        given(1).wait_recv()

    for step in range(1, nrows * nchan):
        arrived(step).wait_recv()
    everything = jnp.sum(jnp.sum(squares[...], axis=0, keepdims=True), axis=1, keepdims=True)
    total_out[...] = jnp.broadcast_to(everything, total_out.shape)
    for step in range(1, nrows * nchan):
        spread(step).wait_send()


def run_cycle(nchan, nrows, positions, residual, psf):
    slab, ncols = residual.shape[1:]
    shard, patch = psf.shape[1:]
    steps, chunks = positions.shape[1], patch // LANES
    nchips, tiles, cols = nrows // 2, slab // 8, ncols // nchan
    rows = slab * (nrows + 4)
    dma, f32, i32 = pltpu.SemaphoreType.DMA, jnp.float32, jnp.int32
    anywhere = pl.BlockSpec(memory_space=pl.ANY)
    vmem = pl.BlockSpec(memory_space=pltpu.VMEM)
    slots = ncols // LANES + 1 + (chunks + 1) * steps
    stage = pltpu.VMEM((tiles + 2, 2, 8, cols // 2), f32)
    small = pltpu.VMEM((8, LANES), f32)
    return pl.pallas_call(
        functools.partial(cycle_kernel, nchan, nrows),
        out_shape=(OUT((slab + 16, ncols), f32), OUT((slab + 16, cols), f32), OUT((8, LANES), f32)),
        in_specs=[pl.BlockSpec(memory_space=pltpu.SMEM), anywhere, anywhere],
        out_specs=(vmem, vmem, vmem),
        scratch_shapes=[
            pltpu.VMEM((tiles + 2, slots, 8, LANES), f32), pltpu.VMEM((rows, patch), f32), pltpu.VMEM((chunks, rows, LANES), f32),
            pltpu.VMEM((chunks * shard, LANES), f32), pltpu.VMEM((steps, 8, LANES), f32), pltpu.VMEM((steps, LANES), f32),
            pltpu.VMEM((steps, LANES), f32), small, pltpu.VMEM((nrows, 8, LANES), f32),
            pltpu.VMEM((2 * nchan, steps + 8, LANES), f32), small, pltpu.VMEM((steps, LANES), i32), pltpu.VMEM((8, LANES), i32),
            stage, stage, stage, stage, pltpu.VMEM((nrows * nchan, LANES), f32), pltpu.VMEM(((chunks + 1) * steps, 8, LANES), f32), pltpu.VMEM((3, steps, LANES), i32), small,
            pltpu.SMEM((steps, LANES), i32), pltpu.SMEM((8, LANES), i32), pltpu.SMEM((8, LANES), f32), pltpu.SMEM((3, steps, LANES), i32),
            pltpu.SemaphoreType.REGULAR((2,)), dma((tiles,)), dma((chunks,)), dma((4,)), dma((4 * nchips,)), dma((nchips + 2,)),
            dma((nchips + 2, 2)), dma((nchips + 4,)), dma((2 * tiles,)), dma((2 * tiles,)), dma((2 * tiles,)),
            dma, dma((nrows,)), dma, dma, dma((2 * nchan,)), dma((2 * nchan,)), dma((nchips,)), dma,
        ] + [dma((tiles + 2, 2))] * 6 + [dma((nrows * nchan,))] * 2 + [dma((8,))],
        compiler_params=pltpu.CompilerParams(collective_id=0, has_side_effects=True, vmem_limit_bytes=VMEM - 4 * ((slab + 16) * (ncols + cols) + 8 * LANES)),
        name="minor_cycle",
    )(positions, residual, psf)


def write_kernel(count, image, parts, total, image_out, normalized, scaled, sems):
    slab, tiles = scaled.shape[0], scaled.shape[0] // 8
    copies = [pltpu.make_async_copy(image.at[pl.ds(8 * t, 8)], image_out.at[0, pl.ds(8 * t, 8)], sems.at[t]) for t in range(tiles)]
    for copy in copies:
        copy.start()
    scale = lax.rsqrt(total[0:1, 0:1] / count + 1e-06)
    for t in range(tiles):
        rows = pl.ds(8 * t, 8)
        scaled[rows, :] = parts[rows, :] * scale
        copies.append(pltpu.make_async_copy(scaled.at[rows], normalized.at[rows], sems.at[tiles + t]))
        copies[-1].start()
    for copy in copies:
        copy.wait()


def write_outputs(count, slab, image, parts, total):
    f32, ncols, cols = jnp.float32, image.shape[1], parts.shape[1]
    anywhere, vmem = pl.BlockSpec(memory_space=pl.ANY), pl.BlockSpec(memory_space=pltpu.VMEM)
    return pl.pallas_call(
        functools.partial(write_kernel, count),
        out_shape=(jax.ShapeDtypeStruct((1, slab, ncols), f32), jax.ShapeDtypeStruct((slab, cols), f32)),
        in_specs=[vmem, vmem, vmem],
        out_specs=(anywhere, anywhere),
        scratch_shapes=[pltpu.VMEM((slab, cols), f32), pltpu.SemaphoreType.DMA((slab // 4,))],
        name="write_outputs",
        compiler_params=pltpu.CompilerParams(vmem_limit_bytes=4 * 2**20),
    )(*(pltpu.with_memory_space_constraint(x, pltpu.VMEM) for x in (image, parts, total)))


def on_device(residual, psf, positions):
    nchan, nrows = lax.axis_size("chan"), lax.axis_size("rows")
    slab, ncols = residual.shape[1:]
    shard, patch = psf.shape[1:]
    steps = positions.shape[0]
    central = slab * nrows == shard and shard * nrows == patch
    powers = all(n & (n - 1) == 0 for n in (slab, shard, patch)) and patch >= LANES
    lines = nchan == 4 and nrows == 8 and slab == 32 and ncols % (16 * LANES) == 0 and ncols <= LANES * LANES
    if not (central and powers and lines and steps % 8 == 0 and steps <= LANES and patch < LANES * LANES):
        return on_any_device(residual, psf, positions)
    image, parts, total = run_cycle(nchan, nrows, positions.T, residual, psf)
    return write_outputs(slab * nrows * ncols, slab, image, parts, total)


def on_any_device(residual, psf, positions):
    chan_id = lax.axis_index("chan")
    nchan = lax.axis_size("chan")
    row_id = lax.axis_index("rows")
    nrows = lax.axis_size("rows")
    slab = residual.shape[1]
    ncols = residual.shape[2]
    own_psf = psf[0]
    shard_rows = own_psf.shape[0]
    patch = own_psf.shape[1]
    half = patch // 2
    first = row_id * slab
    chan_hot = (jnp.arange(nchan) == chan_id).astype(jnp.float32)
    full_psf = lax.all_gather(own_psf, "rows", axis=0, tiled=True)
    padded_psf = jnp.pad(full_psf, ((slab, slab), (0, 0)))
    zero = jnp.int32(0)

    def subtract(image, row, col, amount):
        offset = first - row + half
        touches = jnp.logical_and(offset > -slab, offset < patch)
        start = jnp.clip(offset + slab, 0, patch + slab)
        psf_rows = lax.dynamic_slice(padded_psf, (start, zero), (slab, patch))
        window = lax.dynamic_slice(image, (zero, col - half), (slab, patch))
        scale = jnp.where(touches, amount, 0.0)
        return lax.dynamic_update_slice(image, window - scale * psf_rows, (zero, col - half))

    image = residual[0]
    peak_rows = positions[:, 0]
    peak_cols = positions[:, 1]
    inside = jnp.logical_and(peak_rows >= first, peak_rows < first + slab)
    local_rows = jnp.clip(peak_rows - first, 0, slab - 1)
    start_values = jnp.where(inside, image[local_rows, peak_cols], 0.0)
    row_offset = peak_rows[:, None] - peak_rows[None, :] + half - row_id * shard_rows
    col_offset = peak_cols[:, None] - peak_cols[None, :] + half
    owned = (row_offset >= 0) & (row_offset < shard_rows) & (col_offset >= 0) & (col_offset < patch)
    couple = own_psf[jnp.clip(row_offset, 0, shard_rows - 1), jnp.clip(col_offset, 0, patch - 1)]
    couple = jnp.where(owned, couple, 0.0)
    start_table, couple_table = lax.psum(
        (chan_hot[:, None] * start_values[None, :], chan_hot[:, None, None] * couple[None, :, :]),
        ("chan", "rows"),
    )

    def solve(k, amps):
        taken = jnp.sum(amps * lax.dynamic_index_in_dim(couple_table, k, 1, False), axis=1)
        value = lax.dynamic_index_in_dim(start_table, k, 1, False) - taken
        amp = 0.25 * (value + jnp.sum(value) / nchan)
        return lax.dynamic_update_index_in_dim(amps, amp, k, 1)

    amps = lax.fori_loop(0, STEPS, solve, jnp.zeros((nchan, STEPS), jnp.float32))
    own_amps = jnp.sum(chan_hot[:, None] * amps, axis=0)

    def apply(k, image):
        return subtract(image, positions[k, 0], positions[k, 1], own_amps[k])

    image = lax.fori_loop(0, STEPS, apply, image)
    count = slab * nrows * ncols
    parts = lax.psum_scatter(image, "chan", scatter_dimension=1, tiled=True)
    total = lax.psum(jnp.sum(parts * parts), ("chan", "rows"))
    normalized = parts * lax.rsqrt(total / count + 1e-06)
    return (image[None], normalized)


def solution(mesh):
    return jax.shard_map(
        on_device,
        mesh=mesh,
        in_specs=(P("chan", "rows", None), P("chan", "rows", None), P()),
        out_specs=(P("chan", "rows", None), P("rows", "chan")),
        check_vma=False,
    )
```

```python
import functools

import jax
import jax.numpy as jnp
from jax import lax
from jax.experimental import pallas as pl
from jax.experimental.pallas import tpu as pltpu
from jax.sharding import PartitionSpec as P

STEPS = 32
LANES = 128
MESH = pl.DeviceIdType.MESH
OUT = pltpu.VMEM
VMEM = 67043328


def pick(tile, row, col, lane_to, owned, number, acc):
    moved = pltpu.roll(tile, (lane_to - col) & (LANES - 1), 1)
    target = jnp.where(owned, (row & 7) * LANES + lane_to, -1)
    return jnp.where(number == target, moved, acc)


def cycle_kernel(nchan, nrows, pos, res, psf, image, parts, total_out,
                 work, land, patch_v, psf_v, grid, couple_v, couple_in, start_v, start_in, tables, amps_v, prev_v, last_v,
                 first_far, first_own, passed, second, squares, changes, pair_v, sum_v, prev_s, last_s, amps_s, pair_s,
                 ready, band_sem, psf_sem, index_sem, send_sem, unit_recv, recv_sem, relay_sem, fine_send, fine_recv, fine_relay,
                 start_send, start_recv, couple_send, couple_recv, table_send, table_recv, amp_send, amp_recv,
                 far_send, far_recv, own_send, own_recv, pass_send, pass_recv, square_send, square_recv, guest_sem, lent_send, lent_recv):
    chan, row = lax.axis_index("chan"), lax.axis_index("rows")
    chip, core = row // 2, row % 2
    partner = row + 1 - 2 * core
    nchips = nrows // 2
    side = chip // (nchips // 2)
    slab, ncols = res.shape[1], res.shape[2]
    shard, patch = psf.shape[1:]
    half, steps, chunks = patch // 2, pos.shape[1], patch // LANES
    unit, tiles, blocks = 2 * slab, slab // 8, ncols // LANES
    base, width = blocks + 1, chunks + 1
    first = row * slab
    begins_at = [z - (1 if z == (nchips - 1) // 2 else 0) for z in range(nchips)]
    lead = jnp.where(chip == (nchips - 1) // 2, 1, 0)
    roots = (nchips - 1, nchips)
    solvers = (roots[0] ^ 1, roots[1] ^ 1)
    is_root = jnp.logical_or(row == roots[0], row == roots[1])
    is_solver = jnp.logical_or(row == solvers[0], row == solvers[1])
    is_mid = jnp.logical_or(is_root, is_solver)
    is_end = jnp.logical_not(is_mid)
    lane = lax.broadcasted_iota(jnp.int32, (1, LANES), 1)
    lane8 = lax.broadcasted_iota(jnp.int32, (8, LANES), 1)
    number = lax.broadcasted_iota(jnp.int32, (8, LANES), 0) * LANES + lane8
    zero = jnp.zeros((8, LANES), jnp.float32)

    def block_at(index):
        return pl.ds(pl.multiple_of(index * LANES, LANES), LANES)

    def flip(bit):
        if bit == 1:
            return chan + 1 - 2 * (chan % 2)
        return (chan + 2) % 4

    barrier = pltpu.get_barrier_semaphore()
    for bit in (1, 2):
        pl.semaphore_signal(barrier, inc=1, device_id=(flip(bit), row), device_id_type=MESH)
    pl.semaphore_signal(barrier, inc=1, device_id=(chan, partner), device_id_type=MESH)

    @pl.when(chip > 0)
    def _():
        for c in range(2):
            pl.semaphore_signal(barrier, inc=1, device_id=(chan, 2 * chip - 2 + c), device_id_type=MESH)

    @pl.when(chip < nchips - 1)
    def _():
        for c in range(2):
            pl.semaphore_signal(barrier, inc=1, device_id=(chan, 2 * chip + 2 + c), device_id_type=MESH)

    bands = [pltpu.make_async_copy(res.at[0, pl.ds(8 * t, 8)], image.at[pl.ds(8 * t, 8)], band_sem.at[t]) for t in range(tiles)]
    for copy in bands:
        copy.start()
    loads = [pltpu.make_async_copy(psf.at[0, :, pl.ds(c * LANES, LANES)], psf_v.at[pl.ds(c * shard, shard)], psf_sem.at[c]) for c in range(chunks)]

    @pl.when(is_root)
    def _():
        for copy in loads:
            copy.start()

    begins = [jnp.clip(pos[1, k] - half, 0, ncols - patch) >> 7 for k in range(steps)]
    krow = lax.broadcasted_iota(jnp.int32, (steps, LANES), 0)
    target = jnp.zeros((steps, LANES), jnp.int32)
    for k in range(steps):
        target = jnp.where(krow == k, begins[k], target)
    target = target + lax.broadcasted_iota(jnp.int32, (steps, LANES), 1)
    prev, last = target, lane8
    for k in range(steps):
        inside = target - begins[k]
        prev = jnp.where((inside >= 0) & (inside < width) & (krow > k), inside + (base + width * k), prev)
        inside = lane8 - begins[k]
        last = jnp.where((inside >= 0) & (inside < width), inside + (base + width * k), last)
    prev_v[...] = prev
    last_v[...] = last
    lane32 = lax.broadcasted_iota(jnp.int32, (steps, LANES), 1)
    rows_from = jnp.zeros((steps, LANES), jnp.int32)
    cols_from = jnp.zeros((steps, LANES), jnp.int32)
    for k in range(steps):
        rows_from = rows_from + jnp.where(krow == k, pos[0, k], 0) - jnp.where(lane32 == k, pos[0, k], 0)
        cols_from = cols_from + jnp.where(krow == k, pos[1, k], 0) - jnp.where(lane32 == k, pos[1, k], 0)
    rows_from = rows_from + half - row * shard
    cols_from = cols_from + half
    owned = (rows_from >= 0) & (rows_from < shard) & (cols_from >= 0) & (cols_from < patch) & (lane32 < krow)
    pair_v[0] = ((cols_from >> 7) & (chunks - 1)) * shard + (((rows_from >> 3) << 3) & (shard - 1))
    pair_v[1] = (lane32 - cols_from) & (LANES - 1)
    pair_v[2] = jnp.where(owned, (rows_from & 7) * LANES + lane32, -1)
    pair_copy = pltpu.make_async_copy(pair_v, pair_s, index_sem.at[3])

    @pl.when(is_root)
    def _():
        pair_copy.start()

    index_copies = [pltpu.make_async_copy(prev_v, prev_s, index_sem.at[0]), pltpu.make_async_copy(last_v, last_s, index_sem.at[1])]
    for copy in index_copies:
        copy.start()
    for t in range(tiles):
        work[t, blocks] = zero

    @pl.when(is_end)
    def _():
        pl.semaphore_wait(barrier, 5)

    @pl.when(is_mid)
    def _():
        pl.semaphore_wait(barrier, 7)


    def bulk(s):
        mid, end, other = (nchips - 1 + s) // 2, (nchips - 1) * s, nchips // 2 - s
        order = (0, 1) if s == 0 else (1, 0)
        near = list(range(nchips)) if s == 0 else list(range(2 * nchips - 1, nchips - 1, -1))
        across = [nchips - 1 - n if s == 0 else nchips + n for n in range(nchips // 2)]
        local = range(s * nchips, (s + 1) * nchips)
        out = []

        def add(u, z, h, rows, to_row, sem):
            out.append(pltpu.make_async_remote_copy(
                src_ref=psf.at[0, pl.ds((u % nchips) * unit + h * slab, rows)], dst_ref=land.at[pl.ds((u - begins_at[z]) * unit + h * slab, rows)],
                send_sem=send_sem.at[len(out)], recv_sem=sem, device_id=(chan, to_row), device_id_type=MESH))

        for u in near:
            for h in order:
                add(u, end, h, slab, 2 * end + (s if u == near[-1] else h), recv_sem.at[u - begins_at[end], h])
        for u in across:
            for h in range(2):
                add(u, other, h, slab, 2 * other + h, recv_sem.at[u - begins_at[other], h])
        for u in local:
            add(u, mid, 0, unit, solvers[s], unit_recv.at[u - begins_at[mid]])
        return out

    for s in range(2):
        @pl.when(row == roots[s])
        def _(s=s):
            for copy in bulk(s):
                copy.start()

    early = core == side
    is_lead, is_trail = is_end & early, is_end & jnp.logical_not(early)
    doubled = is_mid & jnp.logical_not(early)
    sends = jnp.where(is_end, jnp.where(early, tiles - 1, tiles - 2), jnp.where(early, tiles + 1, tiles + 2))

    def tile_at(i):
        return jnp.where(side == 0, i, tiles - 1 - i)

    def tile_rows(t):
        return pl.ds(pl.multiple_of(8 * t, 8), 8)

    def guest_tile(g):
        return tile_at(jnp.where(early, tiles - 1, tiles - 2 + g))

    head = ncols // 8

    def lent(g, part):
        width = (head, ncols - head)[part]
        return pltpu.make_async_remote_copy(
            src_ref=res.at[0, tile_rows(guest_tile(g)), pl.ds(head * part, width)],
            dst_ref=image.at[tile_rows(tiles + g), pl.ds(head * part, width)],
            send_sem=lent_send.at[g, part], recv_sem=lent_recv.at[g, part], device_id=(chan, row + 2 - 4 * side), device_id_type=MESH)

    def given(g):
        return pltpu.make_async_remote_copy(
            src_ref=parts.at[tile_rows(tiles + g)], dst_ref=parts.at[tile_rows(guest_tile(g))], send_sem=guest_sem.at[g], recv_sem=guest_sem.at[2 + g],
            device_id=(chan, row - 2 + 4 * side), device_id_type=MESH)

    @pl.when(is_end)
    def _():
        lent(0, 0).start()

    for bit in (1, 2):
        pl.semaphore_signal(ready.at[0], inc=1, device_id=(flip(bit), row), device_id_type=MESH)

    for copy in bands:
        copy.wait()

    def spread_out(b, carry):
        for t in range(tiles):
            work[t, b] = image[pl.ds(8 * t, 8), block_at(b)]
        return carry

    lax.fori_loop(0, blocks, spread_out, 0, unroll=4)
    acc = zero
    for k in range(steps):
        r, c = pos[0, k] - first, pos[1, k]
        tile = work[(r >> 3) & (tiles - 1), c >> 7]
        acc = pick(tile, r, c, k, (r >= 0) & (r < slab), number, acc)
    start_v[...] = acc

    def start_copy(s, source):
        return pltpu.make_async_remote_copy(
            src_ref=start_v, dst_ref=start_in.at[source], send_sem=start_send, recv_sem=start_recv.at[source],
            device_id=(chan, solvers[s]), device_id_type=MESH)

    def couple_copy(s):
        return pltpu.make_async_remote_copy(
            src_ref=couple_v, dst_ref=couple_in, send_sem=couple_send, recv_sem=couple_recv,
            device_id=(chan, solvers[s]), device_id_type=MESH)

    for s in range(2):
        @pl.when((side == s) & (row != solvers[s]))
        def _(s=s):
            start_copy(s, row).start()

    @pl.when(is_end)
    def _():
        lent(0, 1).start()

    @pl.when(is_trail)
    def _():
        for part in range(2):
            lent(1, part).start()

    @pl.when(is_root)
    def _():
        for copy in loads:
            copy.wait()
        pair_copy.wait()

        def fill(count, k, carry):
            acc = zero
            for j in range(count):
                tile = psf_v[pl.ds(pair_s[0, k, j], 8), :]
                acc = jnp.where(number == pair_s[2, k, j], pltpu.roll(tile, pair_s[1, k, j], 1), acc)
            grid[k] = acc
            return carry

        for g in range(steps // 8):
            lax.fori_loop(8 * g, 8 * g + 8, functools.partial(fill, 8 * g + 8), 0)
        couple_v[...] = jnp.sum(grid[...], axis=1)

    for s in range(2):
        @pl.when(row == roots[s])
        def _(s=s):
            couple_copy(s).start()

    def held(m, h, rows=slab):
        return land.at[pl.ds(pl.multiple_of(m * unit + h * slab, 8), rows)]

    def relay(m):
        return pltpu.make_async_remote_copy(
            src_ref=held(m, core), dst_ref=held(m, core), send_sem=relay_sem.at[m], recv_sem=recv_sem.at[m, core],
            device_id=(chan, partner), device_id_type=MESH)

    def arrival(m, h):
        return pltpu.make_async_remote_copy(
            src_ref=held(m, h), dst_ref=held(m, h), send_sem=relay_sem.at[m], recv_sem=recv_sem.at[m, h],
            device_id=(chan, partner), device_id_type=MESH)

    def pass_on(m):
        arrival(m, core).wait_recv()
        relay(m).start()

    def crossed(n):
        return jnp.where(side == 0, nchips + n, 1 - n)

    def streamed(n):
        return jnp.where(side == 0, n, nchips - n)

    def relayout(source, source_row, dest_row, rows):
        def body(g, carry):
            take, put = pl.multiple_of(source_row + 8 * g, 8), pl.multiple_of(dest_row + 8 * g, 8)
            for c in range(chunks):
                narrow = source.shape[1] == LANES
                tile = source[pl.ds(pl.multiple_of(c * shard + take, 8), 8), :] if narrow else source[pl.ds(take, 8), pl.ds(c * LANES, LANES)]
                patch_v[c, pl.ds(put, 8), :] = tile
            return carry

        lax.fori_loop(0, rows // 8, body, 0)

    @pl.when(is_root)
    def _():
        pass_on(crossed(0))

    pl.semaphore_wait(ready.at[0], 2)
    for bit in (1, 2):
        pl.semaphore_signal(ready.at[1], inc=1, device_id=(flip(bit), row), device_id_type=MESH)
    pl.semaphore_wait(ready.at[1], 2)
    me_table = 2 * chan + side

    def table_copy(step):
        other = (me_table + step) % (2 * nchan)
        return pltpu.make_async_remote_copy(
            src_ref=tables.at[me_table], dst_ref=tables.at[me_table], send_sem=table_send.at[step], recv_sem=table_recv.at[step],
            device_id=(other // 2, solvers[0] + (other % 2) * (solvers[1] - solvers[0])), device_id_type=MESH)

    def table_arrival(step):
        other = (me_table + 2 * nchan - step) % (2 * nchan)
        return pltpu.make_async_remote_copy(
            src_ref=tables.at[other], dst_ref=tables.at[other], send_sem=table_send.at[step], recv_sem=table_recv.at[step],
            device_id=(other // 2, solvers[0] + (other % 2) * (solvers[1] - solvers[0])), device_id_type=MESH)

    for s in range(2):
        @pl.when(row == solvers[s])
        def _(s=s):
            total = start_v[...]
            for source in range(s * nchips, (s + 1) * nchips):
                if source != solvers[s]:
                    start_copy(s, source).wait_recv()
                    total = total + start_in[source]
            couple_copy(s).wait_recv()
            tables[me_table, pl.ds(0, steps), :] = couple_in[...]
            tables[me_table, pl.ds(steps, 8), :] = jnp.broadcast_to(jnp.sum(total, axis=0, keepdims=True), total.shape)
            for step in range(1, 2 * nchan):
                table_copy(step).start()
            pass_on(crossed(0))

    def amp_copy(n):
        return pltpu.make_async_remote_copy(
            src_ref=amps_v, dst_ref=amps_v, send_sem=amp_send.at[n], recv_sem=amp_recv,
            device_id=(chan, side * nchips + (row + n) % nchips), device_id_type=MESH)

    @pl.when(is_solver)
    def _():
        for step in range(1, 2 * nchan):
            table_arrival(step).wait_recv()

        def rows_of(index):
            return jnp.concatenate([tables[2 * c, pl.ds(index, 1), :] + tables[2 * c + 1, pl.ds(index, 1), :] for c in range(nchan)], axis=0)

        start = rows_of(steps)

        def solve(k, amps):
            value = jnp.sum(jnp.where(lane == k, start, 0.0) - amps * rows_of(k), axis=1, keepdims=True)
            amp = 0.25 * (value + jnp.sum(value, axis=0, keepdims=True) / nchan)
            return jnp.where(lane == k, amp, amps)

        amps = lax.fori_loop(0, steps, solve, jnp.zeros((nchan, LANES), jnp.float32), unroll=4)
        amps_v[pl.ds(0, nchan), :] = amps
        amps_v[pl.ds(nchan, 8 - nchan), :] = jnp.zeros((8 - nchan, LANES), jnp.float32)
        for n in range(1, nchips):
            amp_copy(n).start()

    def fine_piece(n):
        return jnp.where(side == 0, n, 2 * tiles - 1 - n)

    def fine_at(n):
        return pl.multiple_of(jnp.where(side == 0, nchips, 0) * unit + 8 * fine_piece(n), 8)

    def onward_piece(s, n):
        mid, end = (nchips - 1 + s) // 2, (nchips - 1) * s
        u = nchips - s
        j = n if s == 0 else 2 * tiles - 1 - n
        return pltpu.make_async_remote_copy(
            src_ref=land.at[pl.ds((u - begins_at[mid]) * unit + 8 * j, 8)], dst_ref=land.at[pl.ds((u - begins_at[end]) * unit + 8 * j, 8)],
            send_sem=fine_send.at[n], recv_sem=fine_recv.at[n], device_id=(chan, 2 * end + (s if n == 0 else 1 - s)), device_id_type=MESH)

    def fine_copy(n):
        return pltpu.make_async_remote_copy(
            src_ref=land.at[pl.ds(fine_at(n), 8)], dst_ref=land.at[pl.ds(fine_at(n), 8)],
            send_sem=fine_relay.at[n], recv_sem=fine_recv.at[n], device_id=(chan, partner), device_id_type=MESH)

    for s in range(2):
        offset = s * nchips - begins_at[(nchips - 1 + s) // 2]

        @pl.when(row == roots[s])
        def _(s=s, offset=offset):
            arrival(crossed(0), 1 - core).wait_recv()
            for n in range(2 * tiles):
                onward_piece(s, n).start()
            relayout(psf_v, 0, offset * unit, nchips * unit)

        @pl.when(row == solvers[s])
        def _(s=s, offset=offset):
            arrival(crossed(0), 1 - core).wait_recv()
            for u in range(nchips):
                pltpu.make_async_remote_copy(
                    src_ref=held(u + offset, 0, unit), dst_ref=held(u + offset, 0, unit), send_sem=send_sem.at[0], recv_sem=unit_recv.at[u + offset],
                    device_id=(chan, partner), device_id_type=MESH).wait_recv()
            relayout(land, offset * unit, offset * unit, nchips * unit)

    def relayout_crossed(n):
        begin = pl.multiple_of(crossed(n) * unit, 8)
        relayout(land, begin, begin, unit)

    @pl.when(is_mid)
    def _():
        relayout_crossed(0)

    amps_copy = pltpu.make_async_copy(amps_v, amps_s, index_sem.at[2])
    leading = early

    def half_unit(m, h):
        begin = pl.multiple_of(m * unit + h * slab, 8)
        relayout(land, begin, begin, slab)

    def relay_half(m, h):
        return pltpu.make_async_remote_copy(
            src_ref=held(m, h), dst_ref=held(m, h), send_sem=relay_sem.at[nchips + 2 + h], recv_sem=recv_sem.at[m, h],
            device_id=(chan, partner), device_id_type=MESH)

    @pl.when(is_end)
    def _():
        for n in range(nchips - 1):
            pass_on(streamed(n))
            if n > 0:
                arrival(streamed(n - 1), 1 - core).wait_recv()
                for h in range(2):
                    half_unit(streamed(n - 1), h)
        amp_copy(1).wait_recv()
        amps_copy.start()
        arrival(streamed(nchips - 2), 1 - core).wait_recv()
        for h in range(2):
            half_unit(streamed(nchips - 2), h)

    @pl.when(is_end & leading)
    def _():
        for n in range(2):
            h = jnp.where(side == 0, n, 1 - n)
            arrival(streamed(nchips - 1), h).wait_recv()
            relay_half(streamed(nchips - 1), h).start()
            half_unit(streamed(nchips - 1), h)

    @pl.when(is_end & jnp.logical_not(leading))
    def _():
        for n in range(2):
            h = jnp.where(side == 0, n, 1 - n)
            arrival(streamed(nchips - 1), h).wait_recv()
            half_unit(streamed(nchips - 1), h)

    @pl.when(is_root)
    def _():
        amp_copy(1).wait_recv()

    @pl.when(is_mid)
    def _():
        amps_copy.start()

    for copy in index_copies:
        copy.wait()
    amps_copy.wait()

    cols = ncols // nchan
    span = cols // 2
    bits = ((1, 2), (2, 1))

    diagonal = 3 - chan

    def is_guest(n):
        return (n == 0) | (doubled & (n == 2))

    def own_index(n):
        return jnp.where(is_mid, n - 1 - jnp.where(doubled & (n > 2), 1, 0), n)

    def tile_of(n):
        return jnp.where(is_mid & is_guest(n), tiles + n // 2, tile_at(own_index(n)))

    def rows_at(n):
        return tile_rows(tile_of(n))

    def lift_of(n):
        own_lift = lead * unit + 8 * tile_at(own_index(n))
        guest_lift = side * unit + 8 * guest_tile(n // 2)
        return slab * nrows + core * slab + jnp.where(is_mid & is_guest(n), guest_lift, own_lift)

    def cols_at(c, p):
        return pl.ds(pl.multiple_of(c * cols + p * span, LANES), span)

    def send(i, p, source, dest, send_sem, recv_sem, to):
        return pltpu.make_async_remote_copy(
            src_ref=source, dst_ref=dest.at[i, p], send_sem=send_sem.at[i, p], recv_sem=recv_sem.at[i, p],
            device_id=(to, row), device_id_type=MESH)

    def far(i, p):
        return send(i, p, image.at[rows_at(i), cols_at(diagonal, p)], first_far, far_send, far_recv, flip(bits[p][0]))

    def mine(i, p):
        return send(i, p, image.at[rows_at(i), cols_at(flip(bits[p][0]), p)], first_own, own_send, own_recv, flip(bits[p][0]))

    def onward(i, p):
        return send(i, p, passed.at[i, p], second, pass_send, pass_recv, flip(bits[p][1]))

    def fetch(n):
        fine_copy(n).wait_recv()

    def arrive(n):
        fetch(n)
        relayout(land, fine_at(n), fine_at(n), 8)

    def share(n):
        fetch(n)
        fine_copy(n).start()
        relayout(land, fine_at(n), fine_at(n), 8)

    def scale_and_shift(i):
        lift = lift_of(i)

        def eight(g, carry):
            for n in range(8):
                k = 8 * g + n
                amp = amps_s[chan, k]
                begin = lift - pos[0, k]
                shift = (pos[1, k] - half) & (LANES - 1)
                keep = lane8 < shift
                moved = [zero] + [pltpu.roll(patch_v[c, pl.ds(begin, 8), :] * amp, shift, 1) for c in range(chunks)] + [zero]
                for m in range(width):
                    changes[width * k + m] = jnp.where(keep, moved[m], moved[m + 1])
            return carry

        lax.fori_loop(0, steps // 8, eight, 0)

    def subtract(i):
        t = tile_of(i)

        def eight(g, carry):
            for n in range(8):
                k = 8 * g + n
                after = [work[t, prev_s[k, m]] - changes[width * k + m] for m in range(width)]
                for m in range(width):
                    work[t, base + width * k + m] = after[m]
            return carry

        lax.fori_loop(0, steps // 8, eight, 0)

    def finalize(i, c):
        rows = rows_at(i)
        per = cols // LANES

        def body(g, carry):
            for n in range(8):
                b = c * per + g * 8 + n
                image[rows, block_at(b)] = work[tile_of(i), last_s[0, b]]
            return carry

        lax.fori_loop(0, per // 8, body, 0)

    def combine(i):
        for p in range(2):
            far(i, p).wait_recv()
            passed[i, p] = image[rows_at(i), cols_at(flip(bits[p][1]), p)] + first_far[i, p]
            onward(i, p).start()

    def own(n):
        for p in range(2):
            mine(n, p).wait_recv()
            onward(n, p).wait_recv()
            value = image[rows_at(n), cols_at(chan, p)] + first_own[n, p] + second[n, p]
            parts[rows_at(n), pl.ds(p * span, span)] = value
            square = value * value
            total = zero
            for c in range(span // LANES):
                total = total + square[:, c * LANES:(c + 1) * LANES]
            sum_v[...] = sum_v[...] + total

    def start_far(n):
        for p in range(2):
            far(n, p).start()

    def start_mine(n):
        for p in range(2):
            mine(n, p).start()

    def finish(n):
        for p in range(2):
            finalize(n, flip(bits[p][0]))
        finalize(n, chan)

    sum_v[...] = zero

    def advance(n, carry):
        active = n < sends

        @pl.when(is_lead & (n == 0))
        def _():
            share(0)

        @pl.when(is_lead & (n > 0) & active)
        def _():
            arrive(n)

        @pl.when(is_trail & (n == 0))
        def _():
            arrive(0)
            for piece in range(1, tiles):
                share(piece)

        @pl.when(is_trail & active)
        def _():
            arrive(tiles + n)

        @pl.when(is_mid & is_guest(n))
        def _():
            for part in range(2):
                lent(n // 2, part).wait_recv()

            def guest(b, carry):
                work[tiles + n // 2, b] = image[tile_rows(tiles + n // 2), block_at(b)]
                return carry

            lax.fori_loop(0, blocks, guest, 0, unroll=4)

        @pl.when(is_mid & (n == 1))
        def _():
            arrival(crossed(1), 1 - core).wait_recv()
            relayout_crossed(1)

        @pl.when(active)
        def _():
            scale_and_shift(n)

        @pl.when(is_mid & (n == 0))
        def _():
            pass_on(crossed(1))

        @pl.when(n == sends)
        def _():
            combine(n - 1)

        @pl.when(active)
        def _():
            subtract(n)
            finalize(n, diagonal)

        @pl.when(n < sends)
        def _():
            start_far(n)

        @pl.when(active)
        def _():
            finish(n)

        @pl.when(n < sends)
        def _():
            start_mine(n)

        @pl.when((n > 0) & (n < sends))
        def _():
            combine(n - 1)

        @pl.when(is_mid & (n == 4))
        def _():
            own(0)
            given(0).start()

        @pl.when(doubled & (n == 5))
        def _():
            own(2)
            given(1).start()

        return carry

    lax.fori_loop(0, tiles + 3, advance, 0)

    def settle(n, carry):
        @pl.when((n < sends) & jnp.logical_not(is_mid & is_guest(n)))
        def _():
            own(n)

        return carry

    lax.fori_loop(0, tiles + 2, settle, 0)
    total = sum_v[...]
    me = row * nchan + chan
    squares[pl.ds(me, 1), :] = jnp.sum(total, axis=0, keepdims=True)

    everyone = nrows * nchan

    def spread(step):
        other = (me + jnp.where(side == 0, everyone - step, step)) % everyone
        return pltpu.make_async_remote_copy(
            src_ref=squares.at[pl.ds(me, 1)], dst_ref=squares.at[pl.ds(me, 1)], send_sem=square_send.at[step], recv_sem=square_recv.at[me],
            device_id=(other % nchan, other // nchan), device_id_type=MESH)

    def arrived(step):
        other = (me + step) % everyone
        return pltpu.make_async_remote_copy(
            src_ref=squares.at[pl.ds(other, 1)], dst_ref=squares.at[pl.ds(other, 1)], send_sem=square_send.at[step], recv_sem=square_recv.at[other],
            device_id=(other % nchan, other // nchan), device_id_type=MESH)

    for step in range(1, nrows * nchan):
        spread(step).start()

    def leftover(n, carry):
        @pl.when(is_end & (n >= sends))
        def _():
            arrive(jnp.where(early, n, tiles + n))
            scale_and_shift(n)
            subtract(n)
            finalize(n, diagonal)
            finish(n)

        return carry

    lax.fori_loop(tiles - 2, tiles, leftover, 0)

    for s in range(2):
        @pl.when(row == roots[s])
        def _(s=s):
            for copy in bulk(s):
                copy.wait_send()
            for n in range(2 * tiles):
                onward_piece(s, n).wait_send()
            couple_copy(s).wait_send()

    @pl.when(is_mid)
    def _():
        for n in range(2):
            relay(crossed(n)).wait_send()

    @pl.when(is_end)
    def _():
        for n in range(nchips - 1):
            relay(streamed(n)).wait_send()

    @pl.when(is_end & leading)
    def _():
        for h in range(2):
            relay_half(streamed(nchips - 1), h).wait_send()
        fine_copy(0).wait_send()

    @pl.when(is_trail)
    def _():
        for n in range(1, tiles):
            fine_copy(n).wait_send()

    @pl.when(is_solver)
    def _():
        for step in range(1, 2 * nchan):
            table_copy(step).wait_send()
        for n in range(1, nchips):
            amp_copy(n).wait_send()

    @pl.when(jnp.logical_not(is_solver))
    def _():
        start_copy(0, row).wait_send()

    def sent(n, carry):
        @pl.when(n < sends)
        def _():
            for p in range(2):
                far(n, p).wait_send()
                mine(n, p).wait_send()
                onward(n, p).wait_send()

        return carry

    lax.fori_loop(0, tiles + 2, sent, 0)

    @pl.when(is_mid)
    def _():
        given(0).wait_send()

    @pl.when(doubled)
    def _():
        given(1).wait_send()

    @pl.when(is_end)
    def _():
        for part in range(2):
            lent(0, part).wait_send()
        given(0).wait_recv()

    @pl.when(is_trail)
    def _():
        for part in range(2):
            lent(1, part).wait_send()
        given(1).wait_recv()

    for step in range(1, nrows * nchan):
        arrived(step).wait_recv()
    everything = jnp.sum(jnp.sum(squares[...], axis=0, keepdims=True), axis=1, keepdims=True)
    total_out[...] = jnp.broadcast_to(everything, total_out.shape)
    for step in range(1, nrows * nchan):
        spread(step).wait_send()


def run_cycle(nchan, nrows, positions, residual, psf):
    slab, ncols = residual.shape[1:]
    shard, patch = psf.shape[1:]
    steps, chunks = positions.shape[1], patch // LANES
    nchips, tiles, cols = nrows // 2, slab // 8, ncols // nchan
    rows = slab * (nrows + 4)
    dma, f32, i32 = pltpu.SemaphoreType.DMA, jnp.float32, jnp.int32
    anywhere = pl.BlockSpec(memory_space=pl.ANY)
    vmem = pl.BlockSpec(memory_space=pltpu.VMEM)
    slots = ncols // LANES + 1 + (chunks + 1) * steps
    stage = pltpu.VMEM((tiles + 2, 2, 8, cols // 2), f32)
    small = pltpu.VMEM((8, LANES), f32)
    return pl.pallas_call(
        functools.partial(cycle_kernel, nchan, nrows),
        out_shape=(OUT((slab + 16, ncols), f32), OUT((slab + 16, cols), f32), OUT((8, LANES), f32)),
        in_specs=[pl.BlockSpec(memory_space=pltpu.SMEM), anywhere, anywhere],
        out_specs=(vmem, vmem, vmem),
        scratch_shapes=[
            pltpu.VMEM((tiles + 2, slots, 8, LANES), f32), pltpu.VMEM((rows, patch), f32), pltpu.VMEM((chunks, rows, LANES), f32),
            pltpu.VMEM((chunks * shard, LANES), f32), pltpu.VMEM((steps, 8, LANES), f32), pltpu.VMEM((steps, LANES), f32),
            pltpu.VMEM((steps, LANES), f32), small, pltpu.VMEM((nrows, 8, LANES), f32),
            pltpu.VMEM((2 * nchan, steps + 8, LANES), f32), small, pltpu.VMEM((steps, LANES), i32), pltpu.VMEM((8, LANES), i32),
            stage, stage, stage, stage, pltpu.VMEM((nrows * nchan, LANES), f32), pltpu.VMEM(((chunks + 1) * steps, 8, LANES), f32), pltpu.VMEM((3, steps, LANES), i32), small,
            pltpu.SMEM((steps, LANES), i32), pltpu.SMEM((8, LANES), i32), pltpu.SMEM((8, LANES), f32), pltpu.SMEM((3, steps, LANES), i32),
            pltpu.SemaphoreType.REGULAR((2,)), dma((tiles,)), dma((chunks,)), dma((4,)), dma((4 * nchips,)), dma((nchips + 2,)),
            dma((nchips + 2, 2)), dma((nchips + 4,)), dma((2 * tiles,)), dma((2 * tiles,)), dma((2 * tiles,)),
            dma, dma((nrows,)), dma, dma, dma((2 * nchan,)), dma((2 * nchan,)), dma((nchips,)), dma,
        ] + [dma((tiles + 2, 2))] * 6 + [dma((nrows * nchan,))] * 2 + [dma((4,)), dma((2, 2)), dma((2, 2))],
        compiler_params=pltpu.CompilerParams(collective_id=0, has_side_effects=True, vmem_limit_bytes=VMEM - 4 * ((slab + 16) * (ncols + cols) + 8 * LANES)),
        name="minor_cycle",
    )(positions, residual, psf)


def write_kernel(count, image, parts, total, image_out, normalized, scaled, sems):
    slab, tiles = scaled.shape[0], scaled.shape[0] // 8
    copies = [pltpu.make_async_copy(image.at[pl.ds(8 * t, 8)], image_out.at[0, pl.ds(8 * t, 8)], sems.at[t]) for t in range(tiles)]
    for copy in copies:
        copy.start()
    scale = lax.rsqrt(total[0:1, 0:1] / count + 1e-06)
    for t in range(tiles):
        rows = pl.ds(8 * t, 8)
        scaled[rows, :] = parts[rows, :] * scale
        copies.append(pltpu.make_async_copy(scaled.at[rows], normalized.at[rows], sems.at[tiles + t]))
        copies[-1].start()
    for copy in copies:
        copy.wait()


def write_outputs(count, slab, image, parts, total):
    f32, ncols, cols = jnp.float32, image.shape[1], parts.shape[1]
    anywhere, vmem = pl.BlockSpec(memory_space=pl.ANY), pl.BlockSpec(memory_space=pltpu.VMEM)
    return pl.pallas_call(
        functools.partial(write_kernel, count),
        out_shape=(jax.ShapeDtypeStruct((1, slab, ncols), f32), jax.ShapeDtypeStruct((slab, cols), f32)),
        in_specs=[vmem, vmem, vmem],
        out_specs=(anywhere, anywhere),
        scratch_shapes=[pltpu.VMEM((slab, cols), f32), pltpu.SemaphoreType.DMA((slab // 4,))],
        name="write_outputs",
        compiler_params=pltpu.CompilerParams(vmem_limit_bytes=4 * 2**20),
    )(*(pltpu.with_memory_space_constraint(x, pltpu.VMEM) for x in (image, parts, total)))


def on_device(residual, psf, positions):
    nchan, nrows = lax.axis_size("chan"), lax.axis_size("rows")
    slab, ncols = residual.shape[1:]
    shard, patch = psf.shape[1:]
    steps = positions.shape[0]
    central = slab * nrows == shard and shard * nrows == patch
    powers = all(n & (n - 1) == 0 for n in (slab, shard, patch)) and patch >= LANES
    lines = nchan == 4 and nrows == 8 and slab == 32 and ncols % (16 * LANES) == 0 and ncols <= LANES * LANES
    if not (central and powers and lines and steps % 8 == 0 and steps <= LANES and patch < LANES * LANES):
        return on_any_device(residual, psf, positions)
    image, parts, total = run_cycle(nchan, nrows, positions.T, residual, psf)
    return write_outputs(slab * nrows * ncols, slab, image, parts, total)


def on_any_device(residual, psf, positions):
    chan_id = lax.axis_index("chan")
    nchan = lax.axis_size("chan")
    row_id = lax.axis_index("rows")
    nrows = lax.axis_size("rows")
    slab = residual.shape[1]
    ncols = residual.shape[2]
    own_psf = psf[0]
    shard_rows = own_psf.shape[0]
    patch = own_psf.shape[1]
    half = patch // 2
    first = row_id * slab
    chan_hot = (jnp.arange(nchan) == chan_id).astype(jnp.float32)
    full_psf = lax.all_gather(own_psf, "rows", axis=0, tiled=True)
    padded_psf = jnp.pad(full_psf, ((slab, slab), (0, 0)))
    zero = jnp.int32(0)

    def subtract(image, row, col, amount):
        offset = first - row + half
        touches = jnp.logical_and(offset > -slab, offset < patch)
        start = jnp.clip(offset + slab, 0, patch + slab)
        psf_rows = lax.dynamic_slice(padded_psf, (start, zero), (slab, patch))
        window = lax.dynamic_slice(image, (zero, col - half), (slab, patch))
        scale = jnp.where(touches, amount, 0.0)
        return lax.dynamic_update_slice(image, window - scale * psf_rows, (zero, col - half))

    image = residual[0]
    peak_rows = positions[:, 0]
    peak_cols = positions[:, 1]
    inside = jnp.logical_and(peak_rows >= first, peak_rows < first + slab)
    local_rows = jnp.clip(peak_rows - first, 0, slab - 1)
    start_values = jnp.where(inside, image[local_rows, peak_cols], 0.0)
    row_offset = peak_rows[:, None] - peak_rows[None, :] + half - row_id * shard_rows
    col_offset = peak_cols[:, None] - peak_cols[None, :] + half
    owned = (row_offset >= 0) & (row_offset < shard_rows) & (col_offset >= 0) & (col_offset < patch)
    couple = own_psf[jnp.clip(row_offset, 0, shard_rows - 1), jnp.clip(col_offset, 0, patch - 1)]
    couple = jnp.where(owned, couple, 0.0)
    start_table, couple_table = lax.psum(
        (chan_hot[:, None] * start_values[None, :], chan_hot[:, None, None] * couple[None, :, :]),
        ("chan", "rows"),
    )

    def solve(k, amps):
        taken = jnp.sum(amps * lax.dynamic_index_in_dim(couple_table, k, 1, False), axis=1)
        value = lax.dynamic_index_in_dim(start_table, k, 1, False) - taken
        amp = 0.25 * (value + jnp.sum(value) / nchan)
        return lax.dynamic_update_index_in_dim(amps, amp, k, 1)

    amps = lax.fori_loop(0, STEPS, solve, jnp.zeros((nchan, STEPS), jnp.float32))
    own_amps = jnp.sum(chan_hot[:, None] * amps, axis=0)

    def apply(k, image):
        return subtract(image, positions[k, 0], positions[k, 1], own_amps[k])

    image = lax.fori_loop(0, STEPS, apply, image)
    count = slab * nrows * ncols
    parts = lax.psum_scatter(image, "chan", scatter_dimension=1, tiled=True)
    total = lax.psum(jnp.sum(parts * parts), ("chan", "rows"))
    normalized = parts * lax.rsqrt(total / count + 1e-06)
    return (image[None], normalized)


def solution(mesh):
    return jax.shard_map(
        on_device,
        mesh=mesh,
        in_specs=(P("chan", "rows", None), P("chan", "rows", None), P()),
        out_specs=(P("chan", "rows", None), P("rows", "chan")),
        check_vma=False,
    )
```

```python
import functools

import jax
import jax.numpy as jnp
from jax import lax
from jax.experimental import pallas as pl
from jax.experimental.pallas import tpu as pltpu
from jax.sharding import PartitionSpec as P

STEPS = 32
LANES = 128
MESH = pl.DeviceIdType.MESH
OUT = pltpu.VMEM
VMEM = 67043328


def pick(tile, row, col, lane_to, owned, number, acc):
    moved = pltpu.roll(tile, (lane_to - col) & (LANES - 1), 1)
    target = jnp.where(owned, (row & 7) * LANES + lane_to, -1)
    return jnp.where(number == target, moved, acc)


def cycle_kernel(nchan, nrows, pos, res, psf, image, parts, total_out,
                 work, land, patch_v, psf_v, grid, couple_v, couple_in, start_v, start_in, tables, amps_v, prev_v, last_v,
                 first_far, first_own, passed, second, squares, changes, pair_v, sum_v, prev_s, last_s, amps_s, pair_s,
                 ready, band_sem, psf_sem, index_sem, send_sem, unit_recv, recv_sem, relay_sem, fine_send, fine_recv, fine_relay,
                 start_send, start_recv, couple_send, couple_recv, table_send, table_recv, amp_send, amp_recv,
                 far_send, far_recv, own_send, own_recv, pass_send, pass_recv, square_send, square_recv, guest_sem, lent_send, lent_recv):
    chan, row = lax.axis_index("chan"), lax.axis_index("rows")
    chip, core = row // 2, row % 2
    partner = row + 1 - 2 * core
    nchips = nrows // 2
    side = chip // (nchips // 2)
    slab, ncols = res.shape[1], res.shape[2]
    shard, patch = psf.shape[1:]
    half, steps, chunks = patch // 2, pos.shape[1], patch // LANES
    unit, tiles, blocks = 2 * slab, slab // 8, ncols // LANES
    base, width = blocks + 1, chunks + 1
    first = row * slab
    begins_at = [z - (1 if z == (nchips - 1) // 2 else 0) for z in range(nchips)]
    lead = jnp.where(chip == (nchips - 1) // 2, 1, 0)
    roots = (nchips - 1, nchips)
    solvers = (roots[0] ^ 1, roots[1] ^ 1)
    is_root = jnp.logical_or(row == roots[0], row == roots[1])
    is_solver = jnp.logical_or(row == solvers[0], row == solvers[1])
    is_mid = jnp.logical_or(is_root, is_solver)
    is_end = jnp.logical_not(is_mid)
    lane = lax.broadcasted_iota(jnp.int32, (1, LANES), 1)
    lane8 = lax.broadcasted_iota(jnp.int32, (8, LANES), 1)
    number = lax.broadcasted_iota(jnp.int32, (8, LANES), 0) * LANES + lane8
    zero = jnp.zeros((8, LANES), jnp.float32)

    def block_at(index):
        return pl.ds(pl.multiple_of(index * LANES, LANES), LANES)

    def flip(bit):
        if bit == 1:
            return chan + 1 - 2 * (chan % 2)
        return (chan + 2) % 4

    barrier = pltpu.get_barrier_semaphore()
    for bit in (1, 2):
        pl.semaphore_signal(barrier, inc=1, device_id=(flip(bit), row), device_id_type=MESH)
    pl.semaphore_signal(barrier, inc=1, device_id=(chan, partner), device_id_type=MESH)

    @pl.when(chip > 0)
    def _():
        for c in range(2):
            pl.semaphore_signal(barrier, inc=1, device_id=(chan, 2 * chip - 2 + c), device_id_type=MESH)

    @pl.when(chip < nchips - 1)
    def _():
        for c in range(2):
            pl.semaphore_signal(barrier, inc=1, device_id=(chan, 2 * chip + 2 + c), device_id_type=MESH)

    bands = [pltpu.make_async_copy(res.at[0, pl.ds(8 * t, 8)], image.at[pl.ds(8 * t, 8)], band_sem.at[t]) for t in range(tiles)]
    for copy in bands:
        copy.start()
    loads = [pltpu.make_async_copy(psf.at[0, :, pl.ds(c * LANES, LANES)], psf_v.at[pl.ds(c * shard, shard)], psf_sem.at[c]) for c in range(chunks)]

    @pl.when(is_root)
    def _():
        for copy in loads:
            copy.start()

    begins = [jnp.clip(pos[1, k] - half, 0, ncols - patch) >> 7 for k in range(steps)]
    krow = lax.broadcasted_iota(jnp.int32, (steps, LANES), 0)
    target = jnp.zeros((steps, LANES), jnp.int32)
    for k in range(steps):
        target = jnp.where(krow == k, begins[k], target)
    target = target + lax.broadcasted_iota(jnp.int32, (steps, LANES), 1)
    prev, last = target, lane8
    for k in range(steps):
        inside = target - begins[k]
        prev = jnp.where((inside >= 0) & (inside < width) & (krow > k), inside + (base + width * k), prev)
        inside = lane8 - begins[k]
        last = jnp.where((inside >= 0) & (inside < width), inside + (base + width * k), last)
    prev_v[...] = prev
    last_v[...] = last
    lane32 = lax.broadcasted_iota(jnp.int32, (steps, LANES), 1)
    rows_from = jnp.zeros((steps, LANES), jnp.int32)
    cols_from = jnp.zeros((steps, LANES), jnp.int32)
    for k in range(steps):
        rows_from = rows_from + jnp.where(krow == k, pos[0, k], 0) - jnp.where(lane32 == k, pos[0, k], 0)
        cols_from = cols_from + jnp.where(krow == k, pos[1, k], 0) - jnp.where(lane32 == k, pos[1, k], 0)
    rows_from = rows_from + half - row * shard
    cols_from = cols_from + half
    owned = (rows_from >= 0) & (rows_from < shard) & (cols_from >= 0) & (cols_from < patch) & (lane32 < krow)
    pair_v[0] = ((cols_from >> 7) & (chunks - 1)) * shard + (((rows_from >> 3) << 3) & (shard - 1))
    pair_v[1] = (lane32 - cols_from) & (LANES - 1)
    pair_v[2] = jnp.where(owned, (rows_from & 7) * LANES + lane32, -1)
    pair_copy = pltpu.make_async_copy(pair_v, pair_s, index_sem.at[3])

    @pl.when(is_root)
    def _():
        pair_copy.start()

    index_copies = [pltpu.make_async_copy(prev_v, prev_s, index_sem.at[0]), pltpu.make_async_copy(last_v, last_s, index_sem.at[1])]
    for copy in index_copies:
        copy.start()
    for t in range(tiles):
        work[t, blocks] = zero

    @pl.when(is_end)
    def _():
        pl.semaphore_wait(barrier, 5)

    @pl.when(is_mid)
    def _():
        pl.semaphore_wait(barrier, 7)


    def bulk(s):
        mid, end, other = (nchips - 1 + s) // 2, (nchips - 1) * s, nchips // 2 - s
        order = (0, 1) if s == 0 else (1, 0)
        near = list(range(nchips)) if s == 0 else list(range(2 * nchips - 1, nchips - 1, -1))
        across = [nchips - 1 - n if s == 0 else nchips + n for n in range(nchips // 2)]
        local = range(s * nchips, (s + 1) * nchips)
        out = []

        def add(u, z, h, rows, to_row, sem):
            out.append(pltpu.make_async_remote_copy(
                src_ref=psf.at[0, pl.ds((u % nchips) * unit + h * slab, rows)], dst_ref=land.at[pl.ds((u - begins_at[z]) * unit + h * slab, rows)],
                send_sem=send_sem.at[len(out)], recv_sem=sem, device_id=(chan, to_row), device_id_type=MESH))

        for u in near:
            for h in order:
                add(u, end, h, slab, 2 * end + (s if u == near[-1] else h), recv_sem.at[u - begins_at[end], h])
        for u in across:
            for h in range(2):
                add(u, other, h, slab, 2 * other + h, recv_sem.at[u - begins_at[other], h])
        for u in local:
            add(u, mid, 0, unit, solvers[s], unit_recv.at[u - begins_at[mid]])
        return out

    for s in range(2):
        @pl.when(row == roots[s])
        def _(s=s):
            for copy in bulk(s):
                copy.start()

    early = core == side
    is_lead, is_trail = is_end & early, is_end & jnp.logical_not(early)
    doubled = is_mid & jnp.logical_not(early)
    sends = jnp.where(is_end, jnp.where(early, tiles - 1, tiles - 2), jnp.where(early, tiles + 1, tiles + 2))

    def tile_at(i):
        return jnp.where(side == 0, i, tiles - 1 - i)

    def tile_rows(t):
        return pl.ds(pl.multiple_of(8 * t, 8), 8)

    def guest_tile(g):
        return tile_at(jnp.where(early, tiles - 1, tiles - 2 + g))

    head = ncols // 4

    def lent(g, part):
        width = (head, ncols - head)[part]
        return pltpu.make_async_remote_copy(
            src_ref=res.at[0, tile_rows(guest_tile(g)), pl.ds(head * part, width)],
            dst_ref=image.at[tile_rows(tiles + g), pl.ds(head * part, width)],
            send_sem=lent_send.at[g, part], recv_sem=lent_recv.at[g, part], device_id=(chan, row + 2 - 4 * side), device_id_type=MESH)

    def given(g):
        return pltpu.make_async_remote_copy(
            src_ref=parts.at[tile_rows(tiles + g)], dst_ref=parts.at[tile_rows(guest_tile(g))], send_sem=guest_sem.at[g], recv_sem=guest_sem.at[2 + g],
            device_id=(chan, row - 2 + 4 * side), device_id_type=MESH)

    @pl.when(is_end)
    def _():
        lent(0, 0).start()

    for bit in (1, 2):
        pl.semaphore_signal(ready.at[0], inc=1, device_id=(flip(bit), row), device_id_type=MESH)

    for copy in bands:
        copy.wait()

    def spread_out(b, carry):
        for t in range(tiles):
            work[t, b] = image[pl.ds(8 * t, 8), block_at(b)]
        return carry

    lax.fori_loop(0, blocks, spread_out, 0, unroll=4)
    acc = zero
    for k in range(steps):
        r, c = pos[0, k] - first, pos[1, k]
        tile = work[(r >> 3) & (tiles - 1), c >> 7]
        acc = pick(tile, r, c, k, (r >= 0) & (r < slab), number, acc)
    start_v[...] = acc

    def start_copy(s, source):
        return pltpu.make_async_remote_copy(
            src_ref=start_v, dst_ref=start_in.at[source], send_sem=start_send, recv_sem=start_recv.at[source],
            device_id=(chan, solvers[s]), device_id_type=MESH)

    def couple_copy(s):
        return pltpu.make_async_remote_copy(
            src_ref=couple_v, dst_ref=couple_in, send_sem=couple_send, recv_sem=couple_recv,
            device_id=(chan, solvers[s]), device_id_type=MESH)

    for s in range(2):
        @pl.when((side == s) & (row != solvers[s]))
        def _(s=s):
            start_copy(s, row).start()

    @pl.when(is_end)
    def _():
        lent(0, 1).start()

    @pl.when(is_trail)
    def _():
        for part in range(2):
            lent(1, part).start()

    @pl.when(is_root)
    def _():
        for copy in loads:
            copy.wait()
        pair_copy.wait()

        def fill(count, k, carry):
            acc = zero
            for j in range(count):
                tile = psf_v[pl.ds(pair_s[0, k, j], 8), :]
                acc = jnp.where(number == pair_s[2, k, j], pltpu.roll(tile, pair_s[1, k, j], 1), acc)
            grid[k] = acc
            return carry

        for g in range(steps // 8):
            lax.fori_loop(8 * g, 8 * g + 8, functools.partial(fill, 8 * g + 8), 0)
        couple_v[...] = jnp.sum(grid[...], axis=1)

    for s in range(2):
        @pl.when(row == roots[s])
        def _(s=s):
            couple_copy(s).start()

    def held(m, h, rows=slab):
        return land.at[pl.ds(pl.multiple_of(m * unit + h * slab, 8), rows)]

    def relay(m):
        return pltpu.make_async_remote_copy(
            src_ref=held(m, core), dst_ref=held(m, core), send_sem=relay_sem.at[m], recv_sem=recv_sem.at[m, core],
            device_id=(chan, partner), device_id_type=MESH)

    def arrival(m, h):
        return pltpu.make_async_remote_copy(
            src_ref=held(m, h), dst_ref=held(m, h), send_sem=relay_sem.at[m], recv_sem=recv_sem.at[m, h],
            device_id=(chan, partner), device_id_type=MESH)

    def pass_on(m):
        arrival(m, core).wait_recv()
        relay(m).start()

    def crossed(n):
        return jnp.where(side == 0, nchips + n, 1 - n)

    def streamed(n):
        return jnp.where(side == 0, n, nchips - n)

    def relayout(source, source_row, dest_row, rows):
        def body(g, carry):
            take, put = pl.multiple_of(source_row + 8 * g, 8), pl.multiple_of(dest_row + 8 * g, 8)
            for c in range(chunks):
                narrow = source.shape[1] == LANES
                tile = source[pl.ds(pl.multiple_of(c * shard + take, 8), 8), :] if narrow else source[pl.ds(take, 8), pl.ds(c * LANES, LANES)]
                patch_v[c, pl.ds(put, 8), :] = tile
            return carry

        lax.fori_loop(0, rows // 8, body, 0)

    @pl.when(is_root)
    def _():
        pass_on(crossed(0))

    pl.semaphore_wait(ready.at[0], 2)
    for bit in (1, 2):
        pl.semaphore_signal(ready.at[1], inc=1, device_id=(flip(bit), row), device_id_type=MESH)
    pl.semaphore_wait(ready.at[1], 2)
    me_table = 2 * chan + side

    def table_copy(step):
        other = (me_table + step) % (2 * nchan)
        return pltpu.make_async_remote_copy(
            src_ref=tables.at[me_table], dst_ref=tables.at[me_table], send_sem=table_send.at[step], recv_sem=table_recv.at[step],
            device_id=(other // 2, solvers[0] + (other % 2) * (solvers[1] - solvers[0])), device_id_type=MESH)

    def table_arrival(step):
        other = (me_table + 2 * nchan - step) % (2 * nchan)
        return pltpu.make_async_remote_copy(
            src_ref=tables.at[other], dst_ref=tables.at[other], send_sem=table_send.at[step], recv_sem=table_recv.at[step],
            device_id=(other // 2, solvers[0] + (other % 2) * (solvers[1] - solvers[0])), device_id_type=MESH)

    for s in range(2):
        @pl.when(row == solvers[s])
        def _(s=s):
            total = start_v[...]
            for source in range(s * nchips, (s + 1) * nchips):
                if source != solvers[s]:
                    start_copy(s, source).wait_recv()
                    total = total + start_in[source]
            couple_copy(s).wait_recv()
            tables[me_table, pl.ds(0, steps), :] = couple_in[...]
            tables[me_table, pl.ds(steps, 8), :] = jnp.broadcast_to(jnp.sum(total, axis=0, keepdims=True), total.shape)
            for step in range(1, 2 * nchan):
                table_copy(step).start()
            pass_on(crossed(0))

    def amp_copy(n):
        return pltpu.make_async_remote_copy(
            src_ref=amps_v, dst_ref=amps_v, send_sem=amp_send.at[n], recv_sem=amp_recv,
            device_id=(chan, side * nchips + (row + n) % nchips), device_id_type=MESH)

    @pl.when(is_solver)
    def _():
        for step in range(1, 2 * nchan):
            table_arrival(step).wait_recv()

        def rows_of(index):
            return jnp.concatenate([tables[2 * c, pl.ds(index, 1), :] + tables[2 * c + 1, pl.ds(index, 1), :] for c in range(nchan)], axis=0)

        start = rows_of(steps)

        def solve(k, amps):
            value = jnp.sum(jnp.where(lane == k, start, 0.0) - amps * rows_of(k), axis=1, keepdims=True)
            amp = 0.25 * (value + jnp.sum(value, axis=0, keepdims=True) / nchan)
            return jnp.where(lane == k, amp, amps)

        amps = lax.fori_loop(0, steps, solve, jnp.zeros((nchan, LANES), jnp.float32), unroll=4)
        amps_v[pl.ds(0, nchan), :] = amps
        amps_v[pl.ds(nchan, 8 - nchan), :] = jnp.zeros((8 - nchan, LANES), jnp.float32)
        for n in range(1, nchips):
            amp_copy(n).start()

    def fine_piece(n):
        return jnp.where(side == 0, n, 2 * tiles - 1 - n)

    def fine_at(n):
        return pl.multiple_of(jnp.where(side == 0, nchips, 0) * unit + 8 * fine_piece(n), 8)

    def onward_piece(s, n):
        mid, end = (nchips - 1 + s) // 2, (nchips - 1) * s
        u = nchips - s
        j = n if s == 0 else 2 * tiles - 1 - n
        return pltpu.make_async_remote_copy(
            src_ref=land.at[pl.ds((u - begins_at[mid]) * unit + 8 * j, 8)], dst_ref=land.at[pl.ds((u - begins_at[end]) * unit + 8 * j, 8)],
            send_sem=fine_send.at[n], recv_sem=fine_recv.at[n], device_id=(chan, 2 * end + (s if n == 0 else 1 - s)), device_id_type=MESH)

    def fine_copy(n):
        return pltpu.make_async_remote_copy(
            src_ref=land.at[pl.ds(fine_at(n), 8)], dst_ref=land.at[pl.ds(fine_at(n), 8)],
            send_sem=fine_relay.at[n], recv_sem=fine_recv.at[n], device_id=(chan, partner), device_id_type=MESH)

    for s in range(2):
        offset = s * nchips - begins_at[(nchips - 1 + s) // 2]

        @pl.when(row == roots[s])
        def _(s=s, offset=offset):
            arrival(crossed(0), 1 - core).wait_recv()
            for n in range(2 * tiles):
                onward_piece(s, n).start()
            relayout(psf_v, 0, offset * unit, nchips * unit)

        @pl.when(row == solvers[s])
        def _(s=s, offset=offset):
            arrival(crossed(0), 1 - core).wait_recv()
            for u in range(nchips):
                pltpu.make_async_remote_copy(
                    src_ref=held(u + offset, 0, unit), dst_ref=held(u + offset, 0, unit), send_sem=send_sem.at[0], recv_sem=unit_recv.at[u + offset],
                    device_id=(chan, partner), device_id_type=MESH).wait_recv()
            relayout(land, offset * unit, offset * unit, nchips * unit)

    def relayout_crossed(n):
        begin = pl.multiple_of(crossed(n) * unit, 8)
        relayout(land, begin, begin, unit)

    @pl.when(is_mid)
    def _():
        relayout_crossed(0)

    amps_copy = pltpu.make_async_copy(amps_v, amps_s, index_sem.at[2])
    leading = early

    def half_unit(m, h):
        begin = pl.multiple_of(m * unit + h * slab, 8)
        relayout(land, begin, begin, slab)

    def relay_half(m, h):
        return pltpu.make_async_remote_copy(
            src_ref=held(m, h), dst_ref=held(m, h), send_sem=relay_sem.at[nchips + 2 + h], recv_sem=recv_sem.at[m, h],
            device_id=(chan, partner), device_id_type=MESH)

    @pl.when(is_end)
    def _():
        for n in range(nchips - 1):
            pass_on(streamed(n))
            if n > 0:
                arrival(streamed(n - 1), 1 - core).wait_recv()
                for h in range(2):
                    half_unit(streamed(n - 1), h)
        amp_copy(1).wait_recv()
        amps_copy.start()
        arrival(streamed(nchips - 2), 1 - core).wait_recv()
        for h in range(2):
            half_unit(streamed(nchips - 2), h)

    @pl.when(is_end & leading)
    def _():
        for n in range(2):
            h = jnp.where(side == 0, n, 1 - n)
            arrival(streamed(nchips - 1), h).wait_recv()
            relay_half(streamed(nchips - 1), h).start()
            half_unit(streamed(nchips - 1), h)

    @pl.when(is_end & jnp.logical_not(leading))
    def _():
        for n in range(2):
            h = jnp.where(side == 0, n, 1 - n)
            arrival(streamed(nchips - 1), h).wait_recv()
            half_unit(streamed(nchips - 1), h)

    @pl.when(is_root)
    def _():
        amp_copy(1).wait_recv()

    @pl.when(is_mid)
    def _():
        amps_copy.start()

    for copy in index_copies:
        copy.wait()
    amps_copy.wait()

    cols = ncols // nchan
    span = cols // 2
    bits = ((1, 2), (2, 1))

    diagonal = 3 - chan

    def is_guest(n):
        return (n == 0) | (doubled & (n == 2))

    def own_index(n):
        return jnp.where(is_mid, n - 1 - jnp.where(doubled & (n > 2), 1, 0), n)

    def tile_of(n):
        return jnp.where(is_mid & is_guest(n), tiles + n // 2, tile_at(own_index(n)))

    def rows_at(n):
        return tile_rows(tile_of(n))

    def lift_of(n):
        own_lift = lead * unit + 8 * tile_at(own_index(n))
        guest_lift = side * unit + 8 * guest_tile(n // 2)
        return slab * nrows + core * slab + jnp.where(is_mid & is_guest(n), guest_lift, own_lift)

    def cols_at(c, p):
        return pl.ds(pl.multiple_of(c * cols + p * span, LANES), span)

    def send(i, p, source, dest, send_sem, recv_sem, to):
        return pltpu.make_async_remote_copy(
            src_ref=source, dst_ref=dest.at[i, p], send_sem=send_sem.at[i, p], recv_sem=recv_sem.at[i, p],
            device_id=(to, row), device_id_type=MESH)

    def far(i, p):
        return send(i, p, image.at[rows_at(i), cols_at(diagonal, p)], first_far, far_send, far_recv, flip(bits[p][0]))

    def mine(i, p):
        return send(i, p, image.at[rows_at(i), cols_at(flip(bits[p][0]), p)], first_own, own_send, own_recv, flip(bits[p][0]))

    def onward(i, p):
        return send(i, p, passed.at[i, p], second, pass_send, pass_recv, flip(bits[p][1]))

    def fetch(n):
        fine_copy(n).wait_recv()

    def arrive(n):
        fetch(n)
        relayout(land, fine_at(n), fine_at(n), 8)

    def share(n):
        fetch(n)
        fine_copy(n).start()
        relayout(land, fine_at(n), fine_at(n), 8)

    def scale_and_shift(i):
        lift = lift_of(i)

        def eight(g, carry):
            for n in range(8):
                k = 8 * g + n
                amp = amps_s[chan, k]
                begin = lift - pos[0, k]
                shift = (pos[1, k] - half) & (LANES - 1)
                keep = lane8 < shift
                moved = [zero] + [pltpu.roll(patch_v[c, pl.ds(begin, 8), :] * amp, shift, 1) for c in range(chunks)] + [zero]
                for m in range(width):
                    changes[width * k + m] = jnp.where(keep, moved[m], moved[m + 1])
            return carry

        lax.fori_loop(0, steps // 8, eight, 0)

    def subtract(i):
        t = tile_of(i)

        def eight(g, carry):
            for n in range(8):
                k = 8 * g + n
                after = [work[t, prev_s[k, m]] - changes[width * k + m] for m in range(width)]
                for m in range(width):
                    work[t, base + width * k + m] = after[m]
            return carry

        lax.fori_loop(0, steps // 8, eight, 0)

    def finalize(i, c):
        rows = rows_at(i)
        per = cols // LANES

        def body(g, carry):
            for n in range(8):
                b = c * per + g * 8 + n
                image[rows, block_at(b)] = work[tile_of(i), last_s[0, b]]
            return carry

        lax.fori_loop(0, per // 8, body, 0)

    def combine(i):
        for p in range(2):
            far(i, p).wait_recv()
            passed[i, p] = image[rows_at(i), cols_at(flip(bits[p][1]), p)] + first_far[i, p]
            onward(i, p).start()

    def own(n):
        for p in range(2):
            mine(n, p).wait_recv()
            onward(n, p).wait_recv()
            value = image[rows_at(n), cols_at(chan, p)] + first_own[n, p] + second[n, p]
            parts[rows_at(n), pl.ds(p * span, span)] = value
            square = value * value
            total = zero
            for c in range(span // LANES):
                total = total + square[:, c * LANES:(c + 1) * LANES]
            sum_v[...] = sum_v[...] + total

    def start_far(n):
        for p in range(2):
            far(n, p).start()

    def start_mine(n):
        for p in range(2):
            mine(n, p).start()

    def finish(n):
        for p in range(2):
            finalize(n, flip(bits[p][0]))
        finalize(n, chan)

    sum_v[...] = zero

    def advance(n, carry):
        active = n < sends

        @pl.when(is_lead & (n == 0))
        def _():
            share(0)

        @pl.when(is_lead & (n > 0) & active)
        def _():
            arrive(n)

        @pl.when(is_trail & (n == 0))
        def _():
            arrive(0)
            for piece in range(1, tiles):
                share(piece)

        @pl.when(is_trail & active)
        def _():
            arrive(tiles + n)

        @pl.when(is_mid & is_guest(n))
        def _():
            for part in range(2):
                lent(n // 2, part).wait_recv()

            def guest(b, carry):
                work[tiles + n // 2, b] = image[tile_rows(tiles + n // 2), block_at(b)]
                return carry

            lax.fori_loop(0, blocks, guest, 0, unroll=4)

        @pl.when(is_mid & (n == 1))
        def _():
            arrival(crossed(1), 1 - core).wait_recv()
            relayout_crossed(1)

        @pl.when(active)
        def _():
            scale_and_shift(n)

        @pl.when(is_mid & (n == 0))
        def _():
            pass_on(crossed(1))

        @pl.when(n == sends)
        def _():
            combine(n - 1)

        @pl.when(active)
        def _():
            subtract(n)
            finalize(n, diagonal)

        @pl.when(n < sends)
        def _():
            start_far(n)

        @pl.when(active)
        def _():
            finish(n)

        @pl.when(is_end & (n < sends))
        def _():
            start_mine(n)

        @pl.when((n > 0) & (n < sends))
        def _():
            combine(n - 1)

        @pl.when(is_mid & (n < sends))
        def _():
            start_mine(n)

        @pl.when(is_mid & (n == 4))
        def _():
            own(0)
            given(0).start()

        @pl.when(doubled & (n == 5))
        def _():
            own(2)
            given(1).start()

        return carry

    lax.fori_loop(0, tiles + 3, advance, 0)

    def settle(n, carry):
        @pl.when((n < sends) & jnp.logical_not(is_mid & is_guest(n)))
        def _():
            own(n)

        return carry

    lax.fori_loop(0, tiles + 2, settle, 0)
    total = sum_v[...]
    me = row * nchan + chan
    squares[pl.ds(me, 1), :] = jnp.sum(total, axis=0, keepdims=True)

    everyone = nrows * nchan

    def spread(step):
        other = (me + jnp.where(side == 0, everyone - step, step)) % everyone
        return pltpu.make_async_remote_copy(
            src_ref=squares.at[pl.ds(me, 1)], dst_ref=squares.at[pl.ds(me, 1)], send_sem=square_send.at[step], recv_sem=square_recv.at[me],
            device_id=(other % nchan, other // nchan), device_id_type=MESH)

    def arrived(step):
        other = (me + step) % everyone
        return pltpu.make_async_remote_copy(
            src_ref=squares.at[pl.ds(other, 1)], dst_ref=squares.at[pl.ds(other, 1)], send_sem=square_send.at[step], recv_sem=square_recv.at[other],
            device_id=(other % nchan, other // nchan), device_id_type=MESH)

    for step in range(1, nrows * nchan):
        spread(step).start()

    def leftover(n, carry):
        @pl.when(is_end & (n >= sends))
        def _():
            arrive(jnp.where(early, n, tiles + n))
            scale_and_shift(n)
            subtract(n)
            finalize(n, diagonal)
            finish(n)

        return carry

    lax.fori_loop(tiles - 2, tiles, leftover, 0)

    for s in range(2):
        @pl.when(row == roots[s])
        def _(s=s):
            for copy in bulk(s):
                copy.wait_send()
            for n in range(2 * tiles):
                onward_piece(s, n).wait_send()
            couple_copy(s).wait_send()

    @pl.when(is_mid)
    def _():
        for n in range(2):
            relay(crossed(n)).wait_send()

    @pl.when(is_end)
    def _():
        for n in range(nchips - 1):
            relay(streamed(n)).wait_send()

    @pl.when(is_end & leading)
    def _():
        for h in range(2):
            relay_half(streamed(nchips - 1), h).wait_send()
        fine_copy(0).wait_send()

    @pl.when(is_trail)
    def _():
        for n in range(1, tiles):
            fine_copy(n).wait_send()

    @pl.when(is_solver)
    def _():
        for step in range(1, 2 * nchan):
            table_copy(step).wait_send()
        for n in range(1, nchips):
            amp_copy(n).wait_send()

    @pl.when(jnp.logical_not(is_solver))
    def _():
        start_copy(0, row).wait_send()

    def sent(n, carry):
        @pl.when(n < sends)
        def _():
            for p in range(2):
                far(n, p).wait_send()
                mine(n, p).wait_send()
                onward(n, p).wait_send()

        return carry

    lax.fori_loop(0, tiles + 2, sent, 0)

    @pl.when(is_mid)
    def _():
        given(0).wait_send()

    @pl.when(doubled)
    def _():
        given(1).wait_send()

    @pl.when(is_end)
    def _():
        for part in range(2):
            lent(0, part).wait_send()
        given(0).wait_recv()

    @pl.when(is_trail)
    def _():
        for part in range(2):
            lent(1, part).wait_send()
        given(1).wait_recv()

    for step in range(1, nrows * nchan):
        spread(step).wait_send()
    for step in range(1, nrows * nchan):
        arrived(step).wait_recv()
    everything = jnp.sum(jnp.sum(squares[...], axis=0, keepdims=True), axis=1, keepdims=True)
    total_out[...] = jnp.broadcast_to(everything, total_out.shape)


def run_cycle(nchan, nrows, positions, residual, psf):
    slab, ncols = residual.shape[1:]
    shard, patch = psf.shape[1:]
    steps, chunks = positions.shape[1], patch // LANES
    nchips, tiles, cols = nrows // 2, slab // 8, ncols // nchan
    rows = slab * (nrows + 4)
    dma, f32, i32 = pltpu.SemaphoreType.DMA, jnp.float32, jnp.int32
    anywhere = pl.BlockSpec(memory_space=pl.ANY)
    vmem = pl.BlockSpec(memory_space=pltpu.VMEM)
    slots = ncols // LANES + 1 + (chunks + 1) * steps
    stage = pltpu.VMEM((tiles + 2, 2, 8, cols // 2), f32)
    small = pltpu.VMEM((8, LANES), f32)
    return pl.pallas_call(
        functools.partial(cycle_kernel, nchan, nrows),
        out_shape=(OUT((slab + 16, ncols), f32), OUT((slab + 16, cols), f32), OUT((8, LANES), f32)),
        in_specs=[pl.BlockSpec(memory_space=pltpu.SMEM), anywhere, anywhere],
        out_specs=(vmem, vmem, vmem),
        scratch_shapes=[
            pltpu.VMEM((tiles + 2, slots, 8, LANES), f32), pltpu.VMEM((rows, patch), f32), pltpu.VMEM((chunks, rows, LANES), f32),
            pltpu.VMEM((chunks * shard, LANES), f32), pltpu.VMEM((steps, 8, LANES), f32), pltpu.VMEM((steps, LANES), f32),
            pltpu.VMEM((steps, LANES), f32), small, pltpu.VMEM((nrows, 8, LANES), f32),
            pltpu.VMEM((2 * nchan, steps + 8, LANES), f32), small, pltpu.VMEM((steps, LANES), i32), pltpu.VMEM((8, LANES), i32),
            stage, stage, stage, stage, pltpu.VMEM((nrows * nchan, LANES), f32), pltpu.VMEM(((chunks + 1) * steps, 8, LANES), f32), pltpu.VMEM((3, steps, LANES), i32), small,
            pltpu.SMEM((steps, LANES), i32), pltpu.SMEM((8, LANES), i32), pltpu.SMEM((8, LANES), f32), pltpu.SMEM((3, steps, LANES), i32),
            pltpu.SemaphoreType.REGULAR((2,)), dma((tiles,)), dma((chunks,)), dma((4,)), dma((4 * nchips,)), dma((nchips + 2,)),
            dma((nchips + 2, 2)), dma((nchips + 4,)), dma((2 * tiles,)), dma((2 * tiles,)), dma((2 * tiles,)),
            dma, dma((nrows,)), dma, dma, dma((2 * nchan,)), dma((2 * nchan,)), dma((nchips,)), dma,
        ] + [dma((tiles + 2, 2))] * 6 + [dma((nrows * nchan,))] * 2 + [dma((4,)), dma((2, 2)), dma((2, 2))],
        compiler_params=pltpu.CompilerParams(collective_id=0, has_side_effects=True, vmem_limit_bytes=VMEM - 4 * ((slab + 16) * (ncols + cols) + 8 * LANES)),
        name="minor_cycle",
    )(positions, residual, psf)


def write_kernel(count, image, parts, total, image_out, normalized, scaled, sems):
    slab, tiles = scaled.shape[0], scaled.shape[0] // 8
    copies = [pltpu.make_async_copy(image.at[pl.ds(8 * t, 8)], image_out.at[0, pl.ds(8 * t, 8)], sems.at[t]) for t in range(tiles)]
    for copy in copies:
        copy.start()
    scale = lax.rsqrt(total[0:1, 0:1] / count + 1e-06)
    for t in range(tiles):
        rows = pl.ds(8 * t, 8)
        scaled[rows, :] = parts[rows, :] * scale
        copies.append(pltpu.make_async_copy(scaled.at[rows], normalized.at[rows], sems.at[tiles + t]))
        copies[-1].start()
    for copy in copies:
        copy.wait()


def write_outputs(count, slab, image, parts, total):
    f32, ncols, cols = jnp.float32, image.shape[1], parts.shape[1]
    anywhere, vmem = pl.BlockSpec(memory_space=pl.ANY), pl.BlockSpec(memory_space=pltpu.VMEM)
    return pl.pallas_call(
        functools.partial(write_kernel, count),
        out_shape=(jax.ShapeDtypeStruct((1, slab, ncols), f32), jax.ShapeDtypeStruct((slab, cols), f32)),
        in_specs=[vmem, vmem, vmem],
        out_specs=(anywhere, anywhere),
        scratch_shapes=[pltpu.VMEM((slab, cols), f32), pltpu.SemaphoreType.DMA((slab // 4,))],
        name="write_outputs",
        compiler_params=pltpu.CompilerParams(vmem_limit_bytes=4 * 2**20),
    )(*(pltpu.with_memory_space_constraint(x, pltpu.VMEM) for x in (image, parts, total)))


def on_device(residual, psf, positions):
    nchan, nrows = lax.axis_size("chan"), lax.axis_size("rows")
    slab, ncols = residual.shape[1:]
    shard, patch = psf.shape[1:]
    steps = positions.shape[0]
    central = slab * nrows == shard and shard * nrows == patch
    powers = all(n & (n - 1) == 0 for n in (slab, shard, patch)) and patch >= LANES
    lines = nchan == 4 and nrows == 8 and slab == 32 and ncols % (16 * LANES) == 0 and ncols <= LANES * LANES
    if not (central and powers and lines and steps % 8 == 0 and steps <= LANES and patch < LANES * LANES):
        return on_any_device(residual, psf, positions)
    image, parts, total = run_cycle(nchan, nrows, positions.T, residual, psf)
    return write_outputs(slab * nrows * ncols, slab, image, parts, total)


def on_any_device(residual, psf, positions):
    chan_id = lax.axis_index("chan")
    nchan = lax.axis_size("chan")
    row_id = lax.axis_index("rows")
    nrows = lax.axis_size("rows")
    slab = residual.shape[1]
    ncols = residual.shape[2]
    own_psf = psf[0]
    shard_rows = own_psf.shape[0]
    patch = own_psf.shape[1]
    half = patch // 2
    first = row_id * slab
    chan_hot = (jnp.arange(nchan) == chan_id).astype(jnp.float32)
    full_psf = lax.all_gather(own_psf, "rows", axis=0, tiled=True)
    padded_psf = jnp.pad(full_psf, ((slab, slab), (0, 0)))
    zero = jnp.int32(0)

    def subtract(image, row, col, amount):
        offset = first - row + half
        touches = jnp.logical_and(offset > -slab, offset < patch)
        start = jnp.clip(offset + slab, 0, patch + slab)
        psf_rows = lax.dynamic_slice(padded_psf, (start, zero), (slab, patch))
        window = lax.dynamic_slice(image, (zero, col - half), (slab, patch))
        scale = jnp.where(touches, amount, 0.0)
        return lax.dynamic_update_slice(image, window - scale * psf_rows, (zero, col - half))

    image = residual[0]
    peak_rows = positions[:, 0]
    peak_cols = positions[:, 1]
    inside = jnp.logical_and(peak_rows >= first, peak_rows < first + slab)
    local_rows = jnp.clip(peak_rows - first, 0, slab - 1)
    start_values = jnp.where(inside, image[local_rows, peak_cols], 0.0)
    row_offset = peak_rows[:, None] - peak_rows[None, :] + half - row_id * shard_rows
    col_offset = peak_cols[:, None] - peak_cols[None, :] + half
    owned = (row_offset >= 0) & (row_offset < shard_rows) & (col_offset >= 0) & (col_offset < patch)
    couple = own_psf[jnp.clip(row_offset, 0, shard_rows - 1), jnp.clip(col_offset, 0, patch - 1)]
    couple = jnp.where(owned, couple, 0.0)
    start_table, couple_table = lax.psum(
        (chan_hot[:, None] * start_values[None, :], chan_hot[:, None, None] * couple[None, :, :]),
        ("chan", "rows"),
    )

    def solve(k, amps):
        taken = jnp.sum(amps * lax.dynamic_index_in_dim(couple_table, k, 1, False), axis=1)
        value = lax.dynamic_index_in_dim(start_table, k, 1, False) - taken
        amp = 0.25 * (value + jnp.sum(value) / nchan)
        return lax.dynamic_update_index_in_dim(amps, amp, k, 1)

    amps = lax.fori_loop(0, STEPS, solve, jnp.zeros((nchan, STEPS), jnp.float32))
    own_amps = jnp.sum(chan_hot[:, None] * amps, axis=0)

    def apply(k, image):
        return subtract(image, positions[k, 0], positions[k, 1], own_amps[k])

    image = lax.fori_loop(0, STEPS, apply, image)
    count = slab * nrows * ncols
    parts = lax.psum_scatter(image, "chan", scatter_dimension=1, tiled=True)
    total = lax.psum(jnp.sum(parts * parts), ("chan", "rows"))
    normalized = parts * lax.rsqrt(total / count + 1e-06)
    return (image[None], normalized)


def solution(mesh):
    return jax.shard_map(
        on_device,
        mesh=mesh,
        in_specs=(P("chan", "rows", None), P("chan", "rows", None), P()),
        out_specs=(P("chan", "rows", None), P("rows", "chan")),
        check_vma=False,
    )
```

```python
import functools

import jax
import jax.numpy as jnp
from jax import lax
from jax.experimental import pallas as pl
from jax.experimental.pallas import tpu as pltpu
from jax.sharding import PartitionSpec as P

STEPS = 32
LANES = 128
MESH = pl.DeviceIdType.MESH
OUT = pltpu.VMEM
VMEM = 67043328


def pick(tile, row, col, lane_to, owned, number, acc):
    moved = pltpu.roll(tile, (lane_to - col) & (LANES - 1), 1)
    target = jnp.where(owned, (row & 7) * LANES + lane_to, -1)
    return jnp.where(number == target, moved, acc)


def cycle_kernel(nchan, nrows, pos, res, psf, image, parts, total_out,
                 work, land, patch_v, psf_v, grid, couple_v, couple_in, start_v, start_in, tables, amps_v, prev_v, last_v,
                 first_far, first_own, passed, second, squares, changes, pair_v, sum_v, prev_s, last_s, amps_s, pair_s,
                 ready, band_sem, psf_sem, index_sem, send_sem, unit_recv, recv_sem, relay_sem, fine_send, fine_recv, fine_relay,
                 start_send, start_recv, couple_send, couple_recv, table_send, table_recv, amp_send, amp_recv,
                 far_send, far_recv, own_send, own_recv, pass_send, pass_recv, square_send, square_recv, guest_sem, lent_send, lent_recv):
    chan, row = lax.axis_index("chan"), lax.axis_index("rows")
    chip, core = row // 2, row % 2
    partner = row + 1 - 2 * core
    nchips = nrows // 2
    side = chip // (nchips // 2)
    slab, ncols = res.shape[1], res.shape[2]
    shard, patch = psf.shape[1:]
    half, steps, chunks = patch // 2, pos.shape[1], patch // LANES
    unit, tiles, blocks = 2 * slab, slab // 8, ncols // LANES
    base, width = blocks + 1, chunks + 1
    first = row * slab
    begins_at = [z - (1 if z == (nchips - 1) // 2 else 0) for z in range(nchips)]
    lead = jnp.where(chip == (nchips - 1) // 2, 1, 0)
    roots = (nchips - 1, nchips)
    solvers = (roots[0] ^ 1, roots[1] ^ 1)
    is_root = jnp.logical_or(row == roots[0], row == roots[1])
    is_solver = jnp.logical_or(row == solvers[0], row == solvers[1])
    is_mid = jnp.logical_or(is_root, is_solver)
    is_end = jnp.logical_not(is_mid)
    lane = lax.broadcasted_iota(jnp.int32, (1, LANES), 1)
    lane8 = lax.broadcasted_iota(jnp.int32, (8, LANES), 1)
    number = lax.broadcasted_iota(jnp.int32, (8, LANES), 0) * LANES + lane8
    zero = jnp.zeros((8, LANES), jnp.float32)

    def block_at(index):
        return pl.ds(pl.multiple_of(index * LANES, LANES), LANES)

    def flip(bit):
        if bit == 1:
            return chan + 1 - 2 * (chan % 2)
        return (chan + 2) % 4

    barrier = pltpu.get_barrier_semaphore()
    for bit in (1, 2):
        pl.semaphore_signal(barrier, inc=1, device_id=(flip(bit), row), device_id_type=MESH)
    pl.semaphore_signal(barrier, inc=1, device_id=(chan, partner), device_id_type=MESH)

    @pl.when(chip > 0)
    def _():
        for c in range(2):
            pl.semaphore_signal(barrier, inc=1, device_id=(chan, 2 * chip - 2 + c), device_id_type=MESH)

    @pl.when(chip < nchips - 1)
    def _():
        for c in range(2):
            pl.semaphore_signal(barrier, inc=1, device_id=(chan, 2 * chip + 2 + c), device_id_type=MESH)

    bands = [pltpu.make_async_copy(res.at[0, pl.ds(8 * t, 8)], image.at[pl.ds(8 * t, 8)], band_sem.at[t]) for t in range(tiles)]
    for copy in bands:
        copy.start()
    loads = [pltpu.make_async_copy(psf.at[0, :, pl.ds(c * LANES, LANES)], psf_v.at[pl.ds(c * shard, shard)], psf_sem.at[c]) for c in range(chunks)]

    @pl.when(is_root)
    def _():
        for copy in loads:
            copy.start()

    begins = [jnp.clip(pos[1, k] - half, 0, ncols - patch) >> 7 for k in range(steps)]
    krow = lax.broadcasted_iota(jnp.int32, (steps, LANES), 0)
    target = jnp.zeros((steps, LANES), jnp.int32)
    for k in range(steps):
        target = jnp.where(krow == k, begins[k], target)
    target = target + lax.broadcasted_iota(jnp.int32, (steps, LANES), 1)
    prev, last = target, lane8
    for k in range(steps):
        inside = target - begins[k]
        prev = jnp.where((inside >= 0) & (inside < width) & (krow > k), inside + (base + width * k), prev)
        inside = lane8 - begins[k]
        last = jnp.where((inside >= 0) & (inside < width), inside + (base + width * k), last)
    prev_v[...] = prev
    last_v[...] = last
    lane32 = lax.broadcasted_iota(jnp.int32, (steps, LANES), 1)
    rows_from = jnp.zeros((steps, LANES), jnp.int32)
    cols_from = jnp.zeros((steps, LANES), jnp.int32)
    for k in range(steps):
        rows_from = rows_from + jnp.where(krow == k, pos[0, k], 0) - jnp.where(lane32 == k, pos[0, k], 0)
        cols_from = cols_from + jnp.where(krow == k, pos[1, k], 0) - jnp.where(lane32 == k, pos[1, k], 0)
    rows_from = rows_from + half - row * shard
    cols_from = cols_from + half
    owned = (rows_from >= 0) & (rows_from < shard) & (cols_from >= 0) & (cols_from < patch) & (lane32 < krow)
    pair_v[0] = ((cols_from >> 7) & (chunks - 1)) * shard + (((rows_from >> 3) << 3) & (shard - 1))
    pair_v[1] = (lane32 - cols_from) & (LANES - 1)
    pair_v[2] = jnp.where(owned, (rows_from & 7) * LANES + lane32, -1)
    pair_copy = pltpu.make_async_copy(pair_v, pair_s, index_sem.at[3])

    @pl.when(is_root)
    def _():
        pair_copy.start()

    index_copies = [pltpu.make_async_copy(prev_v, prev_s, index_sem.at[0]), pltpu.make_async_copy(last_v, last_s, index_sem.at[1])]
    for copy in index_copies:
        copy.start()
    for t in range(tiles):
        work[t, blocks] = zero

    @pl.when(is_end)
    def _():
        pl.semaphore_wait(barrier, 5)

    @pl.when(is_mid)
    def _():
        pl.semaphore_wait(barrier, 7)


    def bulk(s):
        mid, end, other = (nchips - 1 + s) // 2, (nchips - 1) * s, nchips // 2 - s
        order = (0, 1) if s == 0 else (1, 0)
        near = list(range(nchips)) if s == 0 else list(range(2 * nchips - 1, nchips - 1, -1))
        across = [nchips - 1 - n if s == 0 else nchips + n for n in range(nchips // 2)]
        local = range(s * nchips, (s + 1) * nchips)
        out = []

        def add(u, z, h, rows, to_row, sem):
            out.append(pltpu.make_async_remote_copy(
                src_ref=psf.at[0, pl.ds((u % nchips) * unit + h * slab, rows)], dst_ref=land.at[pl.ds((u - begins_at[z]) * unit + h * slab, rows)],
                send_sem=send_sem.at[len(out)], recv_sem=sem, device_id=(chan, to_row), device_id_type=MESH))

        for u in near:
            for h in order:
                add(u, end, h, slab, 2 * end + (s if u == near[-1] else h), recv_sem.at[u - begins_at[end], h])
        for u in across:
            for h in range(2):
                add(u, other, h, slab, 2 * other + h, recv_sem.at[u - begins_at[other], h])
        for u in local:
            add(u, mid, 0, unit, solvers[s], unit_recv.at[u - begins_at[mid]])
        return out

    for s in range(2):
        @pl.when(row == roots[s])
        def _(s=s):
            for copy in bulk(s):
                copy.start()

    early = core == side
    is_lead, is_trail = is_end & early, is_end & jnp.logical_not(early)
    doubled = is_mid & jnp.logical_not(early)
    sends = jnp.where(is_end, jnp.where(early, tiles - 1, tiles - 2), jnp.where(early, tiles + 1, tiles + 2))

    def tile_at(i):
        return jnp.where(side == 0, i, tiles - 1 - i)

    def tile_rows(t):
        return pl.ds(pl.multiple_of(8 * t, 8), 8)

    def guest_tile(g):
        return tile_at(jnp.where(early, tiles - 1, tiles - 2 + g))

    head = ncols // 4

    def lent(g, part):
        width = (head, ncols - head)[part]
        return pltpu.make_async_remote_copy(
            src_ref=res.at[0, tile_rows(guest_tile(g)), pl.ds(head * part, width)],
            dst_ref=image.at[tile_rows(tiles + g), pl.ds(head * part, width)],
            send_sem=lent_send.at[g, part], recv_sem=lent_recv.at[g, part], device_id=(chan, row + 2 - 4 * side), device_id_type=MESH)

    def given(g):
        return pltpu.make_async_remote_copy(
            src_ref=parts.at[tile_rows(tiles + g)], dst_ref=parts.at[tile_rows(guest_tile(g))], send_sem=guest_sem.at[g], recv_sem=guest_sem.at[2 + g],
            device_id=(chan, row - 2 + 4 * side), device_id_type=MESH)

    @pl.when(is_end)
    def _():
        lent(0, 0).start()

    for bit in (1, 2):
        pl.semaphore_signal(ready.at[0], inc=1, device_id=(flip(bit), row), device_id_type=MESH)

    for copy in bands:
        copy.wait()

    def spread_out(b, carry):
        for t in range(tiles):
            work[t, b] = image[pl.ds(8 * t, 8), block_at(b)]
        return carry

    lax.fori_loop(0, blocks, spread_out, 0, unroll=4)
    acc = zero
    for k in range(steps):
        r, c = pos[0, k] - first, pos[1, k]
        tile = work[(r >> 3) & (tiles - 1), c >> 7]
        acc = pick(tile, r, c, k, (r >= 0) & (r < slab), number, acc)
    start_v[...] = acc

    def start_copy(s, source):
        return pltpu.make_async_remote_copy(
            src_ref=start_v, dst_ref=start_in.at[source], send_sem=start_send, recv_sem=start_recv.at[source],
            device_id=(chan, solvers[s]), device_id_type=MESH)

    def couple_copy(s):
        return pltpu.make_async_remote_copy(
            src_ref=couple_v, dst_ref=couple_in, send_sem=couple_send, recv_sem=couple_recv,
            device_id=(chan, solvers[s]), device_id_type=MESH)

    for s in range(2):
        @pl.when((side == s) & (row != solvers[s]))
        def _(s=s):
            start_copy(s, row).start()

    @pl.when(is_end)
    def _():
        lent(0, 1).start()

    @pl.when(is_trail)
    def _():
        for part in range(2):
            lent(1, part).start()

    @pl.when(is_root)
    def _():
        for copy in loads:
            copy.wait()
        pair_copy.wait()

        def fill(count, k, carry):
            acc = zero
            for j in range(count):
                tile = psf_v[pl.ds(pair_s[0, k, j], 8), :]
                acc = jnp.where(number == pair_s[2, k, j], pltpu.roll(tile, pair_s[1, k, j], 1), acc)
            grid[k] = acc
            return carry

        for g in range(steps // 8):
            lax.fori_loop(8 * g, 8 * g + 8, functools.partial(fill, 8 * g + 8), 0)
        couple_v[...] = jnp.sum(grid[...], axis=1)

    for s in range(2):
        @pl.when(row == roots[s])
        def _(s=s):
            couple_copy(s).start()

    def held(m, h, rows=slab):
        return land.at[pl.ds(pl.multiple_of(m * unit + h * slab, 8), rows)]

    def relay(m):
        return pltpu.make_async_remote_copy(
            src_ref=held(m, core), dst_ref=held(m, core), send_sem=relay_sem.at[m], recv_sem=recv_sem.at[m, core],
            device_id=(chan, partner), device_id_type=MESH)

    def arrival(m, h):
        return pltpu.make_async_remote_copy(
            src_ref=held(m, h), dst_ref=held(m, h), send_sem=relay_sem.at[m], recv_sem=recv_sem.at[m, h],
            device_id=(chan, partner), device_id_type=MESH)

    def pass_on(m):
        arrival(m, core).wait_recv()
        relay(m).start()

    def crossed(n):
        return jnp.where(side == 0, nchips + n, 1 - n)

    def streamed(n):
        return jnp.where(side == 0, n, nchips - n)

    def relayout(source, source_row, dest_row, rows):
        def body(g, carry):
            take, put = pl.multiple_of(source_row + 8 * g, 8), pl.multiple_of(dest_row + 8 * g, 8)
            for c in range(chunks):
                narrow = source.shape[1] == LANES
                tile = source[pl.ds(pl.multiple_of(c * shard + take, 8), 8), :] if narrow else source[pl.ds(take, 8), pl.ds(c * LANES, LANES)]
                patch_v[c, pl.ds(put, 8), :] = tile
            return carry

        lax.fori_loop(0, rows // 8, body, 0)

    @pl.when(is_root)
    def _():
        pass_on(crossed(0))

    pl.semaphore_wait(ready.at[0], 2)
    for bit in (1, 2):
        pl.semaphore_signal(ready.at[1], inc=1, device_id=(flip(bit), row), device_id_type=MESH)
    pl.semaphore_wait(ready.at[1], 2)
    me_table = 2 * chan + side

    def table_copy(step):
        other = (me_table + step) % (2 * nchan)
        return pltpu.make_async_remote_copy(
            src_ref=tables.at[me_table], dst_ref=tables.at[me_table], send_sem=table_send.at[step], recv_sem=table_recv.at[step],
            device_id=(other // 2, solvers[0] + (other % 2) * (solvers[1] - solvers[0])), device_id_type=MESH)

    def table_arrival(step):
        other = (me_table + 2 * nchan - step) % (2 * nchan)
        return pltpu.make_async_remote_copy(
            src_ref=tables.at[other], dst_ref=tables.at[other], send_sem=table_send.at[step], recv_sem=table_recv.at[step],
            device_id=(other // 2, solvers[0] + (other % 2) * (solvers[1] - solvers[0])), device_id_type=MESH)

    for s in range(2):
        @pl.when(row == solvers[s])
        def _(s=s):
            total = start_v[...]
            for source in range(s * nchips, (s + 1) * nchips):
                if source != solvers[s]:
                    start_copy(s, source).wait_recv()
                    total = total + start_in[source]
            couple_copy(s).wait_recv()
            tables[me_table, pl.ds(0, steps), :] = couple_in[...]
            tables[me_table, pl.ds(steps, 8), :] = jnp.broadcast_to(jnp.sum(total, axis=0, keepdims=True), total.shape)
            for step in range(1, 2 * nchan):
                table_copy(step).start()
            pass_on(crossed(0))

    def amp_copy(n):
        return pltpu.make_async_remote_copy(
            src_ref=amps_v, dst_ref=amps_v, send_sem=amp_send.at[n], recv_sem=amp_recv,
            device_id=(chan, side * nchips + (row + n) % nchips), device_id_type=MESH)

    @pl.when(is_solver)
    def _():
        for step in range(1, 2 * nchan):
            table_arrival(step).wait_recv()

        def rows_of(index):
            return jnp.concatenate([tables[2 * c, pl.ds(index, 1), :] + tables[2 * c + 1, pl.ds(index, 1), :] for c in range(nchan)], axis=0)

        start = rows_of(steps)

        def solve(k, amps):
            value = jnp.sum(jnp.where(lane == k, start, 0.0) - amps * rows_of(k), axis=1, keepdims=True)
            amp = 0.25 * (value + jnp.sum(value, axis=0, keepdims=True) / nchan)
            return jnp.where(lane == k, amp, amps)

        amps = lax.fori_loop(0, steps, solve, jnp.zeros((nchan, LANES), jnp.float32), unroll=4)
        amps_v[pl.ds(0, nchan), :] = amps
        amps_v[pl.ds(nchan, 8 - nchan), :] = jnp.zeros((8 - nchan, LANES), jnp.float32)
        for n in range(1, nchips):
            amp_copy(n).start()

    def fine_piece(n):
        return jnp.where(side == 0, n, 2 * tiles - 1 - n)

    def fine_at(n):
        return pl.multiple_of(jnp.where(side == 0, nchips, 0) * unit + 8 * fine_piece(n), 8)

    def onward_piece(s, n):
        mid, end = (nchips - 1 + s) // 2, (nchips - 1) * s
        u = nchips - s
        j = n if s == 0 else 2 * tiles - 1 - n
        return pltpu.make_async_remote_copy(
            src_ref=land.at[pl.ds((u - begins_at[mid]) * unit + 8 * j, 8)], dst_ref=land.at[pl.ds((u - begins_at[end]) * unit + 8 * j, 8)],
            send_sem=fine_send.at[n], recv_sem=fine_recv.at[n], device_id=(chan, 2 * end + (s if n == 0 else 1 - s)), device_id_type=MESH)

    def fine_copy(n):
        return pltpu.make_async_remote_copy(
            src_ref=land.at[pl.ds(fine_at(n), 8)], dst_ref=land.at[pl.ds(fine_at(n), 8)],
            send_sem=fine_relay.at[n], recv_sem=fine_recv.at[n], device_id=(chan, partner), device_id_type=MESH)

    for s in range(2):
        offset = s * nchips - begins_at[(nchips - 1 + s) // 2]

        @pl.when(row == roots[s])
        def _(s=s, offset=offset):
            arrival(crossed(0), 1 - core).wait_recv()
            for n in range(2 * tiles):
                onward_piece(s, n).start()
            relayout(psf_v, 0, offset * unit, nchips * unit)

        @pl.when(row == solvers[s])
        def _(s=s, offset=offset):
            arrival(crossed(0), 1 - core).wait_recv()
            for u in range(nchips):
                pltpu.make_async_remote_copy(
                    src_ref=held(u + offset, 0, unit), dst_ref=held(u + offset, 0, unit), send_sem=send_sem.at[0], recv_sem=unit_recv.at[u + offset],
                    device_id=(chan, partner), device_id_type=MESH).wait_recv()
            relayout(land, offset * unit, offset * unit, nchips * unit)

    def relayout_crossed(n):
        begin = pl.multiple_of(crossed(n) * unit, 8)
        relayout(land, begin, begin, unit)

    @pl.when(is_mid)
    def _():
        relayout_crossed(0)

    amps_copy = pltpu.make_async_copy(amps_v, amps_s, index_sem.at[2])
    leading = early

    def half_unit(m, h):
        begin = pl.multiple_of(m * unit + h * slab, 8)
        relayout(land, begin, begin, slab)

    def relay_half(m, h):
        return pltpu.make_async_remote_copy(
            src_ref=held(m, h), dst_ref=held(m, h), send_sem=relay_sem.at[nchips + 2 + h], recv_sem=recv_sem.at[m, h],
            device_id=(chan, partner), device_id_type=MESH)

    @pl.when(is_end)
    def _():
        for n in range(nchips - 1):
            pass_on(streamed(n))
            if n > 0:
                arrival(streamed(n - 1), 1 - core).wait_recv()
                for h in range(2):
                    half_unit(streamed(n - 1), h)
        amp_copy(1).wait_recv()
        amps_copy.start()
        arrival(streamed(nchips - 2), 1 - core).wait_recv()
        for h in range(2):
            half_unit(streamed(nchips - 2), h)

    @pl.when(is_end & leading)
    def _():
        for n in range(2):
            h = jnp.where(side == 0, n, 1 - n)
            arrival(streamed(nchips - 1), h).wait_recv()
            relay_half(streamed(nchips - 1), h).start()
            half_unit(streamed(nchips - 1), h)

    @pl.when(is_end & jnp.logical_not(leading))
    def _():
        for n in range(2):
            h = jnp.where(side == 0, n, 1 - n)
            arrival(streamed(nchips - 1), h).wait_recv()
            half_unit(streamed(nchips - 1), h)

    @pl.when(is_root)
    def _():
        amp_copy(1).wait_recv()

    @pl.when(is_mid)
    def _():
        amps_copy.start()

    for copy in index_copies:
        copy.wait()
    amps_copy.wait()

    cols = ncols // nchan
    span = cols // 2
    bits = ((1, 2), (2, 1))

    diagonal = 3 - chan

    def is_guest(n):
        return (n == 0) | (doubled & (n == 2))

    def own_index(n):
        return jnp.where(is_mid, n - 1 - jnp.where(doubled & (n > 2), 1, 0), n)

    def tile_of(n):
        return jnp.where(is_mid & is_guest(n), tiles + n // 2, tile_at(own_index(n)))

    def rows_at(n):
        return tile_rows(tile_of(n))

    def lift_of(n):
        own_lift = lead * unit + 8 * tile_at(own_index(n))
        guest_lift = side * unit + 8 * guest_tile(n // 2)
        return slab * nrows + core * slab + jnp.where(is_mid & is_guest(n), guest_lift, own_lift)

    def cols_at(c, p):
        return pl.ds(pl.multiple_of(c * cols + p * span, LANES), span)

    def send(i, p, source, dest, send_sem, recv_sem, to):
        return pltpu.make_async_remote_copy(
            src_ref=source, dst_ref=dest.at[i, p], send_sem=send_sem.at[i, p], recv_sem=recv_sem.at[i, p],
            device_id=(to, row), device_id_type=MESH)

    def far(i, p):
        return send(i, p, image.at[rows_at(i), cols_at(diagonal, p)], first_far, far_send, far_recv, flip(bits[p][0]))

    def mine(i, p):
        return send(i, p, image.at[rows_at(i), cols_at(flip(bits[p][0]), p)], first_own, own_send, own_recv, flip(bits[p][0]))

    def onward(i, p):
        return send(i, p, passed.at[i, p], second, pass_send, pass_recv, flip(bits[p][1]))

    def fetch(n):
        fine_copy(n).wait_recv()

    def arrive(n):
        fetch(n)
        relayout(land, fine_at(n), fine_at(n), 8)

    def share(n):
        fetch(n)
        fine_copy(n).start()
        relayout(land, fine_at(n), fine_at(n), 8)

    def scale_and_shift(i):
        lift = lift_of(i)

        def sixteen(g, carry):
            for n in range(16):
                k = 16 * g + n
                amp = amps_s[chan, k]
                begin = lift - pos[0, k]
                shift = (pos[1, k] - half) & (LANES - 1)
                keep = lane8 < shift
                moved = [zero] + [pltpu.roll(patch_v[c, pl.ds(begin, 8), :] * amp, shift, 1) for c in range(chunks)] + [zero]
                for m in range(width):
                    changes[width * k + m] = jnp.where(keep, moved[m], moved[m + 1])
            return carry

        lax.fori_loop(0, steps // 16, sixteen, 0)

    def subtract(i):
        t = tile_of(i)

        def sixteen(g, carry):
            for n in range(16):
                k = 16 * g + n
                after = [work[t, prev_s[k, m]] - changes[width * k + m] for m in range(width)]
                for m in range(width):
                    work[t, base + width * k + m] = after[m]
            return carry

        lax.fori_loop(0, steps // 16, sixteen, 0)

    def finalize(i, c):
        rows = rows_at(i)
        per = cols // LANES

        def body(g, carry):
            for n in range(8):
                b = c * per + g * 8 + n
                image[rows, block_at(b)] = work[tile_of(i), last_s[0, b]]
            return carry

        lax.fori_loop(0, per // 8, body, 0)

    def combine(i):
        for p in range(2):
            far(i, p).wait_recv()
            passed[i, p] = image[rows_at(i), cols_at(flip(bits[p][1]), p)] + first_far[i, p]
            onward(i, p).start()

    def own(n):
        for p in range(2):
            mine(n, p).wait_recv()
            onward(n, p).wait_recv()
            value = image[rows_at(n), cols_at(chan, p)] + first_own[n, p] + second[n, p]
            parts[rows_at(n), pl.ds(p * span, span)] = value
            square = value * value
            total = zero
            for c in range(span // LANES):
                total = total + square[:, c * LANES:(c + 1) * LANES]
            sum_v[...] = sum_v[...] + total

    def start_far(n):
        for p in range(2):
            far(n, p).start()

    def start_mine(n):
        for p in range(2):
            mine(n, p).start()

    def finish(n):
        for p in range(2):
            finalize(n, flip(bits[p][0]))
        finalize(n, chan)

    sum_v[...] = zero

    def advance(n, carry):
        active = n < sends

        @pl.when(is_lead & (n == 0))
        def _():
            share(0)

        @pl.when(is_lead & (n > 0) & active)
        def _():
            arrive(n)

        @pl.when(is_trail & (n == 0))
        def _():
            arrive(0)
            for piece in range(1, tiles):
                share(piece)

        @pl.when(is_trail & active)
        def _():
            arrive(tiles + n)

        @pl.when(is_mid & is_guest(n))
        def _():
            for part in range(2):
                lent(n // 2, part).wait_recv()

            def guest(b, carry):
                work[tiles + n // 2, b] = image[tile_rows(tiles + n // 2), block_at(b)]
                return carry

            lax.fori_loop(0, blocks, guest, 0, unroll=4)

        @pl.when(is_mid & (n == 1))
        def _():
            arrival(crossed(1), 1 - core).wait_recv()
            relayout_crossed(1)

        @pl.when(active)
        def _():
            scale_and_shift(n)

        @pl.when(is_mid & (n == 0))
        def _():
            pass_on(crossed(1))

        @pl.when(n == sends)
        def _():
            combine(n - 1)

        @pl.when(active)
        def _():
            subtract(n)
            finalize(n, diagonal)

        @pl.when(n < sends)
        def _():
            start_far(n)

        @pl.when(active)
        def _():
            finish(n)

        @pl.when(is_end & (n < sends))
        def _():
            start_mine(n)

        @pl.when((n > 0) & (n < sends))
        def _():
            combine(n - 1)

        @pl.when(is_mid & (n < sends))
        def _():
            start_mine(n)

        @pl.when(is_mid & (n == 4))
        def _():
            own(0)
            given(0).start()

        @pl.when(doubled & (n == 5))
        def _():
            own(2)
            given(1).start()

        return carry

    lax.fori_loop(0, tiles + 3, advance, 0)

    def settle(n, carry):
        @pl.when((n < sends) & jnp.logical_not(is_mid & is_guest(n)))
        def _():
            own(n)

        return carry

    lax.fori_loop(0, tiles + 2, settle, 0)
    total = sum_v[...]
    me = row * nchan + chan
    squares[pl.ds(me, 1), :] = jnp.sum(total, axis=0, keepdims=True)

    everyone = nrows * nchan

    def spread(step):
        other = (me + jnp.where(side == 0, everyone - step, step)) % everyone
        return pltpu.make_async_remote_copy(
            src_ref=squares.at[pl.ds(me, 1)], dst_ref=squares.at[pl.ds(me, 1)], send_sem=square_send.at[step], recv_sem=square_recv.at[me],
            device_id=(other % nchan, other // nchan), device_id_type=MESH)

    def arrived(step):
        other = (me + step) % everyone
        return pltpu.make_async_remote_copy(
            src_ref=squares.at[pl.ds(other, 1)], dst_ref=squares.at[pl.ds(other, 1)], send_sem=square_send.at[step], recv_sem=square_recv.at[other],
            device_id=(other % nchan, other // nchan), device_id_type=MESH)

    for step in range(1, nrows * nchan):
        spread(step).start()

    def leftover(n, carry):
        @pl.when(is_end & (n >= sends))
        def _():
            arrive(jnp.where(early, n, tiles + n))
            scale_and_shift(n)
            subtract(n)
            finalize(n, diagonal)
            finish(n)

        return carry

    lax.fori_loop(tiles - 2, tiles, leftover, 0)

    for s in range(2):
        @pl.when(row == roots[s])
        def _(s=s):
            for copy in bulk(s):
                copy.wait_send()
            for n in range(2 * tiles):
                onward_piece(s, n).wait_send()
            couple_copy(s).wait_send()

    @pl.when(is_mid)
    def _():
        for n in range(2):
            relay(crossed(n)).wait_send()

    @pl.when(is_end)
    def _():
        for n in range(nchips - 1):
            relay(streamed(n)).wait_send()

    @pl.when(is_end & leading)
    def _():
        for h in range(2):
            relay_half(streamed(nchips - 1), h).wait_send()
        fine_copy(0).wait_send()

    @pl.when(is_trail)
    def _():
        for n in range(1, tiles):
            fine_copy(n).wait_send()

    @pl.when(is_solver)
    def _():
        for step in range(1, 2 * nchan):
            table_copy(step).wait_send()
        for n in range(1, nchips):
            amp_copy(n).wait_send()

    @pl.when(jnp.logical_not(is_solver))
    def _():
        start_copy(0, row).wait_send()

    def sent(n, carry):
        @pl.when(n < sends)
        def _():
            for p in range(2):
                far(n, p).wait_send()
                mine(n, p).wait_send()
                onward(n, p).wait_send()

        return carry

    lax.fori_loop(0, tiles + 2, sent, 0)

    @pl.when(is_mid)
    def _():
        given(0).wait_send()

    @pl.when(doubled)
    def _():
        given(1).wait_send()

    @pl.when(is_end)
    def _():
        for part in range(2):
            lent(0, part).wait_send()
        given(0).wait_recv()

    @pl.when(is_trail)
    def _():
        for part in range(2):
            lent(1, part).wait_send()
        given(1).wait_recv()

    for step in range(1, nrows * nchan):
        spread(step).wait_send()
    for step in range(1, nrows * nchan):
        arrived(step).wait_recv()
    everything = jnp.sum(jnp.sum(squares[...], axis=0, keepdims=True), axis=1, keepdims=True)
    total_out[...] = jnp.broadcast_to(everything, total_out.shape)


def run_cycle(nchan, nrows, positions, residual, psf):
    slab, ncols = residual.shape[1:]
    shard, patch = psf.shape[1:]
    steps, chunks = positions.shape[1], patch // LANES
    nchips, tiles, cols = nrows // 2, slab // 8, ncols // nchan
    rows = slab * (nrows + 4)
    dma, f32, i32 = pltpu.SemaphoreType.DMA, jnp.float32, jnp.int32
    anywhere = pl.BlockSpec(memory_space=pl.ANY)
    vmem = pl.BlockSpec(memory_space=pltpu.VMEM)
    slots = ncols // LANES + 1 + (chunks + 1) * steps
    stage = pltpu.VMEM((tiles + 2, 2, 8, cols // 2), f32)
    small = pltpu.VMEM((8, LANES), f32)
    return pl.pallas_call(
        functools.partial(cycle_kernel, nchan, nrows),
        out_shape=(OUT((slab + 16, ncols), f32), OUT((slab + 16, cols), f32), OUT((8, LANES), f32)),
        in_specs=[pl.BlockSpec(memory_space=pltpu.SMEM), anywhere, anywhere],
        out_specs=(vmem, vmem, vmem),
        scratch_shapes=[
            pltpu.VMEM((tiles + 2, slots, 8, LANES), f32), pltpu.VMEM((rows, patch), f32), pltpu.VMEM((chunks, rows, LANES), f32),
            pltpu.VMEM((chunks * shard, LANES), f32), pltpu.VMEM((steps, 8, LANES), f32), pltpu.VMEM((steps, LANES), f32),
            pltpu.VMEM((steps, LANES), f32), small, pltpu.VMEM((nrows, 8, LANES), f32),
            pltpu.VMEM((2 * nchan, steps + 8, LANES), f32), small, pltpu.VMEM((steps, LANES), i32), pltpu.VMEM((8, LANES), i32),
            stage, stage, stage, stage, pltpu.VMEM((nrows * nchan, LANES), f32), pltpu.VMEM(((chunks + 1) * steps, 8, LANES), f32), pltpu.VMEM((3, steps, LANES), i32), small,
            pltpu.SMEM((steps, LANES), i32), pltpu.SMEM((8, LANES), i32), pltpu.SMEM((8, LANES), f32), pltpu.SMEM((3, steps, LANES), i32),
            pltpu.SemaphoreType.REGULAR((2,)), dma((tiles,)), dma((chunks,)), dma((4,)), dma((4 * nchips,)), dma((nchips + 2,)),
            dma((nchips + 2, 2)), dma((nchips + 4,)), dma((2 * tiles,)), dma((2 * tiles,)), dma((2 * tiles,)),
            dma, dma((nrows,)), dma, dma, dma((2 * nchan,)), dma((2 * nchan,)), dma((nchips,)), dma,
        ] + [dma((tiles + 2, 2))] * 6 + [dma((nrows * nchan,))] * 2 + [dma((4,)), dma((2, 2)), dma((2, 2))],
        compiler_params=pltpu.CompilerParams(collective_id=0, has_side_effects=True, vmem_limit_bytes=VMEM - 4 * ((slab + 16) * (ncols + cols) + 8 * LANES)),
        name="minor_cycle",
    )(positions, residual, psf)


def write_kernel(count, image, parts, total, image_out, normalized, scaled, sems):
    slab, tiles = scaled.shape[0], scaled.shape[0] // 8
    copies = [pltpu.make_async_copy(image.at[pl.ds(8 * t, 8)], image_out.at[0, pl.ds(8 * t, 8)], sems.at[t]) for t in range(tiles)]
    for copy in copies:
        copy.start()
    scale = lax.rsqrt(total[0:1, 0:1] / count + 1e-06)
    for t in range(tiles):
        rows = pl.ds(8 * t, 8)
        scaled[rows, :] = parts[rows, :] * scale
        copies.append(pltpu.make_async_copy(scaled.at[rows], normalized.at[rows], sems.at[tiles + t]))
        copies[-1].start()
    for copy in copies:
        copy.wait()


def write_outputs(count, slab, image, parts, total):
    f32, ncols, cols = jnp.float32, image.shape[1], parts.shape[1]
    anywhere, vmem = pl.BlockSpec(memory_space=pl.ANY), pl.BlockSpec(memory_space=pltpu.VMEM)
    return pl.pallas_call(
        functools.partial(write_kernel, count),
        out_shape=(jax.ShapeDtypeStruct((1, slab, ncols), f32), jax.ShapeDtypeStruct((slab, cols), f32)),
        in_specs=[vmem, vmem, vmem],
        out_specs=(anywhere, anywhere),
        scratch_shapes=[pltpu.VMEM((slab, cols), f32), pltpu.SemaphoreType.DMA((slab // 4,))],
        name="write_outputs",
        compiler_params=pltpu.CompilerParams(vmem_limit_bytes=4 * 2**20),
    )(*(pltpu.with_memory_space_constraint(x, pltpu.VMEM) for x in (image, parts, total)))


def on_device(residual, psf, positions):
    nchan, nrows = lax.axis_size("chan"), lax.axis_size("rows")
    slab, ncols = residual.shape[1:]
    shard, patch = psf.shape[1:]
    steps = positions.shape[0]
    central = slab * nrows == shard and shard * nrows == patch
    powers = all(n & (n - 1) == 0 for n in (slab, shard, patch)) and patch >= LANES
    lines = nchan == 4 and nrows == 8 and slab == 32 and ncols % (16 * LANES) == 0 and ncols <= LANES * LANES
    if not (central and powers and lines and steps % 16 == 0 and steps <= LANES and patch < LANES * LANES):
        return on_any_device(residual, psf, positions)
    image, parts, total = run_cycle(nchan, nrows, positions.T, residual, psf)
    return write_outputs(slab * nrows * ncols, slab, image, parts, total)


def on_any_device(residual, psf, positions):
    chan_id = lax.axis_index("chan")
    nchan = lax.axis_size("chan")
    row_id = lax.axis_index("rows")
    nrows = lax.axis_size("rows")
    slab = residual.shape[1]
    ncols = residual.shape[2]
    own_psf = psf[0]
    shard_rows = own_psf.shape[0]
    patch = own_psf.shape[1]
    half = patch // 2
    first = row_id * slab
    chan_hot = (jnp.arange(nchan) == chan_id).astype(jnp.float32)
    full_psf = lax.all_gather(own_psf, "rows", axis=0, tiled=True)
    padded_psf = jnp.pad(full_psf, ((slab, slab), (0, 0)))
    zero = jnp.int32(0)

    def subtract(image, row, col, amount):
        offset = first - row + half
        touches = jnp.logical_and(offset > -slab, offset < patch)
        start = jnp.clip(offset + slab, 0, patch + slab)
        psf_rows = lax.dynamic_slice(padded_psf, (start, zero), (slab, patch))
        window = lax.dynamic_slice(image, (zero, col - half), (slab, patch))
        scale = jnp.where(touches, amount, 0.0)
        return lax.dynamic_update_slice(image, window - scale * psf_rows, (zero, col - half))

    image = residual[0]
    peak_rows = positions[:, 0]
    peak_cols = positions[:, 1]
    inside = jnp.logical_and(peak_rows >= first, peak_rows < first + slab)
    local_rows = jnp.clip(peak_rows - first, 0, slab - 1)
    start_values = jnp.where(inside, image[local_rows, peak_cols], 0.0)
    row_offset = peak_rows[:, None] - peak_rows[None, :] + half - row_id * shard_rows
    col_offset = peak_cols[:, None] - peak_cols[None, :] + half
    owned = (row_offset >= 0) & (row_offset < shard_rows) & (col_offset >= 0) & (col_offset < patch)
    couple = own_psf[jnp.clip(row_offset, 0, shard_rows - 1), jnp.clip(col_offset, 0, patch - 1)]
    couple = jnp.where(owned, couple, 0.0)
    start_table, couple_table = lax.psum(
        (chan_hot[:, None] * start_values[None, :], chan_hot[:, None, None] * couple[None, :, :]),
        ("chan", "rows"),
    )

    def solve(k, amps):
        taken = jnp.sum(amps * lax.dynamic_index_in_dim(couple_table, k, 1, False), axis=1)
        value = lax.dynamic_index_in_dim(start_table, k, 1, False) - taken
        amp = 0.25 * (value + jnp.sum(value) / nchan)
        return lax.dynamic_update_index_in_dim(amps, amp, k, 1)

    amps = lax.fori_loop(0, STEPS, solve, jnp.zeros((nchan, STEPS), jnp.float32))
    own_amps = jnp.sum(chan_hot[:, None] * amps, axis=0)

    def apply(k, image):
        return subtract(image, positions[k, 0], positions[k, 1], own_amps[k])

    image = lax.fori_loop(0, STEPS, apply, image)
    count = slab * nrows * ncols
    parts = lax.psum_scatter(image, "chan", scatter_dimension=1, tiled=True)
    total = lax.psum(jnp.sum(parts * parts), ("chan", "rows"))
    normalized = parts * lax.rsqrt(total / count + 1e-06)
    return (image[None], normalized)


def solution(mesh):
    return jax.shard_map(
        on_device,
        mesh=mesh,
        in_specs=(P("chan", "rows", None), P("chan", "rows", None), P()),
        out_specs=(P("chan", "rows", None), P("rows", "chan")),
        check_vma=False,
    )
```
